256 devices in a mesh: dp: 16 (over x_lo, y, core), expert: 16 (over x_hi, z).
Axes of the slice: x: 4 (x_hi: 2, x_lo: 2; x = x_hi * 2 + x_lo), y: 4, z: 8, core: 2. Of those that a mesh axis runs over, the one named last changes fastest.
Arguments:
- tokens: bfloat16 [2048, 2048], P('expert', 'dp'), may hold values from -6 to 6
- routes: int32 [2048, 2], P('expert'), may hold values from 0 to 15, all different within a row
- dt_raw: float32 [2048, 32], P('expert', 'dp'), may hold values from -5 to 5
- b_proj: float32 [2048, 16], P('expert'), may hold values from -1.8 to 1.8
- c_proj: float32 [2048, 16], P('expert'), may hold values from -1.8 to 1.8
- decay_rate: float32 [32], P('dp'), may hold values from 0.002 to 0.2
- skip_gain: float32 [32], P('dp'), may hold values from 0.5 to 1.5
- router_weight: float32 [2048, 16], P('dp'), may hold values from -0.125 to 0.125
- gate_weight: bfloat16 [16, 2048, 7168], P('expert', None, 'dp'), may hold values from -0.125 to 0.125
- up_weight: bfloat16 [16, 2048, 7168], P('expert', None, 'dp'), may hold values from -0.125 to 0.125
- down_weight: bfloat16 [16, 7168, 2048], P('expert', 'dp'), may hold values from -0.0625 to 0.0625
- out_grad: bfloat16 [2048, 2048], P('expert', 'dp'), may hold values from -6 to 6
Outputs:
- block_out: bfloat16 [2048, 2048], P('expert', 'dp')
- token_grad: bfloat16 [2048, 2048], P('expert', 'dp')
- gate_grad: bfloat16 [16, 2048, 7168], P('expert', None, 'dp')
- up_grad: bfloat16 [16, 2048, 7168], P('expert', None, 'dp')
- down_grad: bfloat16 [16, 7168, 2048], P('expert', 'dp')
- router_grad: float32 [2048, 16], P('dp')
- rate_grad: float32 [32], P('dp')
- skip_grad: float32 [32], P('dp')
The draws below stay inside these ranges and needn't reach their ends.
Inputs may be any that keep to these rules, and one draw needn't show every extreme that they name: `routes`: each token names two different experts.
All inputs are finite; a program needn't handle non-finite values.
Results may differ from the reference program's by a relative error of at most 0.02.
Values may be sent and summed in bfloat16 or wider, within the bound.
A program may use at most 64 MiB of HBM per device.

```python
import math
import jax
import jax.numpy as jnp
from jax import lax

D = 2048
FF = 7168
HEAD_DIM = 64
STATE = 16
TOK_DEV = 128
CAP = 20
HEADS = 32
EXPERTS = 16
LENGTH = 2048
N_DP = 16
N_EXPERT = 16


def shard_levels(rng, dims, cuts, least, largest):
    level, own = 1.0, jax.random.fold_in(rng, 6)
    for position, shards_of in cuts:
        draws = jnp.exp(jax.random.uniform(jax.random.fold_in(own, position), (shards_of,), jnp.float32, least / len(cuts), largest / len(cuts)))
        level = level * jnp.repeat(draws, dims[position] // shards_of).reshape([-1 if axis == position else 1 for axis in range(len(dims))])
    return level


def different_ones(rng, rows, amount, top, lift):
    order = jax.random.permutation(jax.random.fold_in(rng, 1), amount)
    favour = order
    for power in range(3):
        favour = favour * favour // amount
    favour = favour * lift // amount
    lots = jax.random.randint(jax.random.fold_in(rng, 2), (rows, amount), 0, 4096) + favour
    fixed_rows = jax.random.permutation(jax.random.fold_in(rng, 3), rows)[jnp.arange(amount) % rows]
    lots = jnp.where(jnp.arange(rows)[:, None] == fixed_rows[None, :], 1 << 14, lots)
    priority = lots * amount + jnp.arange(amount)
    return lax.top_k(priority.astype(jnp.int32), top)[1].astype(jnp.int32)


def normal_values(stream_key, dims, scale, bound, cuts=(), kind=jnp.bfloat16):
    loudness = shard_levels(stream_key, dims, cuts, -0.22, 0.18) if cuts else 1.0
    drawn = jax.random.normal(stream_key, dims, jnp.float32) * scale * loudness
    return jnp.minimum(jnp.maximum(drawn, -bound), bound).astype(kind)


def setup_inputs(seed: int = 0) -> dict:
    splits = jax.random.split(jax.random.key(seed), 13)
    tokens = normal_values(splits[0], (LENGTH, D), 1.0, 6.0, ((0, 16), (1, 16)))
    routes = different_ones(splits[1], LENGTH, EXPERTS, 2, 2048)
    dt_raw = normal_values(splits[2], (LENGTH, HEADS), 1.0, 5.0, ((0, 16), (1, 16)), jnp.float32)
    b_proj = normal_values(splits[3], (LENGTH, STATE), 0.3, 1.8, ((0, 16),), jnp.float32)
    c_proj = normal_values(splits[4], (LENGTH, STATE), 0.3, 1.8, ((0, 16),), jnp.float32)
    decay_rate = jnp.clip(jnp.exp(math.log(0.2) - 4.6051702 * jax.random.uniform(splits[5], (HEADS,), jnp.float32) ** shard_levels(splits[5], (HEADS,), ((0, 16),), -0.2, 0.2)), 0.002, 0.2)
    skip_gain = jnp.clip(0.5 + 1.0 * jax.random.uniform(splits[6], (HEADS,), jnp.float32) ** shard_levels(splits[6], (HEADS,), ((0, 16),), -0.2, 0.2), 0.5, 1.5)
    router_weight = normal_values(splits[7], (D, EXPERTS), D ** -0.5, 0.125, ((0, 16),), jnp.float32)
    gate_weight = normal_values(splits[8], (EXPERTS, D, FF), D ** -0.5, 0.125, ((0, 16), (2, 16)))
    up_weight = normal_values(splits[9], (EXPERTS, D, FF), D ** -0.5, 0.125, ((0, 16), (2, 16)))
    down_weight = normal_values(splits[10], (EXPERTS, FF, D), FF ** -0.5, 0.0625, ((0, 16), (1, 16)))
    out_grad = normal_values(splits[11], (LENGTH, D), 1.0, 6.0, ((0, 16), (1, 16)))
    return {"tokens": tokens, "routes": routes, "dt_raw": dt_raw, "b_proj": b_proj, "c_proj": c_proj, "decay_rate": decay_rate, "skip_gain": skip_gain, "router_weight": router_weight, "gate_weight": gate_weight, "up_weight": up_weight, "down_weight": down_weight, "out_grad": out_grad}


EPSILON = 1e-06
HIGHEST = lax.Precision.HIGHEST

def rms_norm(values):
    return values * lax.rsqrt(lax.optimization_barrier(jnp.mean(values * values, axis=-1, keepdims=True)) + EPSILON)

def end_parts(normed, b_rows, dt_rows, decay_rate):
    steps_total = normed.shape[0]
    head_count = decay_rate.shape[0]
    step_size = jax.nn.softplus(dt_rows)
    running = jnp.cumsum(-step_size * decay_rate[None, :], axis=0)
    tail_weight = jnp.exp(running[-1][None, :] - running) * step_size
    head_rows = normed.reshape(steps_total, head_count, -1)
    local_state = jnp.einsum('sh,shp,sn->hpn', tail_weight, head_rows, b_rows, precision=HIGHEST)
    return (jnp.exp(running[-1]), local_state.reshape(head_count, -1))

def ssd_piece(normed, b_rows, c_rows, dt_rows, decay_rate, skip_gain, state_start):
    steps_total = normed.shape[0]
    head_count = decay_rate.shape[0]
    state_width = b_rows.shape[1]
    step_size = jax.nn.softplus(dt_rows)
    running = jnp.cumsum(-step_size * decay_rate[None, :], axis=0)
    positions = jnp.arange(steps_total, dtype=jnp.int32)
    causal = (positions[:, None] >= positions[None, :])[:, :, None]
    spread = jnp.where(causal, running[:, None, :] - running[None, :, :], 0.0)
    decay_table = jnp.where(causal, jnp.exp(spread), 0.0)
    pairing = jnp.dot(c_rows, b_rows.T, precision=HIGHEST)
    mixing = decay_table * pairing[:, :, None] * step_size[None, :, :]
    head_rows = normed.reshape(steps_total, head_count, -1)
    state_three = state_start.reshape(head_count, -1, state_width)
    mixed = jnp.einsum('tsh,shp->thp', mixing, head_rows, precision=HIGHEST)
    mixed = mixed + jnp.einsum('tn,th,hpn->thp', c_rows, jnp.exp(running), state_three, precision=HIGHEST)
    mixed = mixed + skip_gain[None, :, None] * head_rows
    decay_total, local_state = end_parts(normed, b_rows, dt_rows, decay_rate)
    state_end = decay_total[:, None] * state_start + local_state
    return (mixed.reshape(steps_total, -1), state_end)

def dispatch_table(choice_ids, expert_count, capacity):
    flat_ids = choice_ids.reshape(-1)
    row_total = flat_ids.shape[0]
    expert_hot = (flat_ids[:, None] == jnp.arange(expert_count, dtype=jnp.int32)[None, :]).astype(jnp.float32)
    positions = jnp.arange(row_total, dtype=jnp.int32)
    lower = (positions[:, None] > positions[None, :]).astype(jnp.float32)
    earlier = jnp.dot(lower, expert_hot, precision=HIGHEST)
    slot_index = lax.optimization_barrier(jnp.sum(earlier * expert_hot, axis=1))
    target = flat_ids.astype(jnp.float32) * capacity + slot_index
    target = jnp.where(slot_index < capacity, target, -1.0)
    slot_ids = jnp.arange(expert_count * capacity, dtype=jnp.int32).astype(jnp.float32)
    return (slot_ids[:, None] == target[None, :]).astype(jnp.float32)

def block_sum(parts):
    rounded = lax.optimization_barrier(parts.astype(jnp.bfloat16))
    return lax.optimization_barrier(jnp.sum(rounded.astype(jnp.float32), axis=1)).astype(jnp.bfloat16)

def reference(tokens, routes, dt_raw, b_proj, c_proj, decay_rate, skip_gain, router_weight, gate_weight, up_weight, down_weight, out_grad):
    blocks = N_EXPERT
    unit_size = FF // N_DP
    inputs = tokens.astype(jnp.float32)

    def mixer_all(inputs_in, rate_in, skip_in):
        normed = rms_norm(inputs_in).reshape(blocks, TOK_DEV, D)

        def one_block(state, pieces):
            normed_rows, b_rows, c_rows, dt_rows = pieces
            mixed_rows, state_end = ssd_piece(normed_rows, b_rows, c_rows, dt_rows, rate_in, skip_in, state)
            return (state_end, mixed_rows)
        zero_state = jnp.zeros((HEADS, HEAD_DIM * STATE), jnp.float32)
        final_state, mixed_all = lax.scan(one_block, zero_state, (normed, b_proj.reshape(blocks, TOK_DEV, STATE), c_proj.reshape(blocks, TOK_DEV, STATE), dt_raw.reshape(blocks, TOK_DEV, HEADS)))
        return mixed_all.reshape(LENGTH, D)
    mixed, mixer_pull = jax.vjp(mixer_all, inputs, decay_rate, skip_gain)
    resid = (inputs + mixed).astype(jnp.bfloat16)
    resid_f = resid.astype(jnp.float32).reshape(blocks, TOK_DEV, D)
    pre_moe, norm_pull = jax.vjp(rms_norm, resid_f)
    moe_in = pre_moe.astype(jnp.bfloat16)
    moe_f = moe_in.astype(jnp.float32)
    choice_ids = routes.reshape(blocks, TOK_DEV, 2)
    logits = jnp.einsum('btd,de->bte', moe_f, router_weight, precision=HIGHEST)
    expert_ids = jnp.arange(EXPERTS, dtype=jnp.int32)
    first_hot = (choice_ids[:, :, 0:1] == expert_ids).astype(jnp.float32)
    second_hot = (choice_ids[:, :, 1:2] == expert_ids).astype(jnp.float32)
    logit_gap = lax.optimization_barrier(jnp.sum(logits * (first_hot - second_hot), axis=2))
    first_weight = jax.nn.sigmoid(logit_gap)
    second_weight = jax.nn.sigmoid(-logit_gap)
    tables = jax.vmap(lambda ids_block: dispatch_table(ids_block, EXPERTS, CAP))(choice_ids)
    doubled = jnp.repeat(moe_f, 2, axis=1)
    send_rows = jnp.einsum('bsp,bpd->bsd', tables, doubled, precision=HIGHEST).astype(jnp.bfloat16)

    def to_experts(rows):
        shaped = rows.reshape(N_EXPERT, EXPERTS, CAP, D)
        return shaped.transpose(1, 0, 2, 3).reshape(EXPERTS, blocks * CAP, D)

    def from_experts(rows):
        shaped = rows.reshape(EXPERTS, N_EXPERT, CAP, D)
        return shaped.transpose(1, 0, 2, 3).reshape(blocks, EXPERTS * CAP, D)
    expert_rows = to_experts(send_rows)

    def expert_forward(pieces):
        rows, gate_w, up_w, down_w = pieces
        gate_pre = jnp.dot(rows, gate_w, preferred_element_type=jnp.float32)
        up_pre = jnp.dot(rows, up_w, preferred_element_type=jnp.float32)
        hidden = (jax.nn.silu(gate_pre) * up_pre).astype(jnp.bfloat16)
        parts = jnp.einsum('rbf,bfd->rbd', hidden.astype(jnp.float32).reshape(-1, N_DP, unit_size), down_w.astype(jnp.float32).reshape(N_DP, unit_size, D), precision=HIGHEST)
        return block_sum(parts)
    expert_out = lax.map(expert_forward, (expert_rows, gate_weight, up_weight, down_weight))
    back_rows = from_experts(expert_out).astype(jnp.float32)
    per_slot = jnp.einsum('bsp,bsd->bpd', tables, back_rows, precision=HIGHEST).reshape(blocks, TOK_DEV, 2, D)
    moe_sum = first_weight[:, :, None] * per_slot[:, :, 0] + second_weight[:, :, None] * per_slot[:, :, 1]
    block_out = (resid_f + moe_sum).astype(jnp.bfloat16).reshape(LENGTH, D)
    upstream = out_grad.astype(jnp.float32).reshape(blocks, TOK_DEV, D)
    first_back = lax.optimization_barrier(jnp.sum(upstream * per_slot[:, :, 0], axis=2))
    second_back = lax.optimization_barrier(jnp.sum(upstream * per_slot[:, :, 1], axis=2))
    slot_grad = jnp.stack([first_weight[:, :, None] * upstream, second_weight[:, :, None] * upstream], axis=2)
    slot_grad = slot_grad.reshape(blocks, 2 * TOK_DEV, D).astype(jnp.bfloat16)
    grad_send = jnp.einsum('bsp,bpd->bsd', tables, slot_grad.astype(jnp.float32), precision=HIGHEST).astype(jnp.bfloat16)
    grad_rows_all = to_experts(grad_send)

    def expert_backward(pieces):
        rows, grad_rows, gate_w, up_w, down_w = pieces
        gate_pre = jnp.dot(rows, gate_w, preferred_element_type=jnp.float32)
        up_pre = jnp.dot(rows, up_w, preferred_element_type=jnp.float32)
        hidden = (jax.nn.silu(gate_pre) * up_pre).astype(jnp.bfloat16)
        unit_grad = lax.dot_general(grad_rows, down_w, (((1,), (1,)), ((), ())), preferred_element_type=jnp.float32)
        sigma = jax.nn.sigmoid(gate_pre)
        gate_back = (unit_grad * up_pre * sigma * (1.0 + gate_pre * (1.0 - sigma))).astype(jnp.bfloat16)
        up_back = (unit_grad * jax.nn.silu(gate_pre)).astype(jnp.bfloat16)
        down_part = lax.dot_general(hidden, grad_rows, (((0,), (0,)), ((), ())), preferred_element_type=jnp.float32)
        gate_part = lax.dot_general(rows, gate_back, (((0,), (0,)), ((), ())), preferred_element_type=jnp.float32)
        up_part = lax.dot_general(rows, up_back, (((0,), (0,)), ((), ())), preferred_element_type=jnp.float32)
        parts = jnp.einsum('rbf,dbf->rbd', gate_back.astype(jnp.float32).reshape(-1, N_DP, unit_size), gate_w.astype(jnp.float32).reshape(D, N_DP, unit_size), precision=HIGHEST)
        parts = parts + jnp.einsum('rbf,dbf->rbd', up_back.astype(jnp.float32).reshape(-1, N_DP, unit_size), up_w.astype(jnp.float32).reshape(D, N_DP, unit_size), precision=HIGHEST)
        return (block_sum(parts), gate_part.astype(jnp.bfloat16), up_part.astype(jnp.bfloat16), down_part.astype(jnp.bfloat16))
    input_back, gate_grad, up_grad, down_grad = lax.map(expert_backward, (expert_rows, grad_rows_all, gate_weight, up_weight, down_weight))
    returned = from_experts(input_back).astype(jnp.float32)
    slot_back = jnp.einsum('bsp,bsd->bpd', tables, returned, precision=HIGHEST).reshape(blocks, TOK_DEV, 2, D)
    moe_grad = slot_back[:, :, 0] + slot_back[:, :, 1]
    gap_grad = first_weight * second_weight * (first_back - second_back)
    logit_grad = gap_grad[:, :, None] * (first_hot - second_hot)
    moe_in_grad = moe_grad + jnp.einsum('bte,de->btd', logit_grad, router_weight, precision=HIGHEST)
    router_grad = jnp.einsum('btd,bte->de', moe_f, logit_grad, precision=HIGHEST)
    resid_grad = upstream + norm_pull(moe_in_grad)[0]
    resid_grad = resid_grad.reshape(LENGTH, D)
    mixer_input_grad, rate_grad, skip_grad = mixer_pull(resid_grad)
    token_grad = (resid_grad + mixer_input_grad).astype(jnp.bfloat16)
    return (block_out, token_grad, gate_grad, up_grad, down_grad, router_grad, rate_grad, skip_grad)
```

```python
import functools

import jax
import jax.numpy as jnp
from jax import lax
from jax.experimental import pallas as pl
from jax.experimental.pallas import tpu as pltpu
from jax.sharding import PartitionSpec as P

EPSILON = 1e-06
CAPACITY = 20
SLOT_PAD = 32
HIGH = lax.Precision.HIGHEST
F32 = jnp.float32
BF16 = jnp.bfloat16
MESH = pl.DeviceIdType.MESH
NN = (((1,), (0,)), ((), ()))
NT = (((1,), (1,)), ((), ()))


def mm(a, b, dims=NN, precision=None):
    return lax.dot_general(a, b, dims, precision=precision, preferred_element_type=F32)


def iota(shape, dim):
    return lax.broadcasted_iota(jnp.int32, shape, dim)


def remote(src, dst, send_sem, recv_sem, axis, peer):
    return pltpu.make_async_remote_copy(
        src_ref=src,
        dst_ref=dst,
        send_sem=send_sem,
        recv_sem=recv_sem,
        device_id={axis: peer},
        device_id_type=MESH,
    )


class Exchange:
    def __init__(self, axis, me, size, src, dst, sems, same=False):
        self.axis, self.me, self.size = axis, me, size
        self.src, self.dst, self.sems, self.same = src, dst, sems, same

    def copy(self, peer):
        src = self.dst.at[self.me] if self.same else self.src.at[peer]
        return remote(
            src, self.dst.at[self.me], self.sems.at[0, peer], self.sems.at[1, self.me], self.axis, peer
        )

    def arrival(self, peer):
        spot = self.dst.at[peer]
        return remote(spot, spot, self.sems.at[0, peer], self.sems.at[1, peer], self.axis, peer)

    def each(self, act, low=None, high=None):
        if low is None:
            def step(k, carry):
                act(lax.rem(self.me + k, self.size))
                return carry

            lax.fori_loop(1, self.size, step, 0)
        else:
            def step(p, carry):
                act(p)
                return carry

            lax.fori_loop(low, high, step, 0)

    def start(self, low=None, high=None):
        self.each(lambda p: self.copy(p).start(), low, high)

    def wait(self, low=None, high=None):
        self.each(lambda p: self.arrival(p).wait_recv(), low, high)

    def drain(self, low=None, high=None):
        self.each(lambda p: self.copy(p).wait_send(), low, high)


def block_kernel(
    dims,
    x_ref,
    routes_ref,
    dt_ref,
    b_ref,
    c_ref,
    rate_ref,
    skip_ref,
    rw_ref,
    og_ref,
    wg_hbm,
    wu_hbm,
    wd_hbm,
    block_ref,
    token_ref,
    router_ref,
    small_ref,
    u_hbm,
    g_hbm,
    gt_hbm,
    ut_hbm,
    ht_hbm,
    wg,
    wu,
    wd,
    rows_u,
    rows_g,
    gacc,
    uacc,
    vacc,
    hid,
    gb,
    ub,
    gs,
    us,
    hs,
    gst,
    ust,
    hst,
    cols,
    zrow,
    keep,
    pair_out,
    pair_in,
    rs_out,
    rs_in,
    ar1,
    ar2,
    ar3,
    ar4,
    dec,
    st,
    dl,
    sg,
    tot,
    rout,
    og_out,
    og_in,
    xs_out,
    xs_in,
    sq_out,
    sq_in,
    sb_out,
    sb_in,
    bk_out,
    bk_in,
    mt,
    spread,
    local_sem,
    ag_sem,
    pair_sem,
    rs_sem,
    sem_d,
    sem_e,
):
    nd, ne, t_n, f_n, d_all, cap = dims
    pad = SLOT_PAD
    heads = dt_ref.shape[0]
    hp = f_n // heads
    n_state = b_ref.shape[0]
    rows = ne * cap
    spots = ne * pad
    chips = nd // 2
    ny = min(4, chips)
    nx = chips // ny
    me_d = lax.axis_index("dp")
    me_e = lax.axis_index("expert")
    core = lax.rem(me_d, 2)
    chip = me_d // 2
    chip_x, chip_y = chip // ny, lax.rem(chip, ny)
    partner = me_d + 1 - 2 * core

    def chip_after(i):
        return lax.rem(chip_x + i // ny, nx) * ny + lax.rem(chip_y + lax.rem(i, ny), ny)

    def chip_before(i):
        return lax.rem(chip_x + nx - i // ny, nx) * ny + lax.rem(chip_y + ny - lax.rem(i, ny), ny)

    weight_copies = [
        pltpu.make_async_copy(src, dst, local_sem.at[k])
        for k, (src, dst) in enumerate(((wd_hbm, wd), (wg_hbm, wg), (wu_hbm, wu)))
    ]
    for copy in weight_copies:
        copy.start()

    barrier = pltpu.get_barrier_semaphore()

    def greet(axis, me, size):
        def step(k, carry):
            pl.semaphore_signal(
                barrier, inc=1, device_id={axis: lax.rem(me + k, size)}, device_id_type=MESH
            )
            return carry

        lax.fori_loop(1, size, step, 0)

    greet("dp", me_d, nd)
    greet("expert", me_e, ne)

    def on_dp(dst, k):
        return Exchange("dp", me_d, nd, None, dst, sem_d.at[k], same=True)

    def on_expert(dst, k, src=None):
        return Exchange("expert", me_e, ne, src, dst, sem_e.at[k], same=src is None)

    ex_ar1, ex_ar2, ex_ar3, ex_ar4 = (on_dp(r, k) for k, r in enumerate((ar1, ar2, ar3, ar4)))
    ex_dec, ex_st, ex_dl, ex_sg, ex_tot, ex_rout = (
        on_expert(r, k) for k, r in enumerate((dec, st, dl, sg, tot, rout))
    )
    ex_og = on_expert(og_in, 6, og_out)
    ex_xs = on_expert(xs_in, 7, xs_out)
    ex_sq = on_expert(sq_in, 8, sq_out)
    ex_sb = on_expert(sb_in, 9, sb_out)
    ex_bk = [on_expert(bk_in.at[k], 10 + k, bk_out.at[k]) for k in range(2)]

    x_t = x_ref[...].astype(F32).T
    ar1[me_d] = jnp.sum(x_t * x_t, axis=0, keepdims=True)
    row_id, col_id = iota((t_n, t_n), 0), iota((t_n, t_n), 1)
    causal = row_id <= col_id
    step_size = jnp.maximum(dt_ref[...], 0.0) + jnp.log1p(jnp.exp(-jnp.abs(dt_ref[...])))
    cum = mm(step_size, causal.astype(F32), NN, HIGH)
    head_lane = iota((1, f_n), 1) < hp
    head_row = iota((f_n, t_n), 0) < hp
    last = [jnp.sum(step_size[h : h + 1], axis=1, keepdims=True) for h in range(heads)]
    fade = [jnp.exp(-rate_ref[h] * last[h]) for h in range(heads)]
    dec[me_e] = jnp.concatenate(
        [
            jnp.where(head_lane, fade[0], fade[1]),
            jnp.where(head_lane, -last[0] * fade[0], -last[1] * fade[1]),
        ],
        axis=0,
    )

    expert_row = iota((ne, t_n), 0)
    hot_a = (expert_row == routes_ref[0:1, :]).astype(F32)
    hot_b = (expert_row == routes_ref[1:2, :]).astype(F32)
    before = mm((hot_a + hot_b).astype(BF16), (row_id < col_id).astype(BF16))
    spread_rows = (iota((spots, ne), 0) // pad == iota((spots, ne), 1)).astype(BF16)
    slot_of = iota((spots, t_n), 0) % pad
    fits = slot_of < cap
    here = (mm(spread_rows, before.astype(BF16)) == slot_of.astype(F32)) & fits
    pick_a = jnp.where(here, mm(spread_rows, hot_a.astype(BF16)), 0.0)
    pick_b = jnp.where(here, mm(spread_rows, hot_b.astype(BF16)), 0.0)
    pick = (pick_a + pick_b).astype(BF16)
    og = og_ref[...]
    og_out[...] = mm(pick, og).astype(BF16).reshape(ne, pad, f_n)
    og_in[me_e] = og_out[me_e]

    pl.semaphore_wait(barrier, nd + ne - 2)
    ex_ar1.start()
    ex_og.start()
    ex_dec.start()

    b_rows, c_rows = b_ref[...], c_ref[...]
    pairing = mm(b_rows.T, c_rows, NN, HIGH)
    fades, tails = [], []
    for h in range(heads):
        cum_h, dt_h = cum[h : h + 1], step_size[h : h + 1]
        gap = jnp.where(causal, cum_h - jnp.broadcast_to(cum_h, (t_n, t_n)).T, 0.0)
        spread[h] = gap
        mt[h] = (
            jnp.where(causal, jnp.exp(-rate_ref[h] * gap), 0.0)
            * pairing
            * jnp.broadcast_to(dt_h, (t_n, t_n)).T
        )
        fades.append(jnp.exp(-rate_ref[h] * cum_h))
        tails.append(jnp.exp(-rate_ref[h] * (last[h] - cum_h)) * dt_h)
    tail = jnp.where(head_row, tails[0], tails[1])
    reach = jnp.where(head_row, cum[0:1] - last[0], cum[1:2] - last[1])
    skip_f = jnp.where(head_row, skip_ref[0], skip_ref[1])
    hot_gap = hot_a - hot_b
    rw_gap = mm(rw_ref[...].T, hot_gap, NN, HIGH)
    spot_q = iota((rows, spots), 1)
    compact = (
        ((spot_q // pad) * cap + spot_q % pad == iota((rows, spots), 0)) & (spot_q % pad < cap)
    ).astype(BF16)
    of_block_r, of_block_b = iota((rows, ne), 0), iota((rows, ne), 1) * cap
    of_block = ((of_block_r >= of_block_b) & (of_block_r < of_block_b + cap)).astype(F32)
    lane_r = iota((rows, 128), 0)
    slot_r = lane_r - (lane_r * ((1 << 20) // cap + 1) >> 20) * cap
    lane_first = iota((rows, 128), 1) == slot_r
    lane_second = iota((rows, 128), 1) == slot_r + 64

    ex_ar1.wait()
    scale_one = lax.rsqrt(jnp.sum(ar1[...], axis=0) / d_all + EPSILON)
    normed = x_t * scale_one
    st[me_e] = mm(b_rows, normed * tail, NT, HIGH)
    ex_st.start(me_e + 1, ne)
    dl[me_e] = mm(b_rows, normed * tail * reach, NT, HIGH)
    ex_dl.start(me_e + 1, ne)
    mixed = jnp.concatenate(
        [mm(normed[h * hp : (h + 1) * hp], mt[h], NN, HIGH) for h in range(heads)], axis=0
    )
    mixed = mixed + skip_f * normed

    def ag_begin(buf, k):
        def step(i, carry):
            peer = chip_after(i) * 2 + core
            remote(
                buf.at[me_d], buf.at[me_d], ag_sem.at[k, 0, i], ag_sem.at[k, 1, i], "dp", peer
            ).start()
            return carry

        remote(
            buf.at[me_d], buf.at[me_d], ag_sem.at[k, 2, 0], ag_sem.at[k, 3, 0], "dp", partner
        ).start()
        lax.fori_loop(1, chips, step, 0)

    def ag_forward(buf, k, i):
        spot = buf.at[chip_before(i) * 2 + core]
        remote(
            spot, spot, ag_sem.at[k, 0, i], ag_sem.at[k, 1, i], "dp", chip_before(i) * 2 + core
        ).wait_recv()
        remote(spot, spot, ag_sem.at[k, 2, i], ag_sem.at[k, 3, i], "dp", partner).start()

    def ag_partner(buf, k, i):
        spot = buf.at[chip_before(i) * 2 + 1 - core]
        remote(spot, spot, ag_sem.at[k, 2, i], ag_sem.at[k, 3, i], "dp", partner).wait_recv()

    def ag_drain(buf, k):
        def step(i, carry):
            remote(
                buf.at[me_d], buf.at[me_d], ag_sem.at[k, 0, i], ag_sem.at[k, 1, i], "dp", chip_after(i) * 2 + core
            ).wait_send()
            spot = buf.at[chip_before(i) * 2 + core]
            remote(spot, spot, ag_sem.at[k, 2, i], ag_sem.at[k, 3, i], "dp", partner).wait_send()
            return carry

        remote(
            buf.at[me_d], buf.at[me_d], ag_sem.at[k, 2, 0], ag_sem.at[k, 3, 0], "dp", partner
        ).wait_send()
        lax.fori_loop(1, chips, step, 0)

    def ag_consume(buf, k, use):
        def step(i, carry):
            @pl.when(i < chips)
            def _():
                ag_forward(buf, k, i)

            ag_partner(buf, k, i - 1)
            j = chip_before(i - 1)
            both = jnp.concatenate([buf[2 * j], buf[2 * j + 1]], axis=1)
            use(both, pl.ds(pl.multiple_of(j * 2 * f_n, 2 * f_n), 2 * f_n))
            return carry

        lax.fori_loop(1, chips + 1, step, 0)

    ex_og.wait()
    rows_g[me_d] = mm(compact, og_in[...].reshape(spots, f_n)).astype(BF16)
    ag_begin(rows_g, 0)

    ex_dec.wait()

    def carry_state(j, state):
        ex_st.arrival(j).wait_recv()
        return dec[j][0:1] * state + st[j]

    state_in = lax.fori_loop(0, me_e, carry_state, jnp.zeros((n_state, f_n), F32))
    state_col = state_in.T
    from_state = jnp.concatenate(
        [mm(state_col[h * hp : (h + 1) * hp], c_rows * fades[h], NN, HIGH) for h in range(heads)],
        axis=0,
    )
    resid_t = (x_t + (mixed + from_state)).astype(BF16).astype(F32)
    resid = resid_t.T.astype(BF16)
    ar2[me_d] = jnp.concatenate(
        [
            jnp.sum(resid_t * resid_t, axis=0, keepdims=True),
            jnp.sum(resid_t * rw_gap, axis=0, keepdims=True),
        ],
        axis=0,
    )
    ex_ar2.start()
    xs_out[...] = mm(pick, resid).astype(BF16).reshape(ne, pad, f_n)
    xs_in[me_e] = xs_out[me_e]
    ex_xs.start()

    def carry_slope(j, both):
        state, slope = both
        ex_dl.arrival(j).wait_recv()
        here_dec = dec[j]
        return (
            here_dec[0:1] * state + st[j],
            here_dec[0:1] * slope + here_dec[1:2] * state + dl[j],
        )

    zero_state = jnp.zeros((n_state, f_n), F32)
    slope_in = lax.fori_loop(0, me_e, carry_slope, (zero_state, zero_state))[1]

    ex_ar2.wait()
    sums = jnp.sum(ar2[...], axis=0)
    scale_two = lax.rsqrt(sums[0:1] / d_all + EPSILON)
    gap_raw = sums[1:2]
    logit_gap = scale_two * gap_raw
    first_w = 1.0 / (1.0 + jnp.exp(-logit_gap))
    second_w = 1.0 / (1.0 + jnp.exp(logit_gap))
    scale_col = jnp.sum((pick_a + pick_b) * scale_two, axis=1, keepdims=True)
    weight_col = jnp.sum(pick_a * first_w + pick_b * second_w, axis=1, keepdims=True)
    lane_q = iota((spots, 128), 1)
    slot_q = iota((spots, 128), 0) % pad
    lined = jnp.where(lane_q == slot_q, scale_col, 0.0) + jnp.where(
        lane_q == slot_q + 64, weight_col, 0.0
    )
    lined = jnp.sum(lined.reshape(ne, pad, 128), axis=1)
    for e in range(ne):
        sq_out[e] = lined[e : e + 1]
    sq_in[me_e] = sq_out[me_e]
    ex_sq.start()

    weight_copies[0].wait()
    vacc[...] = jnp.zeros_like(vacc)

    def use_grad(both, span):
        vacc[...] += mm(both, wd[:, span], NT)

    ag_consume(rows_g, 0, use_grad)

    ex_xs.wait()
    rows_u[me_d] = mm(compact, xs_in[...].reshape(spots, f_n)).astype(BF16)
    ag_begin(rows_u, 1)
    weight_copies[1].wait()
    weight_copies[2].wait()
    gacc[...] = jnp.zeros_like(gacc)
    uacc[...] = jnp.zeros_like(uacc)
    ex_sq.wait()

    def by_row(ref):
        table = jnp.concatenate([ref[b] for b in range(ne)], axis=0)
        return mm(of_block, table, NN, HIGH)

    wide = by_row(sq_in)
    cols[0] = jnp.sum(jnp.where(lane_first, wide, 0.0), axis=1, keepdims=True)
    cols[1] = jnp.sum(jnp.where(lane_second, wide, 0.0), axis=1, keepdims=True)

    def use_rows(both, span):
        gacc[...] += mm(both, wg[:, span], NT)
        uacc[...] += mm(both, wu[:, span], NT)

    ag_consume(rows_u, 1, use_rows)
    out_copies = [
        pltpu.make_async_copy(rows_g, g_hbm, local_sem.at[3]),
        pltpu.make_async_copy(rows_u, u_hbm, local_sem.at[4]),
    ]
    for copy in out_copies:
        copy.start()

    part = rows // 5

    def units(k, carry):
        span = pl.ds(pl.multiple_of(k * part, part), part)
        scale, weight = cols[0, span], cols[1, span]
        gate_in, up_in, grad_in = gacc[span], uacc[span], vacc[span]
        gate, up, grad = gate_in * scale, up_in * scale, grad_in * weight
        sigma = 1.0 / (1.0 + jnp.exp(-gate))
        silu = gate * sigma
        hidden = silu * up
        gate_back = grad * up * sigma * (1.0 + gate * (1.0 - sigma))
        up_back = grad * silu
        hid[span] = hidden.astype(BF16)
        gb[span] = gate_back.astype(BF16)
        ub[span] = up_back.astype(BF16)
        gs[span] = gate_back * scale
        us[span] = up_back * scale
        hs[span] = hidden * weight
        pair_sum = jnp.sum(hidden * grad_in, axis=1, keepdims=True)
        inner_sum = jnp.sum(gate_back * gate_in + up_back * up_in, axis=1, keepdims=True)
        lane = iota((part, 128), 1)
        row_r = iota((part, 128), 0) + k * part
        slot = row_r - (row_r * ((1 << 20) // cap + 1) >> 20) * cap
        zrow[span] = jnp.where(lane == slot, pair_sum, 0.0) + jnp.where(
            lane == slot + 64, inner_sum, 0.0
        )
        return carry

    lax.fori_loop(0, 5, units, 0)
    block_t_b, block_t_r = iota((ne, rows), 0) * cap, iota((ne, rows), 1)
    of_block_t = ((block_t_r >= block_t_b) & (block_t_r < block_t_b + cap)).astype(F32)
    ar3[me_d] = mm(of_block_t, zrow[...], NN, HIGH)
    ex_ar3.start()

    def rs_pass(k, terms):
        def finish(i):
            j = chip_after(i)
            remote(
                pair_in.at[k, j], pair_in.at[k, j], pair_sem.at[k, 0, j], pair_sem.at[k, 1, j], "dp", partner
            ).wait_recv()
            total = keep[k, j] + pair_in[k, j].astype(F32)
            rs_out[k, i] = total.astype(BF16)

            @pl.when(i > 0)
            def _():
                rs_copy(k, i).start()

        def step(n, carry):
            @pl.when(n < chips)
            def _():
                i = lax.rem(n + 1, chips)
                j = chip_after(i)
                both = terms(pl.ds(pl.multiple_of(j * 2 * f_n, 2 * f_n), 2 * f_n))
                low, high = both[:, :f_n], both[:, f_n:]
                first = core == 0
                keep[k, j] = jnp.where(first, low, high)
                pair_out[k, j] = jnp.where(first, high, low).astype(BF16)
                pair_copy(k, j).start()

            @pl.when(n > 0)
            def _():
                finish(lax.rem(n, chips))

            return carry

        lax.fori_loop(0, chips + 1, step, 0)

    def pair_copy(k, j):
        return remote(
            pair_out.at[k, j], pair_in.at[k, j], pair_sem.at[k, 0, j], pair_sem.at[k, 1, j], "dp", partner
        )

    def rs_copy(k, i):
        return remote(
            rs_out.at[k, i], rs_in.at[k, i], rs_sem.at[k, 0, i], rs_sem.at[k, 1, i], "dp", chip_after(i) * 2 + core
        )

    rs_pass(0, lambda span: mm(hid[...], wd[:, span]))
    rs_pass(1, lambda span: mm(gb[...], wg[:, span]) + mm(ub[...], wu[:, span]))

    ex_ar3.wait()
    line = jnp.sum(ar3[...], axis=0)
    for b in range(ne):
        sb_out[b] = line[b : b + 1]
    sb_in[me_e] = sb_out[me_e]
    ex_sb.start()

    for k, (src, dst, out) in enumerate(((gs, gst, gt_hbm), (us, ust, ut_hbm), (hs, hst, ht_hbm))):
        dst[...] = src[...].T.astype(BF16)
        copy = pltpu.make_async_copy(dst, out, local_sem.at[5 + k])
        copy.start()
        out_copies.append(copy)

    def rs_finish(k):
        def step(i, total):
            remote(
                rs_in.at[k, i], rs_in.at[k, i], rs_sem.at[k, 0, i], rs_sem.at[k, 1, i], "dp", chip_before(i) * 2 + core
            ).wait_recv()
            return total + rs_in[k, i].astype(F32)

        total = lax.fori_loop(1, chips, step, rs_out[k, 0].astype(F32))
        wide_rows = lax.dot_general(
            compact, total.astype(BF16), (((0,), (0,)), ((), ())), preferred_element_type=F32
        )
        bk_out[k] = wide_rows.astype(BF16).reshape(ne, pad, f_n)
        bk_in[k, me_e] = bk_out[k, me_e]
        ex_bk[k].start()

    rs_finish(0)

    ex_sb.wait()
    table = jnp.concatenate([sb_in[e] for e in range(ne)], axis=0)
    by_spot = mm(spread_rows.astype(F32), table, NN, HIGH)
    pair_spot = jnp.sum(jnp.where(lane_q == slot_q, by_spot, 0.0), axis=1, keepdims=True)
    inner_spot = jnp.sum(jnp.where(lane_q == slot_q + 64, by_spot, 0.0), axis=1, keepdims=True)
    back_gap = jnp.sum((pick_a - pick_b) * pair_spot, axis=0, keepdims=True)
    inner_two = jnp.sum((pick_a + pick_b) * inner_spot, axis=0, keepdims=True)
    gap_grad = first_w * second_w * back_gap
    inner_two = inner_two + gap_grad * gap_raw
    rout[me_e] = mm(hot_gap * (gap_grad * scale_two), resid_t, NT, HIGH)
    ex_rout.start()

    pick_at, pick_bt = pick_a.T.astype(BF16), pick_b.T.astype(BF16)
    resid_base = og.astype(F32).T + scale_two * (gap_grad * rw_gap) - resid_t * (
        scale_two * scale_two * scale_two * inner_two / d_all
    )
    first_m = jnp.broadcast_to(first_w, (f_n, t_n)).T
    second_m = jnp.broadcast_to(second_w, (f_n, t_n)).T

    rs_finish(1)
    ex_bk[0].wait()
    came = bk_in[0].reshape(spots, f_n)
    block_ref[...] = (
        resid.astype(F32) + (first_m * mm(pick_at, came) + second_m * mm(pick_bt, came))
    ).astype(BF16)

    ex_bk[1].wait()
    moe_grad = mm(pick_at + pick_bt, bk_in[1].reshape(spots, f_n)).T
    grad = resid_base + scale_two * moe_grad
    state_grads = [mm(c_rows * fades[h], grad, NT, HIGH) for h in range(heads)]
    state_grad = jnp.where(head_lane, state_grads[0], state_grads[1])
    sg[me_e] = state_grad
    ex_sg.start(0, me_e)

    normed_rows = normed.T
    cum_f = jnp.where(head_row, cum[0:1], cum[1:2])
    rate_row = jnp.sum(state_grad * slope_in, axis=0, keepdims=True)
    state_part = grad * from_state * cum_f
    skip_part = grad * normed
    lane_s = iota((1, 128), 1)
    small = jnp.zeros((1, 128), F32)
    for h in range(heads):
        mine = head_row if h == 0 else jnp.logical_not(head_row)
        mine_lane = head_lane if h == 0 else jnp.logical_not(head_lane)
        pair_grad = mm(normed_rows, jnp.where(mine, grad, 0.0), NN, HIGH)
        table_part = pair_grad * mt[h] * spread[h]
        rows_h = slice(h * hp, (h + 1) * hp)
        rate_h = (
            jnp.sum(jnp.where(mine_lane, rate_row, 0.0), axis=1, keepdims=True)
            - jnp.sum(jnp.sum(table_part, axis=0, keepdims=True), axis=1, keepdims=True)
            - jnp.sum(jnp.sum(state_part[rows_h], axis=0, keepdims=True), axis=1, keepdims=True)
        )
        skip_h = jnp.sum(jnp.sum(skip_part[rows_h], axis=0, keepdims=True), axis=1, keepdims=True)
        small = small + jnp.where(lane_s == h, rate_h, 0.0)
        small = small + jnp.where(lane_s == heads + h, skip_h, 0.0)
    tot[me_e] = small
    ex_tot.start()
    normed_grad = jnp.concatenate(
        [mm(grad[h * hp : (h + 1) * hp], mt[h], NT, HIGH) for h in range(heads)], axis=0
    )
    normed_grad = normed_grad + skip_f * grad

    def carry_grad(n, later):
        j = ne - 1 - n
        ex_sg.arrival(j).wait_recv()
        return dec[j][0:1] * later + sg[j]

    later = lax.fori_loop(0, ne - 1 - me_e, carry_grad, zero_state)
    normed_grad = normed_grad + tail * mm(later.T, b_rows, NN, HIGH)
    ar4[me_d] = jnp.sum(normed_grad * x_t, axis=0, keepdims=True)
    ex_ar4.start()
    ex_rout.wait()
    router_ref[...] = jnp.sum(rout[...], axis=0)
    ex_ar4.wait()
    inner_one = jnp.sum(ar4[...], axis=0)
    token_grad = (
        grad + scale_one * normed_grad - x_t * (scale_one * scale_one * scale_one * inner_one / d_all)
    )
    token_ref[...] = token_grad.T.astype(BF16)
    ex_tot.wait()
    small_ref[...] = jnp.sum(tot[...], axis=0)

    for ex in (ex_ar1, ex_ar2, ex_ar3, ex_ar4, ex_dec, ex_tot, ex_rout, ex_og, ex_xs, ex_sq, ex_sb, *ex_bk):
        ex.drain()
    ex_st.drain(me_e + 1, ne)
    ex_dl.drain(me_e + 1, ne)
    ex_sg.drain(0, me_e)
    ag_drain(rows_g, 0)
    ag_drain(rows_u, 1)
    for k in range(2):
        def step(i, carry, k=k):
            pair_copy(k, i).wait_send()

            @pl.when(i > 0)
            def _():
                rs_copy(k, i).wait_send()

            return carry

        lax.fori_loop(0, chips, step, 0)
    for copy in out_copies:
        copy.wait()


def grads_kernel(u_ref, g_ref, gt_ref, ut_ref, ht_ref, gate_ref, up_ref, down_ref):
    both_u = jnp.concatenate([u_ref[0], u_ref[1]], axis=1)
    both_g = jnp.concatenate([g_ref[0], g_ref[1]], axis=1)
    gate_ref[...] = mm(gt_ref[...], both_u).astype(BF16)
    up_ref[...] = mm(ut_ref[...], both_u).astype(BF16)
    down_ref[...] = mm(ht_ref[...], both_g).astype(BF16)


def body(
    tokens,
    routes,
    dt_raw,
    b_proj,
    c_proj,
    decay_rate,
    skip_gain,
    router_weight,
    gate_weight,
    up_weight,
    down_weight,
    out_grad,
):
    nd, ne = lax.axis_size("dp"), lax.axis_size("expert")
    t_n, f_n = tokens.shape
    heads, n_state = dt_raw.shape[1], b_proj.shape[1]
    d_all = nd * f_n
    units = down_weight.shape[1]
    cap, pad = CAPACITY, SLOT_PAD
    rows, chips = ne * cap, nd // 2
    vmem, hbm, smem = (
        pl.BlockSpec(memory_space=space) for space in (pltpu.VMEM, pl.ANY, pltpu.SMEM)
    )
    def v(*s):
        return pltpu.VMEM(s, F32)

    def h(*s):
        return pltpu.VMEM(s, BF16)

    def shape(s, t):
        return jax.ShapeDtypeStruct(s, t)
    scratch = [
        h(units, d_all),
        h(units, d_all),
        h(units, d_all),
        h(nd, rows, f_n),
        h(nd, rows, f_n),
        v(rows, units),
        v(rows, units),
        v(rows, units),
        h(rows, units),
        h(rows, units),
        h(rows, units),
        v(rows, units),
        v(rows, units),
        v(rows, units),
        h(units, rows),
        h(units, rows),
        h(units, rows),
        v(2, rows, 1),
        v(rows, 128),
        v(2, chips, rows, f_n),
        h(2, chips, rows, f_n),
        h(2, chips, rows, f_n),
        h(2, chips, rows, f_n),
        h(2, chips, rows, f_n),
        v(nd, 1, t_n),
        v(nd, 2, t_n),
        v(nd, ne, 128),
        v(nd, 1, t_n),
        v(ne, 2, f_n),
        v(ne, n_state, f_n),
        v(ne, n_state, f_n),
        v(ne, n_state, f_n),
        v(ne, 1, 128),
        v(ne, ne, f_n),
        h(ne, pad, f_n),
        h(ne, pad, f_n),
        h(ne, pad, f_n),
        h(ne, pad, f_n),
        v(ne, 1, 128),
        v(ne, 1, 128),
        v(ne, 1, 128),
        v(ne, 1, 128),
        h(2, ne, pad, f_n),
        h(2, ne, pad, f_n),
        v(heads, t_n, t_n),
        v(heads, t_n, t_n),
        pltpu.SemaphoreType.DMA((8,)),
        pltpu.SemaphoreType.DMA((2, 4, chips)),
        pltpu.SemaphoreType.DMA((2, 2, chips)),
        pltpu.SemaphoreType.DMA((2, 2, chips)),
        pltpu.SemaphoreType.DMA((4, 2, nd)),
        pltpu.SemaphoreType.DMA((12, 2, ne)),
    ]
    wide = shape((nd, rows, f_n), BF16)
    tall = shape((units, rows), BF16)
    made = pl.pallas_call(
        functools.partial(block_kernel, (nd, ne, t_n, f_n, d_all, cap)),
        out_shape=[
            shape((t_n, f_n), BF16),
            shape((t_n, f_n), BF16),
            shape((ne, f_n), F32),
            shape((1, 128), F32),
            wide,
            wide,
            tall,
            tall,
            tall,
        ],
        in_specs=[vmem] * 5 + [smem] * 2 + [vmem] * 2 + [hbm] * 3,
        out_specs=[vmem] * 4 + [hbm] * 5,
        scratch_shapes=scratch,
        compiler_params=pltpu.CompilerParams(
            collective_id=0, has_side_effects=True, vmem_limit_bytes=44 * 1024 * 1024
        ),
        name="block",
    )(
        tokens,
        routes.T,
        dt_raw.T,
        b_proj.T,
        c_proj.T,
        decay_rate,
        skip_gain,
        router_weight.T,
        out_grad,
        gate_weight[0].T,
        up_weight[0].T,
        down_weight[0],
    )
    block_out, token_grad, router_grad, small, u_rows, g_rows, gt, ut, ht = made
    two = pl.BlockSpec((2, rows, f_n), lambda j: (j, 0, 0))
    whole = pl.BlockSpec((units, rows), lambda j: (0, 0))
    span = pl.BlockSpec((units, 2 * f_n), lambda j: (0, j))
    gate_grad, up_grad, down_grad = pl.pallas_call(
        grads_kernel,
        grid=(chips,),
        out_shape=[shape((units, d_all), BF16)] * 3,
        in_specs=[two, two, whole, whole, whole],
        out_specs=[span] * 3,
        name="grads",
    )(u_rows, g_rows, gt, ut, ht)
    return (
        block_out,
        token_grad,
        gate_grad.T[None],
        up_grad.T[None],
        down_grad[None],
        router_grad.T,
        small[0, :heads],
        small[0, heads : 2 * heads],
    )


def solution(mesh):
    return jax.shard_map(
        body,
        mesh=mesh,
        in_specs=(
            P("expert", "dp"),
            P("expert", None),
            P("expert", "dp"),
            P("expert", None),
            P("expert", None),
            P("dp"),
            P("dp"),
            P("dp", None),
            P("expert", None, "dp"),
            P("expert", None, "dp"),
            P("expert", "dp", None),
            P("expert", "dp"),
        ),
        out_specs=(
            P("expert", "dp"),
            P("expert", "dp"),
            P("expert", None, "dp"),
            P("expert", None, "dp"),
            P("expert", "dp", None),
            P("dp", None),
            P("dp"),
            P("dp"),
        ),
        check_vma=False,
    )
```

```python
import functools

import jax
import jax.numpy as jnp
from jax import lax
from jax.experimental import pallas as pl
from jax.experimental.pallas import tpu as pltpu
from jax.sharding import PartitionSpec as P

EPSILON = 1e-06
CAPACITY = 20
SLOT_PAD = 24
HIGH = lax.Precision.HIGHEST
F32 = jnp.float32
BF16 = jnp.bfloat16
MESH = pl.DeviceIdType.MESH
NN = (((1,), (0,)), ((), ()))
NT = (((1,), (1,)), ((), ()))


def mm(a, b, dims=NN, precision=None):
    return lax.dot_general(a, b, dims, precision=precision, preferred_element_type=F32)


def iota(shape, dim):
    return lax.broadcasted_iota(jnp.int32, shape, dim)


def remote(src, dst, send_sem, recv_sem, axis, peer):
    return pltpu.make_async_remote_copy(
        src_ref=src,
        dst_ref=dst,
        send_sem=send_sem,
        recv_sem=recv_sem,
        device_id={axis: peer},
        device_id_type=MESH,
    )


class Exchange:
    def __init__(self, axis, me, size, src, dst, sems, width=None):
        self.axis, self.me, self.size = axis, me, size
        self.src, self.dst, self.sems, self.width = src, dst, sems, width

    def part(self, ref, spot):
        if self.width is None:
            return ref.at[spot]
        return ref.at[spot, pl.ds(0, self.width)]

    def copy(self, peer):
        src = self.part(self.dst, self.me) if self.src is None else self.part(self.src, peer)
        return remote(
            src, self.part(self.dst, self.me), self.sems.at[0], self.sems.at[1], self.axis, peer
        )

    def start(self):
        def step(k, carry):
            self.copy(lax.rem(self.me + k, self.size)).start()
            return carry

        lax.fori_loop(1, self.size, step, 0)

    def all_blocks(self):
        span = self.part(self.dst, pl.ds(0, self.size - 1))
        peer = lax.rem(self.me + 1, self.size)
        return remote(span, span, self.sems.at[0], self.sems.at[1], self.axis, peer)

    def wait(self):
        self.all_blocks().wait_recv()

    def drain(self):
        self.all_blocks().wait_send()


class Chain:
    def __init__(self, axis, me, size, dst, sems, later):
        self.axis, self.me, self.dst, self.sems = axis, me, dst, sems
        self.low, self.high = (me + 1, size) if later else (0, me)

    def copy(self, peer):
        spot = self.dst.at[self.me]
        return remote(spot, spot, self.sems.at[0, peer], self.sems.at[1, self.me], self.axis, peer)

    def each(self, act):
        def step(p, carry):
            act(self.copy(p))
            return carry

        lax.fori_loop(self.low, self.high, step, 0)

    def start(self):
        self.each(lambda copy: copy.start())

    def drain(self):
        self.each(lambda copy: copy.wait_send())

    def wait_for(self, peer):
        spot = self.dst.at[peer]
        remote(spot, spot, self.sems.at[0, peer], self.sems.at[1, peer], self.axis, peer).wait_recv()


def block_kernel(
    dims,
    *refs,
):
    inputs, outputs, rest = refs[:12], refs[12:19], refs[19:]
    loaded, scratch = rest[:9], rest[9:]
    block_phases(dims, inputs, *loaded, *inputs[9:], *outputs, *scratch)


def block_phases(
    dims,
    inputs,
    x_ref,
    routes_ref,
    dt_ref,
    b_ref,
    c_ref,
    rate_ref,
    skip_ref,
    rw_ref,
    og_ref,
    wg_hbm,
    wu_hbm,
    wd_hbm,
    block_ref,
    token_ref,
    router_ref,
    small_ref,
    gate_ref,
    up_ref,
    down_ref,
    wg,
    wu,
    wd,
    rows_u,
    rows_g,
    gacc,
    uacc,
    vacc,
    hid,
    gb,
    ub,
    gs,
    us,
    hs,
    gst,
    ust,
    hst,
    cols,
    zrow,
    keep,
    pair_out,
    pair_in,
    rs_out,
    rs_in,
    ar1,
    ar2,
    ar3,
    ar4,
    dec,
    st,
    dl,
    sg,
    tot,
    rout,
    og_out,
    og_in,
    xs_out,
    xs_in,
    sq_out,
    sq_in,
    sb_out,
    sb_in,
    bk_out,
    bk_in,
    mt,
    spread,
    local_sem,
    ag_sem,
    pair_sem,
    rs_sem,
    sem_x,
    sem_e,
):
    nd, ne, t_n, f_n, d_all, cap = dims
    pad = SLOT_PAD
    heads = dt_ref.shape[0]
    hp = f_n // heads
    n_state = b_ref.shape[0]
    rows = ne * cap
    spots = ne * pad
    chips = nd // 2
    ny = min(4, chips)
    nx = chips // ny
    me_d = lax.axis_index("dp")
    me_e = lax.axis_index("expert")
    core = lax.rem(me_d, 2)
    chip = me_d // 2
    chip_x, chip_y = chip // ny, lax.rem(chip, ny)
    partner = me_d + 1 - 2 * core

    def chip_after(i):
        return lax.rem(chip_x + i // ny, nx) * ny + lax.rem(chip_y + lax.rem(i, ny), ny)

    def chip_before(i):
        return lax.rem(chip_x + nx - i // ny, nx) * ny + lax.rem(chip_y + ny - lax.rem(i, ny), ny)

    loaded = (x_ref, routes_ref, dt_ref, b_ref, c_ref, rate_ref, skip_ref, rw_ref, og_ref)
    small_copies = [
        pltpu.make_async_copy(src, dst, local_sem.at[3 + k])
        for k, (src, dst) in enumerate(zip(inputs, loaded))
    ]
    for copy in small_copies:
        copy.start()
    weight_copies = [
        pltpu.make_async_copy(src, dst, local_sem.at[k])
        for k, (src, dst) in enumerate(((wd_hbm, wd), (wg_hbm, wg), (wu_hbm, wu)))
    ]
    for copy in weight_copies:
        copy.start()

    barrier = pltpu.get_barrier_semaphore()

    def greet(axis, me, size):
        def step(k, carry):
            pl.semaphore_signal(
                barrier, inc=1, device_id={axis: lax.rem(me + k, size)}, device_id_type=MESH
            )
            return carry

        lax.fori_loop(1, size, step, 0)

    greet("dp", me_d, nd)
    greet("expert", me_e, ne)

    def on_dp(dst, k):
        return Exchange("dp", me_d, nd, None, dst, sem_x.at[k])

    def on_expert(dst, k, src=None):
        return Exchange("expert", me_e, ne, src, dst, sem_x.at[k])

    ex_ar1, ex_ar2, ex_ar3, ex_ar4 = (on_dp(r, k) for k, r in enumerate((ar1, ar2, ar3, ar4)))
    ex_dec, ex_tot, ex_rout = (on_expert(r, 4 + k) for k, r in enumerate((dec, tot, rout)))
    ex_og = on_expert(og_in, 7, og_out)
    ex_xs = on_expert(xs_in, 8, xs_out)
    ex_sq = on_expert(sq_in, 9, sq_out)
    ex_sb = on_expert(sb_in, 10, sb_out)
    ex_bk = [on_expert(bk_in.at[k], 11 + k, bk_out.at[k]) for k in range(2)]
    ex_st, ex_dl, ex_sg = (
        Chain("expert", me_e, ne, r, sem_e.at[k], k < 2) for k, r in enumerate((st, dl, sg))
    )

    for copy in small_copies:
        copy.wait()

    def to_blocks(ref, value):
        for e in range(ne):
            ref[e] = value[e * pad : (e + 1) * pad].astype(BF16)

    def from_blocks(ref):
        return jnp.concatenate([ref[e].astype(F32) for e in range(ne)], axis=0).astype(BF16)

    x_t = x_ref[...].astype(F32).T
    ar1[me_d] = jnp.sum(x_t * x_t, axis=0, keepdims=True)
    row_id, col_id = iota((t_n, t_n), 0), iota((t_n, t_n), 1)
    causal = row_id <= col_id
    step_size = jnp.maximum(dt_ref[...], 0.0) + jnp.log1p(jnp.exp(-jnp.abs(dt_ref[...])))
    cum = mm(step_size, causal.astype(F32), NN, HIGH)
    head_lane = iota((1, f_n), 1) < hp
    head_row = iota((f_n, t_n), 0) < hp
    last = [jnp.sum(step_size[h : h + 1], axis=1, keepdims=True) for h in range(heads)]
    fade = [jnp.exp(-rate_ref[h] * last[h]) for h in range(heads)]
    dec[me_e] = jnp.concatenate(
        [
            jnp.where(head_lane, fade[0], fade[1]),
            jnp.where(head_lane, -last[0] * fade[0], -last[1] * fade[1]),
        ],
        axis=0,
    )

    expert_row = iota((ne, t_n), 0)
    hot_a = (expert_row == routes_ref[0:1, :]).astype(F32)
    hot_b = (expert_row == routes_ref[1:2, :]).astype(F32)
    before = mm((hot_a + hot_b).astype(BF16), (row_id < col_id).astype(BF16))
    spread_rows = (iota((spots, ne), 0) // pad == iota((spots, ne), 1)).astype(BF16)
    slot_of = iota((spots, t_n), 0) % pad
    fits = slot_of < cap
    here = (mm(spread_rows, before.astype(BF16)) == slot_of.astype(F32)) & fits
    pick_a = jnp.where(here, mm(spread_rows, hot_a.astype(BF16)), 0.0)
    pick_b = jnp.where(here, mm(spread_rows, hot_b.astype(BF16)), 0.0)
    pick = (pick_a + pick_b).astype(BF16)
    og = og_ref[...]
    to_blocks(og_out, mm(pick, og))
    og_in[me_e] = og_out[me_e]

    pl.semaphore_wait(barrier, nd + ne - 2)
    ex_ar1.start()
    ex_og.start()
    ex_dec.start()

    b_rows, c_rows = b_ref[...], c_ref[...]
    pairing = mm(b_rows.T, c_rows, NN, HIGH)
    fades, tails = [], []
    for h in range(heads):
        cum_h, dt_h = cum[h : h + 1], step_size[h : h + 1]
        gap = jnp.where(causal, cum_h - jnp.broadcast_to(cum_h, (t_n, t_n)).T, 0.0)
        spread[h] = gap
        mt[h] = (
            jnp.where(causal, jnp.exp(-rate_ref[h] * gap), 0.0)
            * pairing
            * jnp.broadcast_to(dt_h, (t_n, t_n)).T
        )
        fades.append(jnp.exp(-rate_ref[h] * cum_h))
        tails.append(jnp.exp(-rate_ref[h] * (last[h] - cum_h)) * dt_h)
    tail = jnp.where(head_row, tails[0], tails[1])
    reach = jnp.where(head_row, cum[0:1] - last[0], cum[1:2] - last[1])
    skip_f = jnp.where(head_row, skip_ref[0], skip_ref[1])
    hot_gap = hot_a - hot_b
    rw_gap = mm(rw_ref[...].T, hot_gap, NN, HIGH)
    spot_q = iota((rows, spots), 1)
    compact = (
        ((spot_q // pad) * cap + spot_q % pad == iota((rows, spots), 0)) & (spot_q % pad < cap)
    ).astype(BF16)
    of_block_r, of_block_b = iota((rows, ne), 0), iota((rows, ne), 1) * cap
    of_block = ((of_block_r >= of_block_b) & (of_block_r < of_block_b + cap)).astype(F32)
    lane_r = iota((rows, 128), 0)
    slot_r = lane_r - (lane_r * ((1 << 20) // cap + 1) >> 20) * cap
    lane_first = iota((rows, 128), 1) == slot_r
    lane_second = iota((rows, 128), 1) == slot_r + 64

    ex_ar1.wait()
    scale_one = lax.rsqrt(jnp.sum(ar1[...], axis=0) / d_all + EPSILON)
    normed = x_t * scale_one
    st[me_e] = mm(b_rows, normed * tail, NT, HIGH)
    ex_st.start()
    dl[me_e] = mm(b_rows, normed * tail * reach, NT, HIGH)
    mixed = jnp.concatenate(
        [mm(normed[h * hp : (h + 1) * hp], mt[h], NN, HIGH) for h in range(heads)], axis=0
    )
    mixed = mixed + skip_f * normed

    def ag_begin(buf, k):
        def step(i, carry):
            peer = chip_after(i) * 2 + core
            remote(
                buf.at[me_d], buf.at[me_d], ag_sem.at[k, 0, i], ag_sem.at[k, 1, i], "dp", peer
            ).start()
            return carry

        remote(
            buf.at[me_d], buf.at[me_d], ag_sem.at[k, 2, 0], ag_sem.at[k, 3, 0], "dp", partner
        ).start()
        lax.fori_loop(1, chips, step, 0)

    def ag_forward(buf, k, i):
        spot = buf.at[chip_before(i) * 2 + core]
        remote(
            spot, spot, ag_sem.at[k, 0, i], ag_sem.at[k, 1, i], "dp", chip_before(i) * 2 + core
        ).wait_recv()
        remote(spot, spot, ag_sem.at[k, 2, i], ag_sem.at[k, 3, i], "dp", partner).start()

    def ag_partner(buf, k, i):
        spot = buf.at[chip_before(i) * 2 + 1 - core]
        remote(spot, spot, ag_sem.at[k, 2, i], ag_sem.at[k, 3, i], "dp", partner).wait_recv()

    def ag_drain(buf, k):
        def step(i, carry):
            remote(
                buf.at[me_d], buf.at[me_d], ag_sem.at[k, 0, i], ag_sem.at[k, 1, i], "dp", chip_after(i) * 2 + core
            ).wait_send()
            spot = buf.at[chip_before(i) * 2 + core]
            remote(spot, spot, ag_sem.at[k, 2, i], ag_sem.at[k, 3, i], "dp", partner).wait_send()
            return carry

        remote(
            buf.at[me_d], buf.at[me_d], ag_sem.at[k, 2, 0], ag_sem.at[k, 3, 0], "dp", partner
        ).wait_send()
        lax.fori_loop(1, chips, step, 0)

    def ag_forwards(buf, k, low, high):
        def step(i, carry):
            ag_forward(buf, k, i)
            return carry

        lax.fori_loop(low, high, step, 0)

    def ag_partners(buf, k, low, high):
        def step(i, carry):
            ag_partner(buf, k, i)
            return carry

        lax.fori_loop(low, high, step, 0)

    def ag_chips(buf, low, high):
        places = [chip_before(i) for i in range(low, high)]
        rows_of = jnp.concatenate([buf[2 * j + c] for j in places for c in range(2)], axis=1)
        return [pl.ds(pl.multiple_of(j * 2 * f_n, 2 * f_n), 2 * f_n) for j in places], rows_of

    ex_og.wait()
    rows_g[me_d] = mm(compact, from_blocks(og_in)).astype(BF16)

    ex_dec.wait()

    def carry_state(j, state):
        ex_st.wait_for(j)
        return dec[j][0:1] * state + st[j]

    state_in = lax.fori_loop(0, me_e, carry_state, jnp.zeros((n_state, f_n), F32))
    state_col = state_in.T
    from_state = jnp.concatenate(
        [mm(state_col[h * hp : (h + 1) * hp], c_rows * fades[h], NN, HIGH) for h in range(heads)],
        axis=0,
    )
    resid_t = (x_t + (mixed + from_state)).astype(BF16).astype(F32)
    resid = resid_t.T.astype(BF16)
    ar2[me_d] = jnp.concatenate(
        [
            jnp.sum(resid_t * resid_t, axis=0, keepdims=True),
            jnp.sum(resid_t * rw_gap, axis=0, keepdims=True),
        ],
        axis=0,
    )
    ex_ar2.start()
    to_blocks(xs_out, mm(pick, resid))
    xs_in[me_e] = xs_out[me_e]
    ex_xs.start()

    ag_begin(rows_g, 0)
    ex_dl.start()
    ex_ar2.wait()
    sums = jnp.sum(ar2[...], axis=0)
    scale_two = lax.rsqrt(sums[0:1] / d_all + EPSILON)
    gap_raw = sums[1:2]
    logit_gap = scale_two * gap_raw
    first_w = 1.0 / (1.0 + jnp.exp(-logit_gap))
    second_w = 1.0 / (1.0 + jnp.exp(logit_gap))
    scale_col = jnp.sum((pick_a + pick_b) * scale_two, axis=1, keepdims=True)
    weight_col = jnp.sum(pick_a * first_w + pick_b * second_w, axis=1, keepdims=True)
    lane_q = iota((spots, 128), 1)
    slot_q = iota((spots, 128), 0) % pad
    lined = jnp.where(lane_q == slot_q, scale_col, 0.0) + jnp.where(
        lane_q == slot_q + 64, weight_col, 0.0
    )
    lined = jnp.sum(lined.reshape(ne, pad, 128), axis=1)
    for e in range(ne):
        sq_out[e] = lined[e : e + 1]
    sq_in[me_e] = sq_out[me_e]
    ex_sq.start()

    ex_xs.wait()
    rows_u[me_d] = mm(compact, from_blocks(xs_in)).astype(BF16)
    ag_begin(rows_u, 1)
    ag_forwards(rows_g, 0, 1, chips)
    weight_copies[0].wait()
    ex_sq.wait()

    def by_row(ref):
        table = jnp.concatenate([ref[b] for b in range(ne)], axis=0)
        return mm(of_block, table, NN, HIGH)

    wide = by_row(sq_in)
    cols[0] = jnp.sum(jnp.where(lane_first, wide, 0.0), axis=1, keepdims=True)
    cols[1] = jnp.sum(jnp.where(lane_second, wide, 0.0), axis=1, keepdims=True)
    ag_partners(rows_g, 0, 0, chips)
    vacc[...] = mm(jnp.concatenate([rows_g[d] for d in range(nd)], axis=1), wd[...], NT)
    weight_copies[1].wait()
    weight_copies[2].wait()
    half = chips // 2
    more = min(chips, half + 2)
    ag_forwards(rows_u, 1, 1, more)
    ag_partners(rows_u, 1, 0, half)
    spans, both = ag_chips(rows_u, 0, half)
    gacc[...] = mm(both, jnp.concatenate([wg[:, span] for span in spans], axis=1), NT)
    uacc[...] = mm(both, jnp.concatenate([wu[:, span] for span in spans], axis=1), NT)
    ag_forwards(rows_u, 1, more, chips)
    ag_partners(rows_u, 1, half, chips)
    spans, both = ag_chips(rows_u, half, chips)
    gacc[...] += mm(both, jnp.concatenate([wg[:, span] for span in spans], axis=1), NT)
    uacc[...] += mm(both, jnp.concatenate([wu[:, span] for span in spans], axis=1), NT)
    part = rows // 5

    def units(k, carry):
        span = pl.ds(pl.multiple_of(k * part, part), part)
        scale, weight = cols[0, span], cols[1, span]
        gate_in, up_in, grad_in = gacc[span], uacc[span], vacc[span]
        gate, up, grad = gate_in * scale, up_in * scale, grad_in * weight
        sigma = 1.0 / (1.0 + jnp.exp(-gate))
        silu = gate * sigma
        hidden = silu * up
        gate_back = grad * up * sigma * (1.0 + gate * (1.0 - sigma))
        up_back = grad * silu
        hid[span] = hidden.astype(BF16)
        gb[span] = gate_back.astype(BF16)
        ub[span] = up_back.astype(BF16)
        gs[span] = gate_back * scale
        us[span] = up_back * scale
        hs[span] = hidden * weight
        pair_sum = jnp.sum(hidden * grad_in, axis=1, keepdims=True)
        inner_sum = jnp.sum(gate_back * gate_in + up_back * up_in, axis=1, keepdims=True)
        lane = iota((part, 128), 1)
        row_r = iota((part, 128), 0) + k * part
        slot = row_r - (row_r * ((1 << 20) // cap + 1) >> 20) * cap
        zrow[span] = jnp.where(lane == slot, pair_sum, 0.0) + jnp.where(
            lane == slot + 64, inner_sum, 0.0
        )
        return carry

    lax.fori_loop(0, 5, units, 0)
    block_t_b, block_t_r = iota((ne, rows), 0) * cap, iota((ne, rows), 1)
    of_block_t = ((block_t_r >= block_t_b) & (block_t_r < block_t_b + cap)).astype(F32)
    ar3[me_d] = mm(of_block_t, zrow[...], NN, HIGH)
    ex_ar3.start()

    def pair_copy(k, j):
        return remote(
            pair_out.at[k, j], pair_in.at[k, j], pair_sem.at[k, 0, j], pair_sem.at[k, 1, j], "dp", partner
        )

    def rs_copy(k, i):
        return remote(
            rs_out.at[k, i], rs_in.at[k, i], rs_sem.at[k, 0, i], rs_sem.at[k, 1, i], "dp", chip_after(i) * 2 + core
        )

    def rs_terms(k, n, terms):
        j = chip_after(lax.rem(n + 1, chips))
        both = terms(pl.ds(pl.multiple_of(j * 2 * f_n, 2 * f_n), 2 * f_n))
        low, high = both[:, :f_n], both[:, f_n:]
        first = core == 0
        keep[k, j] = jnp.where(first, low, high)
        pair_out[k, j] = jnp.where(first, high, low).astype(BF16)
        pair_copy(k, j).start()

    def rs_send(m):
        k, i = m // chips, lax.rem(m + 1, chips)
        j = chip_after(i)
        remote(
            pair_in.at[k, j], pair_in.at[k, j], pair_sem.at[k, 0, j], pair_sem.at[k, 1, j], "dp", partner
        ).wait_recv()
        rs_out[k, i] = (keep[k, j] + pair_in[k, j].astype(F32)).astype(BF16)

        @pl.when(i > 0)
        def _():
            rs_copy(k, i).start()

    lag = 3

    def rs_step(n, carry):
        @pl.when(n < chips)
        def _():
            rs_terms(0, n, lambda span: mm(hid[...], wd[:, span]))

        @pl.when((n >= chips) & (n < 2 * chips))
        def _():
            rs_terms(
                1, n - chips, lambda span: mm(gb[...], wg[:, span]) + mm(ub[...], wu[:, span])
            )

        @pl.when(n >= lag)
        def _():
            rs_send(n - lag)

        return carry

    lax.fori_loop(0, 2 * chips + lag, rs_step, 0)

    ex_ar3.wait()
    line = jnp.sum(ar3[...], axis=0)
    for b in range(ne):
        sb_out[b] = line[b : b + 1]
    sb_in[me_e] = sb_out[me_e]
    ex_sb.start()

    for src, dst in ((gs, gst), (us, ust), (hs, hst)):
        dst[...] = src[...].T.astype(BF16)

    def weight_grads(j, carry):
        span = pl.ds(pl.multiple_of(j * 2 * f_n, 2 * f_n), 2 * f_n)
        both_u = jnp.concatenate([rows_u[2 * j], rows_u[2 * j + 1]], axis=1)
        both_g = jnp.concatenate([rows_g[2 * j], rows_g[2 * j + 1]], axis=1)
        gate_ref[:, span] = mm(gst[...], both_u).astype(BF16)
        up_ref[:, span] = mm(ust[...], both_u).astype(BF16)
        down_ref[:, span] = mm(hst[...], both_g).astype(BF16)
        return carry

    lax.fori_loop(0, chips, weight_grads, 0)

    def rs_finish(k):
        def step(i, total):
            remote(
                rs_in.at[k, i], rs_in.at[k, i], rs_sem.at[k, 0, i], rs_sem.at[k, 1, i], "dp", chip_before(i) * 2 + core
            ).wait_recv()
            return total + rs_in[k, i].astype(F32)

        total = lax.fori_loop(1, chips, step, rs_out[k, 0].astype(F32))
        wide_rows = lax.dot_general(
            compact, total.astype(BF16), (((0,), (0,)), ((), ())), preferred_element_type=F32
        )
        to_blocks(bk_out.at[k], wide_rows)
        bk_in[k, me_e] = bk_out[k, me_e]
        ex_bk[k].start()

    rs_finish(0)

    rs_finish(1)
    ex_sb.wait()
    table = jnp.concatenate([sb_in[e] for e in range(ne)], axis=0)
    by_spot = mm(spread_rows.astype(F32), table, NN, HIGH)
    pair_spot = jnp.sum(jnp.where(lane_q == slot_q, by_spot, 0.0), axis=1, keepdims=True)
    inner_spot = jnp.sum(jnp.where(lane_q == slot_q + 64, by_spot, 0.0), axis=1, keepdims=True)
    back_gap = jnp.sum((pick_a - pick_b) * pair_spot, axis=0, keepdims=True)
    inner_two = jnp.sum((pick_a + pick_b) * inner_spot, axis=0, keepdims=True)
    gap_grad = first_w * second_w * back_gap
    inner_two = inner_two + gap_grad * gap_raw
    rout[me_e] = mm(hot_gap * (gap_grad * scale_two), resid_t, NT, HIGH)
    ex_rout.start()

    pick_at, pick_bt = pick_a.T.astype(BF16), pick_b.T.astype(BF16)
    resid_base = og.astype(F32).T + scale_two * (gap_grad * rw_gap) - resid_t * (
        scale_two * scale_two * scale_two * inner_two / d_all
    )
    first_m = jnp.broadcast_to(first_w, (f_n, t_n)).T
    second_m = jnp.broadcast_to(second_w, (f_n, t_n)).T

    def carry_slope(j, both):
        state, slope = both
        ex_dl.wait_for(j)
        here_dec = dec[j]
        return (
            here_dec[0:1] * state + st[j],
            here_dec[0:1] * slope + here_dec[1:2] * state + dl[j],
        )

    zero_state = jnp.zeros((n_state, f_n), F32)
    slope_in = lax.fori_loop(0, me_e, carry_slope, (zero_state, zero_state))[1]

    for ex in (ex_ar1, ex_ar2, ex_ar3, ex_dec, ex_og, ex_xs, ex_sq):
        ex.drain()
    ex_st.drain()
    ex_dl.drain()
    ag_drain(rows_g, 0)
    ag_drain(rows_u, 1)
    for k in range(2):
        def step(i, carry, k=k):
            pair_copy(k, i).wait_send()

            @pl.when(i > 0)
            def _():
                rs_copy(k, i).wait_send()

            return carry

        lax.fori_loop(0, chips, step, 0)

    ex_bk[0].wait()
    came = from_blocks(bk_in.at[0])
    block_ref[...] = (
        resid.astype(F32) + (first_m * mm(pick_at, came) + second_m * mm(pick_bt, came))
    ).astype(BF16)

    ex_bk[1].wait()
    moe_grad = mm(pick_at + pick_bt, from_blocks(bk_in.at[1])).T
    grad = resid_base + scale_two * moe_grad
    state_grads = [mm(c_rows * fades[h], grad, NT, HIGH) for h in range(heads)]
    state_grad = jnp.where(head_lane, state_grads[0], state_grads[1])
    sg[me_e] = state_grad
    ex_sg.start()

    normed_rows = normed.T
    cum_f = jnp.where(head_row, cum[0:1], cum[1:2])
    rate_row = jnp.sum(state_grad * slope_in, axis=0, keepdims=True)
    state_part = grad * from_state * cum_f
    skip_part = grad * normed
    lane_s = iota((1, 128), 1)
    small = jnp.zeros((1, 128), F32)
    for h in range(heads):
        mine = head_row if h == 0 else jnp.logical_not(head_row)
        mine_lane = head_lane if h == 0 else jnp.logical_not(head_lane)
        pair_grad = mm(normed_rows, jnp.where(mine, grad, 0.0), NN, HIGH)
        table_part = pair_grad * mt[h] * spread[h]
        rows_h = slice(h * hp, (h + 1) * hp)
        rate_h = (
            jnp.sum(jnp.where(mine_lane, rate_row, 0.0), axis=1, keepdims=True)
            - jnp.sum(jnp.sum(table_part, axis=0, keepdims=True), axis=1, keepdims=True)
            - jnp.sum(jnp.sum(state_part[rows_h], axis=0, keepdims=True), axis=1, keepdims=True)
        )
        skip_h = jnp.sum(jnp.sum(skip_part[rows_h], axis=0, keepdims=True), axis=1, keepdims=True)
        small = small + jnp.where(lane_s == h, rate_h, 0.0)
        small = small + jnp.where(lane_s == heads + h, skip_h, 0.0)
    tot[me_e] = small
    ex_tot.start()
    normed_grad = jnp.concatenate(
        [mm(grad[h * hp : (h + 1) * hp], mt[h], NT, HIGH) for h in range(heads)], axis=0
    )
    normed_grad = normed_grad + skip_f * grad

    def carry_grad(n, later):
        j = ne - 1 - n
        ex_sg.wait_for(j)
        return dec[j][0:1] * later + sg[j]

    later = lax.fori_loop(0, ne - 1 - me_e, carry_grad, zero_state)
    normed_grad = normed_grad + tail * mm(later.T, b_rows, NN, HIGH)
    ar4[me_d] = jnp.sum(normed_grad * x_t, axis=0, keepdims=True)
    ex_ar4.start()
    ex_rout.wait()
    router_ref[...] = jnp.sum(rout[...], axis=0)
    ex_ar4.wait()
    inner_one = jnp.sum(ar4[...], axis=0)
    token_grad = (
        grad + scale_one * normed_grad - x_t * (scale_one * scale_one * scale_one * inner_one / d_all)
    )
    token_ref[...] = token_grad.T.astype(BF16)
    ex_tot.wait()
    small_ref[...] = jnp.sum(tot[...], axis=0)

    for ex in (ex_ar4, ex_tot, ex_rout, ex_sb, *ex_bk):
        ex.drain()
    ex_sg.drain()


def flush_kernel(*refs):
    made, small_ref, outs, sem = refs[:6], refs[6], refs[7:13], refs[15]
    copies = [pltpu.make_async_copy(a, b, sem.at[k]) for k, (a, b) in enumerate(zip(made, outs))]
    for copy in copies:
        copy.start()
    rate_ref, skip_ref = refs[13], refs[14]
    heads = rate_ref.shape[0]
    rate_ref[...] = small_ref[0, 0:heads]
    skip_ref[...] = small_ref[0, heads : 2 * heads]
    for copy in copies:
        copy.wait()


def body(
    tokens,
    routes,
    dt_raw,
    b_proj,
    c_proj,
    decay_rate,
    skip_gain,
    router_weight,
    gate_weight,
    up_weight,
    down_weight,
    out_grad,
):
    nd, ne = lax.axis_size("dp"), lax.axis_size("expert")
    t_n, f_n = tokens.shape
    heads, n_state = dt_raw.shape[1], b_proj.shape[1]
    d_all = nd * f_n
    units = down_weight.shape[1]
    cap, pad = CAPACITY, SLOT_PAD
    rows, chips = ne * cap, nd // 2
    vmem, hbm, anywhere = (
        pl.BlockSpec(memory_space=space) for space in (pltpu.VMEM, pltpu.HBM, pl.ANY)
    )
    def v(*s):
        return pltpu.VMEM(s, F32)

    def h(*s):
        return pltpu.VMEM(s, BF16)

    def shape(s, t):
        return jax.ShapeDtypeStruct(s, t)
    scratch = [
        h(t_n, f_n),
        pltpu.VMEM((2, t_n), jnp.int32),
        v(heads, t_n),
        v(n_state, t_n),
        v(n_state, t_n),
        pltpu.SMEM((heads,), F32),
        pltpu.SMEM((heads,), F32),
        v(ne, f_n),
        h(t_n, f_n),
        h(units, d_all),
        h(units, d_all),
        h(units, d_all),
        h(nd, rows, f_n),
        h(nd, rows, f_n),
        v(rows, units),
        v(rows, units),
        v(rows, units),
        h(rows, units),
        h(rows, units),
        h(rows, units),
        v(rows, units),
        v(rows, units),
        v(rows, units),
        h(units, rows),
        h(units, rows),
        h(units, rows),
        v(2, rows, 1),
        v(rows, 128),
        v(2, chips, rows, f_n),
        h(2, chips, rows, f_n),
        h(2, chips, rows, f_n),
        h(2, chips, rows, f_n),
        h(2, chips, rows, f_n),
        v(nd, 1, t_n),
        v(nd, 2, t_n),
        v(nd, ne, 128),
        v(nd, 1, t_n),
        v(ne, 2, f_n),
        v(ne, n_state, f_n),
        v(ne, n_state, f_n),
        v(ne, n_state, f_n),
        v(ne, 1, 128),
        v(ne, ne, f_n),
        h(ne, pad, f_n),
        h(ne, pad, f_n),
        h(ne, pad, f_n),
        h(ne, pad, f_n),
        v(ne, 1, 128),
        v(ne, 1, 128),
        v(ne, 1, 128),
        v(ne, 1, 128),
        h(2, ne, pad, f_n),
        h(2, ne, pad, f_n),
        v(heads, t_n, t_n),
        v(heads, t_n, t_n),
        pltpu.SemaphoreType.DMA((12,)),
        pltpu.SemaphoreType.DMA((2, 4, chips)),
        pltpu.SemaphoreType.DMA((2, 2, chips)),
        pltpu.SemaphoreType.DMA((2, 2, chips)),
        pltpu.SemaphoreType.DMA((13, 2)),
        pltpu.SemaphoreType.DMA((3, 2, ne)),
    ]
    grad_shape = h(units, d_all)
    token_shape = h(t_n, f_n)
    made = pl.pallas_call(
        functools.partial(block_kernel, (nd, ne, t_n, f_n, d_all, cap)),
        out_shape=[
            token_shape,
            token_shape,
            v(ne, f_n),
            v(1, 128),
            grad_shape,
            grad_shape,
            grad_shape,
        ],
        in_specs=[hbm] * 12,
        out_specs=[vmem] * 7,
        scratch_shapes=scratch,
        compiler_params=pltpu.CompilerParams(
            collective_id=0, has_side_effects=True, vmem_limit_bytes=61400000
        ),
        name="block",
    )(
        tokens,
        routes.T,
        dt_raw.T,
        b_proj.T,
        c_proj.T,
        decay_rate,
        skip_gain,
        router_weight.T,
        out_grad,
        gate_weight[0].T,
        up_weight[0].T,
        down_weight[0],
    )
    block_out, token_grad, router_grad, small, gate_grad, up_grad, down_grad = made
    outs = (gate_grad, up_grad, down_grad, block_out, token_grad, router_grad)
    gate_grad, up_grad, down_grad, block_out, token_grad, router_grad, rate_grad, skip_grad = pl.pallas_call(
        flush_kernel,
        out_shape=[shape(a.shape, a.dtype) for a in outs] + [shape((heads,), F32)] * 2,
        in_specs=[anywhere] * 6 + [vmem],
        out_specs=[hbm] * 6 + [vmem] * 2,
        scratch_shapes=[pltpu.SemaphoreType.DMA((6,))],
        compiler_params=pltpu.CompilerParams(vmem_limit_bytes=4 * 1024 * 1024),
        name="flush",
    )(*outs, small)
    return (
        block_out,
        token_grad,
        gate_grad.T[None],
        up_grad.T[None],
        down_grad[None],
        router_grad.T,
        rate_grad,
        skip_grad,
    )


def solution(mesh):
    return jax.shard_map(
        body,
        mesh=mesh,
        in_specs=(
            P("expert", "dp"),
            P("expert", None),
            P("expert", "dp"),
            P("expert", None),
            P("expert", None),
            P("dp"),
            P("dp"),
            P("dp", None),
            P("expert", None, "dp"),
            P("expert", None, "dp"),
            P("expert", "dp", None),
            P("expert", "dp"),
        ),
        out_specs=(
            P("expert", "dp"),
            P("expert", "dp"),
            P("expert", None, "dp"),
            P("expert", None, "dp"),
            P("expert", "dp", None),
            P("dp", None),
            P("dp"),
            P("dp"),
        ),
        check_vma=False,
    )
```

```python
import functools

import jax
import jax.numpy as jnp
from jax import lax
from jax.experimental import pallas as pl
from jax.experimental.pallas import tpu as pltpu
from jax.sharding import PartitionSpec as P

EPSILON = 1e-06
CAPACITY = 20
SLOT_PAD = 24
HIGH = lax.Precision.HIGHEST
F32 = jnp.float32
BF16 = jnp.bfloat16
MESH = pl.DeviceIdType.MESH
NN = (((1,), (0,)), ((), ()))
NT = (((1,), (1,)), ((), ()))


def mm(a, b, dims=NN, precision=None):
    return lax.dot_general(a, b, dims, precision=precision, preferred_element_type=F32)


def iota(shape, dim):
    return lax.broadcasted_iota(jnp.int32, shape, dim)


def remote(src, dst, send_sem, recv_sem, axis, peer):
    return pltpu.make_async_remote_copy(
        src_ref=src,
        dst_ref=dst,
        send_sem=send_sem,
        recv_sem=recv_sem,
        device_id={axis: peer},
        device_id_type=MESH,
    )


def far_first(size):
    ring = min(8, size)
    order = sorted(range(ring), key=lambda k: -min(k, ring - k))
    return [base + k for base in range(size - ring, -1, -ring) for k in order if base + k]


class Exchange:
    def __init__(self, axis, me, size, src, dst, sems, width=None):
        self.axis, self.me, self.size = axis, me, size
        self.src, self.dst, self.sems, self.width = src, dst, sems, width

    def part(self, ref, spot):
        if self.width is None:
            return ref.at[spot]
        return ref.at[spot, pl.ds(0, self.width)]

    def copy(self, peer):
        src = self.part(self.dst, self.me) if self.src is None else self.part(self.src, peer)
        return remote(
            src, self.part(self.dst, self.me), self.sems.at[0], self.sems.at[1], self.axis, peer
        )

    def start(self):
        for k in far_first(self.size):
            self.copy(lax.rem(self.me + k, self.size)).start()

    def all_blocks(self):
        span = self.part(self.dst, pl.ds(0, self.size - 1))
        peer = lax.rem(self.me + 1, self.size)
        return remote(span, span, self.sems.at[0], self.sems.at[1], self.axis, peer)

    def wait(self):
        self.all_blocks().wait_recv()

    def drain(self):
        self.all_blocks().wait_send()


class Chain:
    def __init__(self, axis, me, size, dst, sems, later):
        self.axis, self.me, self.size, self.dst, self.sems = axis, me, size, dst, sems
        self.later = later

    def copy(self, peer):
        spot = self.dst.at[self.me]
        return remote(spot, spot, self.sems.at[0, peer], self.sems.at[1, self.me], self.axis, peer)

    def each(self, act):
        low, high = (self.me + 1, self.size) if self.later else (0, self.me)

        def step(p, carry):
            act(self.copy(p))
            return carry

        lax.fori_loop(low, high, step, 0)

    def start(self):
        self.each(lambda copy: copy.start())

    def drain(self):
        self.each(lambda copy: copy.wait_send())

    def wait_for(self, peer):
        spot = self.dst.at[peer]
        remote(spot, spot, self.sems.at[0, peer], self.sems.at[1, peer], self.axis, peer).wait_recv()


def block_kernel(
    dims,
    *refs,
):
    inputs, outputs, rest = refs[:12], refs[12:19], refs[19:]
    loaded, scratch = rest[:9], rest[9:]
    block_phases(dims, inputs, *loaded, *inputs[9:], *outputs, *scratch)


def block_phases(
    dims,
    inputs,
    x_ref,
    routes_ref,
    dt_ref,
    b_ref,
    c_ref,
    rate_ref,
    skip_ref,
    rw_ref,
    og_ref,
    wg_hbm,
    wu_hbm,
    wd_hbm,
    block_ref,
    token_ref,
    router_ref,
    small_ref,
    gate_ref,
    up_ref,
    down_ref,
    wg,
    wu,
    wd,
    rows_u,
    rows_g,
    gacc,
    uacc,
    vacc,
    hid,
    gb,
    ub,
    gs,
    us,
    hs,
    gst,
    ust,
    hst,
    cols,
    zrow,
    keep,
    pair_out,
    pair_in,
    rs_out,
    rs_in,
    cross,
    ar1,
    ar2,
    ar3,
    ar4,
    dec,
    st,
    dl,
    sg,
    tot,
    rout,
    og_out,
    og_in,
    xs_out,
    xs_in,
    sq_out,
    sq_in,
    sb_out,
    sb_in,
    bk_out,
    bk_in,
    mt,
    spread,
    local_sem,
    ag_sem,
    pair_sem,
    rs_sem,
    sem_x,
    sem_e,
):
    nd, ne, t_n, f_n, d_all, cap = dims
    pad = SLOT_PAD
    heads = dt_ref.shape[0]
    hp = f_n // heads
    n_state = b_ref.shape[0]
    rows = ne * cap
    spots = ne * pad
    chips = nd // 2
    ny = chips // 2
    nx = chips // ny
    me_d = lax.axis_index("dp")
    me_e = lax.axis_index("expert")
    core = lax.rem(me_d, 2)
    chip = me_d // 2
    chip_x, chip_y = chip // ny, lax.rem(chip, ny)
    partner = me_d + 1 - 2 * core

    def chip_after(i):
        return lax.rem(chip_x + i // ny, nx) * ny + lax.rem(chip_y + lax.rem(i, ny), ny)

    def chip_before(i):
        return lax.rem(chip_x + nx - i // ny, nx) * ny + lax.rem(chip_y + ny - lax.rem(i, ny), ny)

    barrier = pltpu.get_barrier_semaphore()

    def greet(axis, me, size):
        for k in far_first(size):
            pl.semaphore_signal(
                barrier, inc=1, device_id={axis: lax.rem(me + k, size)}, device_id_type=MESH
            )

    greet("expert", me_e, ne)
    greet("dp", me_d, nd)

    loaded = (x_ref, routes_ref, dt_ref, b_ref, c_ref, rate_ref, skip_ref, rw_ref, og_ref)
    small_copies = [
        pltpu.make_async_copy(src, dst, local_sem.at[3 + k])
        for k, (src, dst) in enumerate(zip(inputs, loaded))
    ]
    for copy in small_copies:
        copy.start()
    weight_copies = [
        pltpu.make_async_copy(src, dst, local_sem.at[k])
        for k, (src, dst) in enumerate(((wd_hbm, wd), (wg_hbm, wg), (wu_hbm, wu)))
    ]
    for copy in weight_copies:
        copy.start()

    def on_dp(dst, k):
        return Exchange("dp", me_d, nd, None, dst, sem_x.at[k])

    def on_expert(dst, k, src=None):
        return Exchange("expert", me_e, ne, src, dst, sem_x.at[k])

    ex_ar1, ex_ar2, ex_ar3, ex_ar4 = (on_dp(r, k) for k, r in enumerate((ar1, ar2, ar3, ar4)))
    ex_dec, ex_tot, ex_rout = (on_expert(r, 4 + k) for k, r in enumerate((dec, tot, rout)))
    ex_og = on_expert(og_in, 7, og_out)
    ex_xs = on_expert(xs_in, 8, xs_out)
    ex_sq = on_expert(sq_in, 9, sq_out)
    ex_sb = on_expert(sb_in, 10, sb_out)
    ex_bk = [on_expert(bk_in.at[k], 11 + k, bk_out.at[k]) for k in range(2)]
    ex_st, ex_dl, ex_sg = (
        Chain("expert", me_e, ne, r, sem_e.at[k], k < 2) for k, r in enumerate((st, dl, sg))
    )

    for copy in small_copies:
        copy.wait()

    def to_blocks(ref, value):
        for e in range(ne):
            ref[e] = value[e * pad : (e + 1) * pad].astype(BF16)

    def from_blocks(ref):
        return jnp.concatenate([ref[e].astype(F32) for e in range(ne)], axis=0).astype(BF16)

    x_t = x_ref[...].astype(F32).T
    ar1[me_d] = jnp.sum(x_t * x_t, axis=0, keepdims=True)
    row_id, col_id = iota((t_n, t_n), 0), iota((t_n, t_n), 1)
    causal = row_id <= col_id
    step_size = jnp.maximum(dt_ref[...], 0.0) + jnp.log1p(jnp.exp(-jnp.abs(dt_ref[...])))
    cum = mm(step_size, causal.astype(F32), NN, HIGH)
    head_lane = iota((1, f_n), 1) < hp
    head_row = iota((f_n, t_n), 0) < hp
    last = [jnp.sum(step_size[h : h + 1], axis=1, keepdims=True) for h in range(heads)]
    fade = [jnp.exp(-rate_ref[h] * last[h]) for h in range(heads)]
    dec[me_e] = jnp.concatenate(
        [
            jnp.where(head_lane, fade[0], fade[1]),
            jnp.where(head_lane, -last[0] * fade[0], -last[1] * fade[1]),
        ],
        axis=0,
    )

    expert_row = iota((ne, t_n), 0)
    hot_a = (expert_row == routes_ref[0:1, :]).astype(F32)
    hot_b = (expert_row == routes_ref[1:2, :]).astype(F32)
    before = mm((hot_a + hot_b).astype(BF16), (row_id < col_id).astype(BF16))
    spread_rows = (iota((spots, ne), 0) // pad == iota((spots, ne), 1)).astype(BF16)
    slot_of = iota((spots, t_n), 0) % pad
    fits = slot_of < cap
    here = (mm(spread_rows, before.astype(BF16)) == slot_of.astype(F32)) & fits
    pick_a = jnp.where(here, mm(spread_rows, hot_a.astype(BF16)), 0.0)
    pick_b = jnp.where(here, mm(spread_rows, hot_b.astype(BF16)), 0.0)
    pick = (pick_a + pick_b).astype(BF16)
    og = og_ref[...]
    to_blocks(og_out, mm(pick, og))
    og_in[me_e] = og_out[me_e]

    pl.semaphore_wait(barrier, nd + ne - 2)
    ex_ar1.start()
    ex_og.start()
    ex_dec.start()

    b_rows, c_rows = b_ref[...], c_ref[...]
    pairing = mm(b_rows.T, c_rows, NN, HIGH)
    fades, tails = [], []
    for h in range(heads):
        cum_h, dt_h = cum[h : h + 1], step_size[h : h + 1]
        gap = jnp.where(causal, cum_h - jnp.broadcast_to(cum_h, (t_n, t_n)).T, 0.0)
        spread[h] = gap
        mt[h] = (
            jnp.where(causal, jnp.exp(-rate_ref[h] * gap), 0.0)
            * pairing
            * jnp.broadcast_to(dt_h, (t_n, t_n)).T
        )
        fades.append(jnp.exp(-rate_ref[h] * cum_h))
        tails.append(jnp.exp(-rate_ref[h] * (last[h] - cum_h)) * dt_h)
    tail = jnp.where(head_row, tails[0], tails[1])
    reach = jnp.where(head_row, cum[0:1] - last[0], cum[1:2] - last[1])
    skip_f = jnp.where(head_row, skip_ref[0], skip_ref[1])
    hot_gap = hot_a - hot_b
    rw_gap = mm(rw_ref[...].T, hot_gap, NN, HIGH)
    spot_q = iota((rows, spots), 1)
    compact = (
        ((spot_q // pad) * cap + spot_q % pad == iota((rows, spots), 0)) & (spot_q % pad < cap)
    ).astype(BF16)
    of_block_r, of_block_b = iota((rows, ne), 0), iota((rows, ne), 1) * cap
    of_block = ((of_block_r >= of_block_b) & (of_block_r < of_block_b + cap)).astype(F32)
    lane_r = iota((rows, 128), 0)
    slot_r = lane_r - (lane_r * ((1 << 20) // cap + 1) >> 20) * cap
    lane_first = iota((rows, 128), 1) == slot_r
    lane_second = iota((rows, 128), 1) == slot_r + 64

    ex_ar1.wait()
    scale_one = lax.rsqrt(jnp.sum(ar1[...], axis=0) / d_all + EPSILON)
    normed = x_t * scale_one
    st[me_e] = mm(b_rows, normed * tail, NT, HIGH).astype(BF16)
    ex_st.start()
    dl[me_e] = mm(b_rows, normed * tail * reach, NT, HIGH).astype(BF16)
    mixed = jnp.concatenate(
        [mm(normed[h * hp : (h + 1) * hp], mt[h], NN, HIGH) for h in range(heads)], axis=0
    )
    mixed = mixed + skip_f * normed

    def ag_send(buf, k, i, spot, peer):
        piece = buf.at[spot]
        remote(piece, piece, ag_sem.at[k, 0, i], ag_sem.at[k, 1, i], "dp", peer * 2 + core).start()

    def ag_begin(buf, k):
        for i in (2, ny, 1, 3):
            ag_send(buf, k, i, me_d, chip_after(i))
        remote(
            buf.at[me_d], buf.at[me_d], ag_sem.at[k, 2, 0], ag_sem.at[k, 3, 0], "dp", partner
        ).start()

    def ag_relay(buf, k):
        spot = ag_arrived(buf, k, ny)
        for i in (1, 3):
            ag_send(buf, k, ny + i, spot, chip_after(i))
        ag_pass(buf, k, ny)
        spot = ag_arrived(buf, k, 2)
        ag_send(buf, k, ny + 2, spot, chip_after(ny))
        ag_pass(buf, k, 2)

    def ag_arrived(buf, k, i):
        spot = chip_before(i) * 2 + core
        remote(
            buf.at[spot], buf.at[spot], ag_sem.at[k, 0, i], ag_sem.at[k, 1, i], "dp", chip_before(i) * 2 + core
        ).wait_recv()
        return spot

    def ag_pass(buf, k, i):
        spot = buf.at[chip_before(i) * 2 + core]
        remote(spot, spot, ag_sem.at[k, 2, i], ag_sem.at[k, 3, i], "dp", partner).start()

    def ag_forward(buf, k, i):
        ag_arrived(buf, k, i)
        ag_pass(buf, k, i)

    def ag_partner(buf, k, i):
        spot = buf.at[chip_before(i) * 2 + 1 - core]
        remote(spot, spot, ag_sem.at[k, 2, i], ag_sem.at[k, 3, i], "dp", partner).wait_recv()

    def ag_drain(buf, k):
        def step(i, carry):
            remote(
                buf.at[me_d], buf.at[me_d], ag_sem.at[k, 0, i], ag_sem.at[k, 1, i], "dp", chip_after(i) * 2 + core
            ).wait_send()
            spot = buf.at[chip_before(i) * 2 + core]
            remote(spot, spot, ag_sem.at[k, 2, i], ag_sem.at[k, 3, i], "dp", partner).wait_send()
            return carry

        remote(
            buf.at[me_d], buf.at[me_d], ag_sem.at[k, 2, 0], ag_sem.at[k, 3, 0], "dp", partner
        ).wait_send()
        lax.fori_loop(1, chips, step, 0)

    def ag_forwards(buf, k, turns):
        for i in turns:
            ag_forward(buf, k, i)

    def ag_partners(buf, k, turns):
        for i in turns:
            ag_partner(buf, k, i)

    def ag_chips(buf, turns):
        places = [chip_before(i) for i in turns]
        rows_of = jnp.concatenate([buf[2 * j + c] for j in places for c in range(2)], axis=1)
        return [pl.ds(pl.multiple_of(j * 2 * f_n, 2 * f_n), 2 * f_n) for j in places], rows_of

    def take_rows(turns, first):
        ag_partners(rows_u, 1, turns)
        spans, both = ag_chips(rows_u, turns)
        for acc, weight in ((gacc, wg), (uacc, wu)):
            part = mm(both, jnp.concatenate([weight[:, span] for span in spans], axis=1), NT)
            acc[...] = part if first else acc[...] + part

    ex_og.wait()
    rows_g[me_d] = mm(compact, from_blocks(og_in)).astype(BF16)
    ag_begin(rows_g, 0)

    ex_dec.wait()
    ag_relay(rows_g, 0)

    def carry_state(j, state):
        ex_st.wait_for(j)
        return dec[j][0:1] * state + st[j].astype(F32)

    state_in = lax.fori_loop(0, me_e, carry_state, jnp.zeros((n_state, f_n), F32))
    state_col = state_in.T
    from_state = jnp.concatenate(
        [mm(state_col[h * hp : (h + 1) * hp], c_rows * fades[h], NN, HIGH) for h in range(heads)],
        axis=0,
    )
    resid_t = (x_t + (mixed + from_state)).astype(BF16).astype(F32)
    resid = resid_t.T.astype(BF16)
    to_blocks(xs_out, mm(pick, resid))
    xs_in[me_e] = xs_out[me_e]
    ex_xs.start()
    ar2[me_d] = jnp.concatenate(
        [
            jnp.sum(resid_t * resid_t, axis=0, keepdims=True),
            jnp.sum(resid_t * rw_gap, axis=0, keepdims=True),
        ],
        axis=0,
    )
    ex_ar2.start()
    ag_forwards(rows_g, 0, (1, 3, 5, 7, 6))

    ex_ar2.wait()
    sums = jnp.sum(ar2[...], axis=0)
    scale_two = lax.rsqrt(sums[0:1] / d_all + EPSILON)
    gap_raw = sums[1:2]
    logit_gap = scale_two * gap_raw
    first_w = 1.0 / (1.0 + jnp.exp(-logit_gap))
    second_w = 1.0 / (1.0 + jnp.exp(logit_gap))
    scale_col = jnp.sum((pick_a + pick_b) * scale_two, axis=1, keepdims=True)
    weight_col = jnp.sum(pick_a * first_w + pick_b * second_w, axis=1, keepdims=True)
    lane_q = iota((spots, 128), 1)
    slot_q = iota((spots, 128), 0) % pad
    lined = jnp.where(lane_q == slot_q, scale_col, 0.0) + jnp.where(
        lane_q == slot_q + 64, weight_col, 0.0
    )
    lined = jnp.sum(lined.reshape(ne, pad, 128), axis=1)
    for e in range(ne):
        sq_out[e] = lined[e : e + 1]
    sq_in[me_e] = sq_out[me_e]
    ex_sq.start()

    ex_xs.wait()
    rows_u[me_d] = mm(compact, from_blocks(xs_in)).astype(BF16)
    ag_begin(rows_u, 1)
    weight_copies[0].wait()
    ag_partners(rows_g, 0, range(chips))
    vacc[...] = mm(jnp.concatenate([rows_g[d] for d in range(nd)], axis=1), wd[...], NT)
    weight_copies[1].wait()
    weight_copies[2].wait()
    ex_dl.start()
    ag_relay(rows_u, 1)
    ag_forwards(rows_u, 1, (1, 3))
    take_rows((0, 1, 2, 3), True)
    ex_sq.wait()

    def by_row(ref):
        table = jnp.concatenate([ref[b] for b in range(ne)], axis=0)
        return mm(of_block, table, NN, HIGH)

    wide = by_row(sq_in)
    cols[0] = jnp.sum(jnp.where(lane_first, wide, 0.0), axis=1, keepdims=True)
    cols[1] = jnp.sum(jnp.where(lane_second, wide, 0.0), axis=1, keepdims=True)
    ag_forwards(rows_u, 1, (5, 7, 6))
    take_rows((4, 5, 7), False)
    take_rows((6,), False)
    part = rows // 5

    def units(k, carry):
        span = pl.ds(pl.multiple_of(k * part, part), part)
        scale, weight = cols[0, span], cols[1, span]
        gate_in, up_in, grad_in = gacc[span], uacc[span], vacc[span]
        gate, up, grad = gate_in * scale, up_in * scale, grad_in * weight
        sigma = 0.5 + 0.5 * jnp.tanh(0.5 * gate)
        silu = gate * sigma
        hidden = silu * up
        gate_back = grad * up * sigma * (1.0 + gate * (1.0 - sigma))
        up_back = grad * silu
        hid[span] = hidden.astype(BF16)
        gb[span] = gate_back.astype(BF16)
        ub[span] = up_back.astype(BF16)
        gs[span] = gate_back * scale
        us[span] = up_back * scale
        hs[span] = hidden * weight
        pair_sum = jnp.sum(hidden * grad_in, axis=1, keepdims=True)
        inner_sum = jnp.sum(gate_back * gate_in + up_back * up_in, axis=1, keepdims=True)
        lane = iota((part, 128), 1)
        row_r = iota((part, 128), 0) + k * part
        slot = row_r - (row_r * ((1 << 20) // cap + 1) >> 20) * cap
        zrow[span] = jnp.where(lane == slot, pair_sum, 0.0) + jnp.where(
            lane == slot + 64, inner_sum, 0.0
        )
        return carry

    lax.fori_loop(0, rows // part, units, 0)
    block_t_b, block_t_r = iota((ne, rows), 0) * cap, iota((ne, rows), 1)
    of_block_t = ((block_t_r >= block_t_b) & (block_t_r < block_t_b + cap)).astype(F32)
    ar3[me_d] = mm(of_block_t, zrow[...], NN, HIGH)
    ex_ar3.start()

    def pair_copy(k, j):
        return remote(
            pair_out.at[k, j], pair_in.at[k, j], pair_sem.at[k, 0, j], pair_sem.at[k, 1, j], "dp", partner
        )

    def rs_copy(k, i):
        return remote(
            rs_out.at[k, i], rs_in.at[k, i], rs_sem.at[k, 0, i], rs_sem.at[k, 1, i], "dp", chip_after(lax.rem(i, ny)) * 2 + core
        )

    def rs_arrival(k, i):
        spot = rs_in.at[k, i]
        return remote(spot, spot, rs_sem.at[k, 0, i], rs_sem.at[k, 1, i], "dp", partner)

    def rs_side_copy(k):
        return remote(
            rs_out.at[k, ny + 2], rs_in.at[k, ny + 2], rs_sem.at[k, 0, ny + 2], rs_sem.at[k, 1, ny + 2], "dp", chip_after(ny) * 2 + core
        )

    def rs_far(k):
        rs_arrival(k, ny + 2).wait_recv()
        rs_out[k, 2] = (rs_out[k, 2].astype(F32) + rs_in[k, ny + 2].astype(F32)).astype(BF16)
        rs_copy(k, 2).start()

    def rs_cross(k):
        return remote(
            cross.at[k], rs_in.at[k, ny], rs_sem.at[k, 0, ny], rs_sem.at[k, 1, ny], "dp", chip_after(ny) * 2 + core
        )

    def rs_total(k, first, turns):
        total = rs_out[k, first].astype(F32)
        for i in turns:
            rs_arrival(k, i).wait_recv()
            total = total + rs_in[k, i].astype(F32)
        return total

    def rs_relay(k):
        cross[k] = rs_total(k, ny, (ny + 3, ny + 1)).astype(BF16)
        rs_cross(k).start()

    def rs_index(n):
        return (1 - n // ny) * ny + lax.rem(n + 2 + n // ny, ny)

    def rs_terms(k, n, terms):
        j = chip_after(rs_index(n))
        both = terms(pl.ds(pl.multiple_of(j * 2 * f_n, 2 * f_n), 2 * f_n))
        low, high = both[:, :f_n], both[:, f_n:]
        first = core == 0
        keep[k, j] = jnp.where(first, low, high)
        pair_out[k, j] = jnp.where(first, high, low).astype(BF16)
        pair_copy(k, j).start()

    def rs_join(k, n):
        i = rs_index(n)
        j = chip_after(i)
        remote(
            pair_in.at[k, j], pair_in.at[k, j], pair_sem.at[k, 0, j], pair_sem.at[k, 1, j], "dp", partner
        ).wait_recv()
        rs_out[k, i] = (keep[k, j] + pair_in[k, j].astype(F32)).astype(BF16)
        return i

    def rs_send(k, i):
        @pl.when(lax.rem(i, 2) == 1)
        def _():
            rs_copy(k, i).start()

        @pl.when(i == ny + 2)
        def _():
            rs_side_copy(k).start()

    lag = 3

    def side_step(n, carry):
        @pl.when(n < chips)
        def _():
            rs_terms(1, n, lambda span: mm(gb[...], wg[:, span]) + mm(ub[...], wu[:, span]))

        @pl.when(n >= lag)
        def _():
            rs_send(1, rs_join(1, n - lag))

        return carry

    lax.fori_loop(0, chips + lag, side_step, 0)

    def down_step(n, carry):
        @pl.when(n < chips)
        def _():
            rs_terms(0, n, lambda span: mm(hid[...], wd[:, span]))

        @pl.when(n >= lag)
        def _():
            rs_join(0, n - lag)

        return carry

    lax.fori_loop(0, ny, down_step, 0)
    rs_far(1)
    rs_relay(1)
    lax.fori_loop(ny, chips + lag, down_step, 0)

    ex_ar3.wait()
    line = jnp.sum(ar3[...], axis=0)
    for b in range(ne):
        sb_out[b] = line[b : b + 1]
    sb_in[me_e] = sb_out[me_e]
    ex_sb.start()

    for src, dst in ((gs, gst), (us, ust), (hs, hst)):
        dst[...] = src[...].T.astype(BF16)
    def down_sends(n, carry):
        rs_send(0, rs_index(n))
        return carry

    lax.fori_loop(0, chips, down_sends, 0)

    def weight_grads(j, carry):
        span = pl.ds(pl.multiple_of(j * 2 * f_n, 2 * f_n), 2 * f_n)
        both_u = jnp.concatenate([rows_u[2 * j], rows_u[2 * j + 1]], axis=1)
        both_g = jnp.concatenate([rows_g[2 * j], rows_g[2 * j + 1]], axis=1)
        gate_ref[:, span] = mm(gst[...], both_u).astype(BF16)
        up_ref[:, span] = mm(ust[...], both_u).astype(BF16)
        down_ref[:, span] = mm(hst[...], both_g).astype(BF16)
        return carry

    early = chips - 3
    lax.fori_loop(0, early, weight_grads, 0)

    def rs_finish(k):
        total = rs_total(k, 0, (3, 1, 4, 2))
        wide_rows = lax.dot_general(
            compact, total.astype(BF16), (((0,), (0,)), ((), ())), preferred_element_type=F32
        )
        to_blocks(bk_out.at[k], wide_rows)
        bk_in[k, me_e] = bk_out[k, me_e]
        ex_bk[k].start()

    rs_finish(1)
    rs_far(0)

    lax.fori_loop(early, chips, weight_grads, 0)
    ex_sb.wait()
    table = jnp.concatenate([sb_in[e] for e in range(ne)], axis=0)
    by_spot = mm(spread_rows.astype(F32), table, NN, HIGH)
    pair_spot = jnp.sum(jnp.where(lane_q == slot_q, by_spot, 0.0), axis=1, keepdims=True)
    inner_spot = jnp.sum(jnp.where(lane_q == slot_q + 64, by_spot, 0.0), axis=1, keepdims=True)
    back_gap = jnp.sum((pick_a - pick_b) * pair_spot, axis=0, keepdims=True)
    inner_two = jnp.sum((pick_a + pick_b) * inner_spot, axis=0, keepdims=True)
    gap_grad = first_w * second_w * back_gap
    inner_two = inner_two + gap_grad * gap_raw
    rout[me_e] = mm(hot_gap * (gap_grad * scale_two), resid_t, NT, HIGH)
    ex_rout.start()

    pick_at, pick_bt = pick_a.T.astype(BF16), pick_b.T.astype(BF16)
    resid_base = og.astype(F32).T + scale_two * (gap_grad * rw_gap) - resid_t * (
        scale_two * scale_two * scale_two * inner_two / d_all
    )
    first_m = jnp.broadcast_to(first_w, (f_n, t_n)).T
    second_m = jnp.broadcast_to(second_w, (f_n, t_n)).T

    def carry_slope(j, both):
        state, slope = both
        ex_dl.wait_for(j)
        here_dec = dec[j]
        return (
            here_dec[0:1] * state + st[j].astype(F32),
            here_dec[0:1] * slope + here_dec[1:2] * state + dl[j].astype(F32),
        )

    zero_state = jnp.zeros((n_state, f_n), F32)
    slope_in = lax.fori_loop(0, me_e, carry_slope, (zero_state, zero_state))[1]

    rs_relay(0)
    ex_bk[1].wait()
    moe_grad = mm(pick_at + pick_bt, from_blocks(bk_in.at[1])).T
    grad = resid_base + scale_two * moe_grad
    state_grads = [mm(c_rows * fades[h], grad, NT, HIGH) for h in range(heads)]
    state_grad = jnp.where(head_lane, state_grads[0], state_grads[1])
    sg[me_e] = state_grad.astype(BF16)
    ex_sg.start()

    normed_rows = normed.T
    cum_f = jnp.where(head_row, cum[0:1], cum[1:2])
    rate_row = jnp.sum(state_grad * slope_in, axis=0, keepdims=True)
    state_part = grad * from_state * cum_f
    skip_part = grad * normed
    lane_s = iota((1, 128), 1)
    small = jnp.zeros((1, 128), F32)
    for h in range(heads):
        mine = head_row if h == 0 else jnp.logical_not(head_row)
        mine_lane = head_lane if h == 0 else jnp.logical_not(head_lane)
        pair_grad = mm(normed_rows, jnp.where(mine, grad, 0.0), NN, HIGH)
        table_part = pair_grad * mt[h] * spread[h]
        rows_h = slice(h * hp, (h + 1) * hp)
        rate_h = (
            jnp.sum(jnp.where(mine_lane, rate_row, 0.0), axis=1, keepdims=True)
            - jnp.sum(jnp.sum(table_part, axis=0, keepdims=True), axis=1, keepdims=True)
            - jnp.sum(jnp.sum(state_part[rows_h], axis=0, keepdims=True), axis=1, keepdims=True)
        )
        skip_h = jnp.sum(jnp.sum(skip_part[rows_h], axis=0, keepdims=True), axis=1, keepdims=True)
        small = small + jnp.where(lane_s == h, rate_h, 0.0)
        small = small + jnp.where(lane_s == heads + h, skip_h, 0.0)
    tot[me_e] = small
    ex_tot.start()
    normed_grad = jnp.concatenate(
        [mm(grad[h * hp : (h + 1) * hp], mt[h], NT, HIGH) for h in range(heads)], axis=0
    )
    normed_grad = normed_grad + skip_f * grad

    rs_finish(0)
    for ex in (ex_ar1, ex_ar2, ex_ar3, ex_dec, ex_og, ex_xs, ex_sq):
        ex.drain()
    ex_st.drain()
    ex_dl.drain()
    ag_drain(rows_g, 0)
    ag_drain(rows_u, 1)
    for k in range(2):
        def step(i, carry, k=k):
            pair_copy(k, i).wait_send()

            @pl.when((lax.rem(i, 2) == 1) | (i == 2))
            def _():
                rs_copy(k, i).wait_send()

            return carry

        lax.fori_loop(0, chips, step, 0)
        rs_cross(k).wait_send()
        rs_side_copy(k).wait_send()

    def carry_grad(n, later):
        j = ne - 1 - n
        ex_sg.wait_for(j)
        return dec[j][0:1] * later + sg[j].astype(F32)

    later = lax.fori_loop(0, ne - 1 - me_e, carry_grad, zero_state)
    normed_grad = normed_grad + tail * mm(later.T, b_rows, NN, HIGH)
    ar4[me_d] = jnp.sum(normed_grad * x_t, axis=0, keepdims=True)
    ex_ar4.start()
    ex_rout.wait()
    router_ref[...] = jnp.sum(rout[...], axis=0)
    ex_bk[0].wait()
    came = from_blocks(bk_in.at[0])
    block_ref[...] = (
        resid.astype(F32) + (first_m * mm(pick_at, came) + second_m * mm(pick_bt, came))
    ).astype(BF16)

    ex_ar4.wait()
    inner_one = jnp.sum(ar4[...], axis=0)
    token_grad = (
        grad + scale_one * normed_grad - x_t * (scale_one * scale_one * scale_one * inner_one / d_all)
    )
    token_ref[...] = token_grad.T.astype(BF16)
    ex_tot.wait()
    small_ref[...] = jnp.sum(tot[...], axis=0)

    for ex in (ex_ar4, ex_tot, ex_rout, ex_sb, *ex_bk):
        ex.drain()
    ex_sg.drain()


def flush_kernel(*refs):
    made, small_ref, outs, sem = refs[:6], refs[6], refs[7:13], refs[15]
    copies = [pltpu.make_async_copy(a, b, sem.at[k]) for k, (a, b) in enumerate(zip(made, outs))]
    for copy in copies:
        copy.start()
    rate_ref, skip_ref = refs[13], refs[14]
    heads = rate_ref.shape[0]
    rate_ref[...] = small_ref[0, 0:heads]
    skip_ref[...] = small_ref[0, heads : 2 * heads]
    for copy in copies:
        copy.wait()


def body(
    tokens,
    routes,
    dt_raw,
    b_proj,
    c_proj,
    decay_rate,
    skip_gain,
    router_weight,
    gate_weight,
    up_weight,
    down_weight,
    out_grad,
):
    nd, ne = lax.axis_size("dp"), lax.axis_size("expert")
    t_n, f_n = tokens.shape
    heads, n_state = dt_raw.shape[1], b_proj.shape[1]
    d_all = nd * f_n
    units = down_weight.shape[1]
    cap, pad = CAPACITY, SLOT_PAD
    rows, chips = ne * cap, nd // 2
    vmem, hbm, anywhere = (
        pl.BlockSpec(memory_space=space) for space in (pltpu.VMEM, pltpu.HBM, pl.ANY)
    )
    def v(*s):
        return pltpu.VMEM(s, F32)

    def h(*s):
        return pltpu.VMEM(s, BF16)

    def shape(s, t):
        return jax.ShapeDtypeStruct(s, t)
    scratch = [
        h(t_n, f_n),
        pltpu.VMEM((2, t_n), jnp.int32),
        v(heads, t_n),
        v(n_state, t_n),
        v(n_state, t_n),
        pltpu.SMEM((heads,), F32),
        pltpu.SMEM((heads,), F32),
        v(ne, f_n),
        h(t_n, f_n),
        h(units, d_all),
        h(units, d_all),
        h(units, d_all),
        h(nd, rows, f_n),
        h(nd, rows, f_n),
        v(rows, units),
        v(rows, units),
        v(rows, units),
        h(rows, units),
        h(rows, units),
        h(rows, units),
        v(rows, units),
        v(rows, units),
        v(rows, units),
        h(units, rows),
        h(units, rows),
        h(units, rows),
        v(2, rows, 1),
        v(rows, 128),
        v(2, chips, rows, f_n),
        h(2, chips, rows, f_n),
        h(2, chips, rows, f_n),
        h(2, chips, rows, f_n),
        h(2, chips, rows, f_n),
        h(2, rows, f_n),
        v(nd, 1, t_n),
        v(nd, 2, t_n),
        v(nd, ne, 128),
        v(nd, 1, t_n),
        v(ne, 2, f_n),
        h(ne, n_state, f_n),
        h(ne, n_state, f_n),
        h(ne, n_state, f_n),
        v(ne, 1, 128),
        v(ne, ne, f_n),
        h(ne, pad, f_n),
        h(ne, pad, f_n),
        h(ne, pad, f_n),
        h(ne, pad, f_n),
        v(ne, 1, 128),
        v(ne, 1, 128),
        v(ne, 1, 128),
        v(ne, 1, 128),
        h(2, ne, pad, f_n),
        h(2, ne, pad, f_n),
        v(heads, t_n, t_n),
        v(heads, t_n, t_n),
        pltpu.SemaphoreType.DMA((12,)),
        pltpu.SemaphoreType.DMA((2, 4, chips)),
        pltpu.SemaphoreType.DMA((2, 2, chips)),
        pltpu.SemaphoreType.DMA((2, 2, chips)),
        pltpu.SemaphoreType.DMA((13, 2)),
        pltpu.SemaphoreType.DMA((3, 2, ne)),
    ]
    grad_shape = h(units, d_all)
    token_shape = h(t_n, f_n)
    made = pl.pallas_call(
        functools.partial(block_kernel, (nd, ne, t_n, f_n, d_all, cap)),
        out_shape=[
            token_shape,
            token_shape,
            v(ne, f_n),
            v(1, 128),
            grad_shape,
            grad_shape,
            grad_shape,
        ],
        in_specs=[hbm] * 12,
        out_specs=[vmem] * 7,
        scratch_shapes=scratch,
        compiler_params=pltpu.CompilerParams(
            collective_id=0, has_side_effects=True, vmem_limit_bytes=61400000
        ),
        name="block",
    )(
        tokens,
        routes.T,
        dt_raw.T,
        b_proj.T,
        c_proj.T,
        decay_rate,
        skip_gain,
        router_weight.T,
        out_grad,
        gate_weight[0].T,
        up_weight[0].T,
        down_weight[0],
    )
    block_out, token_grad, router_grad, small, gate_grad, up_grad, down_grad = made
    outs = (gate_grad, up_grad, down_grad, block_out, token_grad, router_grad)
    gate_grad, up_grad, down_grad, block_out, token_grad, router_grad, rate_grad, skip_grad = pl.pallas_call(
        flush_kernel,
        out_shape=[shape(a.shape, a.dtype) for a in outs] + [shape((heads,), F32)] * 2,
        in_specs=[anywhere] * 6 + [vmem],
        out_specs=[hbm] * 6 + [vmem] * 2,
        scratch_shapes=[pltpu.SemaphoreType.DMA((6,))],
        compiler_params=pltpu.CompilerParams(vmem_limit_bytes=4 * 1024 * 1024),
        name="flush",
    )(*outs, small)
    return (
        block_out,
        token_grad,
        gate_grad.T[None],
        up_grad.T[None],
        down_grad[None],
        router_grad.T,
        rate_grad,
        skip_grad,
    )


def solution(mesh):
    return jax.shard_map(
        body,
        mesh=mesh,
        in_specs=(
            P("expert", "dp"),
            P("expert", None),
            P("expert", "dp"),
            P("expert", None),
            P("expert", None),
            P("dp"),
            P("dp"),
            P("dp", None),
            P("expert", None, "dp"),
            P("expert", None, "dp"),
            P("expert", "dp", None),
            P("expert", "dp"),
        ),
        out_specs=(
            P("expert", "dp"),
            P("expert", "dp"),
            P("expert", None, "dp"),
            P("expert", None, "dp"),
            P("expert", "dp", None),
            P("dp", None),
            P("dp"),
            P("dp"),
        ),
        check_vma=False,
    )
```

```python
import functools

import jax
import jax.numpy as jnp
from jax import lax
from jax.experimental import pallas as pl
from jax.experimental.pallas import tpu as pltpu
from jax.sharding import PartitionSpec as P

EPSILON = 1e-06
CAPACITY = 20
SLOT_PAD = 24
HIGH = lax.Precision.HIGHEST
F32 = jnp.float32
BF16 = jnp.bfloat16
MESH = pl.DeviceIdType.MESH
NN = (((1,), (0,)), ((), ()))
NT = (((1,), (1,)), ((), ()))


def mm(a, b, dims=NN, precision=None):
    return lax.dot_general(a, b, dims, precision=precision, preferred_element_type=F32)


def iota(shape, dim):
    return lax.broadcasted_iota(jnp.int32, shape, dim)


def remote(src, dst, send_sem, recv_sem, axis, peer):
    return pltpu.make_async_remote_copy(
        src_ref=src,
        dst_ref=dst,
        send_sem=send_sem,
        recv_sem=recv_sem,
        device_id={axis: peer},
        device_id_type=MESH,
    )


def far_first(size):
    ring = min(8, size)
    order = sorted(range(ring), key=lambda k: -min(k, ring - k))
    return [base + k for base in range(size - ring, -1, -ring) for k in order if base + k]


class Exchange:
    def __init__(self, axis, me, size, src, dst, sems, width=None):
        self.axis, self.me, self.size = axis, me, size
        self.src, self.dst, self.sems, self.width = src, dst, sems, width

    def part(self, ref, spot):
        if self.width is None:
            return ref.at[spot]
        return ref.at[spot, pl.ds(0, self.width)]

    def copy(self, peer):
        src = self.part(self.dst, self.me) if self.src is None else self.part(self.src, peer)
        return remote(
            src, self.part(self.dst, self.me), self.sems.at[0], self.sems.at[1], self.axis, peer
        )

    def start(self):
        for k in far_first(self.size):
            self.copy(lax.rem(self.me + k, self.size)).start()

    def all_blocks(self):
        span = self.part(self.dst, pl.ds(0, self.size - 1))
        peer = lax.rem(self.me + 1, self.size)
        return remote(span, span, self.sems.at[0], self.sems.at[1], self.axis, peer)

    def wait(self):
        self.all_blocks().wait_recv()

    def drain(self):
        self.all_blocks().wait_send()


class Chain:
    def __init__(self, axis, me, size, dst, sems, later):
        self.axis, self.me, self.size, self.dst, self.sems = axis, me, size, dst, sems
        self.later = later

    def copy(self, peer):
        spot = self.dst.at[self.me]
        return remote(spot, spot, self.sems.at[0, peer], self.sems.at[1, self.me], self.axis, peer)

    def each(self, act):
        low, high = (self.me + 1, self.size) if self.later else (0, self.me)

        def step(p, carry):
            act(self.copy(p))
            return carry

        lax.fori_loop(low, high, step, 0)

    def start(self):
        self.each(lambda copy: copy.start())

    def drain(self):
        self.each(lambda copy: copy.wait_send())

    def wait_for(self, peer):
        spot = self.dst.at[peer]
        remote(spot, spot, self.sems.at[0, peer], self.sems.at[1, peer], self.axis, peer).wait_recv()


def block_kernel(
    dims,
    *refs,
):
    inputs, outputs, rest = refs[:12], refs[12:19], refs[19:]
    loaded, scratch = rest[:9], rest[9:]
    block_phases(dims, inputs, *loaded, *inputs[9:], *outputs, *scratch)


def block_phases(
    dims,
    inputs,
    x_ref,
    routes_ref,
    dt_ref,
    b_ref,
    c_ref,
    rate_ref,
    skip_ref,
    rw_ref,
    og_ref,
    wg_hbm,
    wu_hbm,
    wd_hbm,
    block_ref,
    token_ref,
    router_ref,
    small_ref,
    gate_ref,
    up_ref,
    down_ref,
    wg,
    wu,
    wd,
    rows_u,
    rows_g,
    gacc,
    uacc,
    vacc,
    hid,
    gb,
    ub,
    gs,
    us,
    hs,
    gst,
    ust,
    hst,
    cols,
    zrow,
    keep,
    pair_out,
    pair_in,
    rs_out,
    rs_in,
    cross,
    ar1,
    ar2,
    ar3,
    ar4,
    dec,
    st,
    dl,
    sg,
    tot,
    rout,
    og_out,
    og_in,
    xs_out,
    xs_in,
    sq_out,
    sq_in,
    sb_out,
    sb_in,
    bk_out,
    bk_in,
    mt,
    spread,
    gate_made,
    up_made,
    down_made,
    cf_out,
    cf_in,
    diag,
    lo_out,
    lo_in,
    local_sem,
    ag_sem,
    pair_sem,
    rs_sem,
    sem_x,
    sem_e,
):
    nd, ne, t_n, f_n, d_all, cap = dims
    pad = SLOT_PAD
    heads = dt_ref.shape[0]
    hp = f_n // heads
    n_state = b_ref.shape[0]
    rows = ne * cap
    spots = ne * pad
    chips = nd // 2
    ny = chips // 2
    nx = chips // ny
    me_d = lax.axis_index("dp")
    me_e = lax.axis_index("expert")
    core = lax.rem(me_d, 2)
    chip = me_d // 2
    chip_x, chip_y = chip // ny, lax.rem(chip, ny)
    partner = me_d + 1 - 2 * core

    def chip_after(i):
        return lax.rem(chip_x + i // ny, nx) * ny + lax.rem(chip_y + lax.rem(i, ny), ny)

    def chip_before(i):
        return lax.rem(chip_x + nx - i // ny, nx) * ny + lax.rem(chip_y + ny - lax.rem(i, ny), ny)

    barrier = pltpu.get_barrier_semaphore()

    def greet(axis, me, size):
        for k in far_first(size):
            pl.semaphore_signal(
                barrier, inc=1, device_id={axis: lax.rem(me + k, size)}, device_id_type=MESH
            )

    greet("expert", me_e, ne)
    greet("dp", me_d, nd)

    loaded = (x_ref, routes_ref, dt_ref, b_ref, c_ref, rate_ref, skip_ref, rw_ref, og_ref)
    small_copies = [
        pltpu.make_async_copy(src, dst, local_sem.at[3 + k])
        for k, (src, dst) in enumerate(zip(inputs, loaded))
    ]
    for copy in small_copies:
        copy.start()
    weight_copies = [
        pltpu.make_async_copy(src, dst, local_sem.at[k])
        for k, (src, dst) in enumerate(((wd_hbm, wd), (wg_hbm, wg), (wu_hbm, wu)))
    ]
    for copy in weight_copies:
        copy.start()

    def on_dp(dst, k):
        return Exchange("dp", me_d, nd, None, dst, sem_x.at[k])

    def on_expert(dst, k, src=None):
        return Exchange("expert", me_e, ne, src, dst, sem_x.at[k])

    ex_ar1, ex_ar2, ex_ar3, ex_ar4 = (on_dp(r, k) for k, r in enumerate((ar1, ar2, ar3, ar4)))
    ex_dec, ex_tot, ex_rout = (on_expert(r, 4 + k) for k, r in enumerate((dec, tot, rout)))
    ex_og = on_expert(og_in, 7, og_out)
    ex_xs = on_expert(xs_in, 8, xs_out)
    ex_sq = on_expert(sq_in, 9, sq_out)
    ex_sb = on_expert(sb_in, 10, sb_out)
    ex_bk = [on_expert(bk_in.at[k], 11 + k, bk_out.at[k]) for k in range(2)]
    ex_cf = on_expert(cf_in, 13, cf_out)
    ex_lo = on_expert(lo_in, 14, lo_out)
    ex_dl = on_expert(dl, 15)
    ex_st, ex_sg = (
        Chain("expert", me_e, ne, r, sem_e, k == 0) for k, r in enumerate((st, sg))
    )

    for copy in small_copies:
        copy.wait()

    def to_blocks(ref, value):
        for e in range(ne):
            ref[e] = value[e * pad : (e + 1) * pad].astype(BF16)

    def from_blocks(ref):
        return jnp.concatenate([ref[e].astype(F32) for e in range(ne)], axis=0).astype(BF16)

    x_t = x_ref[...].astype(F32).T
    ar1[me_d] = jnp.sum(x_t * x_t, axis=0, keepdims=True)
    row_id, col_id = iota((t_n, t_n), 0), iota((t_n, t_n), 1)
    causal = row_id <= col_id
    step_size = jnp.maximum(dt_ref[...], 0.0) + jnp.log1p(jnp.exp(-jnp.abs(dt_ref[...])))
    cum = mm(step_size, causal.astype(F32), NN, HIGH)
    head_lane = iota((1, f_n), 1) < hp
    head_row = iota((f_n, t_n), 0) < hp
    last = [jnp.sum(step_size[h : h + 1], axis=1, keepdims=True) for h in range(heads)]
    fade = [jnp.exp(-rate_ref[h] * last[h]) for h in range(heads)]
    dec[me_e] = jnp.concatenate(
        [
            jnp.where(head_lane, fade[0], fade[1]),
            jnp.where(head_lane, -last[0] * fade[0], -last[1] * fade[1]),
        ],
        axis=0,
    )

    expert_row = iota((ne, t_n), 0)
    hot_a = (expert_row == routes_ref[0:1, :]).astype(F32)
    hot_b = (expert_row == routes_ref[1:2, :]).astype(F32)
    before = mm((hot_a + hot_b).astype(BF16), (row_id < col_id).astype(BF16))
    spread_rows = (iota((spots, ne), 0) // pad == iota((spots, ne), 1)).astype(BF16)
    slot_of = iota((spots, t_n), 0) % pad
    fits = slot_of < cap
    here = (mm(spread_rows, before.astype(BF16)) == slot_of.astype(F32)) & fits
    pick_a = jnp.where(here, mm(spread_rows, hot_a.astype(BF16)), 0.0)
    pick_b = jnp.where(here, mm(spread_rows, hot_b.astype(BF16)), 0.0)
    pick = (pick_a + pick_b).astype(BF16)
    og = og_ref[...]
    to_blocks(og_out, mm(pick, og))
    og_in[me_e] = og_out[me_e]

    pl.semaphore_wait(barrier, nd + ne - 2)
    ex_ar1.start()
    ex_og.start()
    ex_dec.start()

    b_rows, c_rows = b_ref[...], c_ref[...]
    pairing = mm(b_rows.T, c_rows, NN, HIGH)
    fades, tails = [], []
    for h in range(heads):
        cum_h, dt_h = cum[h : h + 1], step_size[h : h + 1]
        gap = jnp.where(causal, cum_h - jnp.broadcast_to(cum_h, (t_n, t_n)).T, 0.0)
        spread[h] = gap
        mt[h] = (
            jnp.where(causal, jnp.exp(-rate_ref[h] * gap), 0.0)
            * pairing
            * jnp.broadcast_to(dt_h, (t_n, t_n)).T
        )
        fades.append(jnp.exp(-rate_ref[h] * cum_h))
        tails.append(jnp.exp(-rate_ref[h] * (last[h] - cum_h)) * dt_h)
    tail = jnp.where(head_row, tails[0], tails[1])
    reach = jnp.where(head_row, cum[0:1] - last[0], cum[1:2] - last[1])
    skip_f = jnp.where(head_row, skip_ref[0], skip_ref[1])
    hot_gap = hot_a - hot_b
    rw_gap = mm(rw_ref[...].T, hot_gap, NN, HIGH)
    spot_q = iota((rows, spots), 1)
    compact = (
        ((spot_q // pad) * cap + spot_q % pad == iota((rows, spots), 0)) & (spot_q % pad < cap)
    ).astype(BF16)
    of_block_r, of_block_b = iota((rows, ne), 0), iota((rows, ne), 1) * cap
    of_block = ((of_block_r >= of_block_b) & (of_block_r < of_block_b + cap)).astype(F32)
    lane_r = iota((rows, 128), 0)
    slot_r = lane_r - (lane_r * ((1 << 20) // cap + 1) >> 20) * cap
    lane_first = iota((rows, 128), 1) == slot_r
    lane_second = iota((rows, 128), 1) == slot_r + 64

    ex_ar1.wait()
    scale_one = lax.rsqrt(jnp.sum(ar1[...], axis=0) / d_all + EPSILON)
    normed = x_t * scale_one
    st[me_e] = mm(b_rows, normed * tail, NT, HIGH).astype(BF16)
    ex_st.start()
    dl[me_e] = mm(b_rows, normed * tail * reach, NT, HIGH).astype(BF16)
    mixed = jnp.concatenate(
        [mm(normed[h * hp : (h + 1) * hp], mt[h], NN, HIGH) for h in range(heads)], axis=0
    )
    mixed = mixed + skip_f * normed

    def ag_group(k, i):
        return chips if k == 0 or i < ny else chips + 1 if i != ny + 2 else chips + 2

    def ag_send(buf, k, i, spot, peer):
        piece = buf.at[spot]
        remote(piece, piece, ag_sem.at[k, 0], ag_sem.at[k, i], "dp", peer * 2 + core).start()

    def ag_pass(buf, k, i):
        piece = buf.at[chip_before(i) * 2 + core]
        remote(piece, piece, ag_sem.at[k, 0], ag_sem.at[k, ag_group(k, i)], "dp", partner).start()

    def ag_begin(buf, k):
        for i in (2, ny, 1, 3):
            ag_send(buf, k, i, me_d, chip_after(i))
        ag_pass(buf, k, 0)

    def ag_arrived(buf, k, i):
        spot = chip_before(i) * 2 + core
        remote(buf.at[spot], buf.at[spot], ag_sem.at[k, 0], ag_sem.at[k, i], "dp", spot).wait_recv()
        return spot

    def ag_relay(buf, k):
        spot = ag_arrived(buf, k, ny)
        for i in (1, 3):
            ag_send(buf, k, ny + i, spot, chip_after(i))
        ag_pass(buf, k, ny)
        spot = ag_arrived(buf, k, 2)
        ag_send(buf, k, ny + 2, spot, chip_after(ny))
        ag_pass(buf, k, 2)

    def ag_forward(buf, k, i):
        ag_arrived(buf, k, i)
        ag_pass(buf, k, i)

    def ag_drain(buf, k):
        every = buf.at[pl.ds(0, 2 * chips - 1)]
        remote(every, every, ag_sem.at[k, 0], ag_sem.at[k, 1], "dp", partner).wait_send()

    def ag_forwards(buf, k, turns):
        for i in turns:
            ag_forward(buf, k, i)

    def ag_partners(buf, k, turns):
        group = buf.at[pl.ds(0, len(turns))]
        remote(group, group, ag_sem.at[k, 0], ag_sem.at[k, ag_group(k, turns[0])], "dp", partner).wait_recv()

    def ag_chips(buf, turns):
        places = [chip_before(i) for i in turns]
        rows_of = jnp.concatenate([buf[2 * j + c] for j in places for c in range(2)], axis=1)
        return [pl.ds(pl.multiple_of(j * 2 * f_n, 2 * f_n), 2 * f_n) for j in places], rows_of

    def take_rows(turns, first):
        ag_partners(rows_u, 1, turns)
        spans, both = ag_chips(rows_u, turns)
        for acc, weight in ((gacc, wg), (uacc, wu)):
            part = mm(both, jnp.concatenate([weight[:, span] for span in spans], axis=1), NT)
            acc[...] = part if first else acc[...] + part

    ex_og.wait()
    rows_g[me_d] = mm(compact, from_blocks(og_in)).astype(BF16)
    ag_begin(rows_g, 0)

    ex_dec.wait()

    def carry_state(j, state):
        ex_st.wait_for(j)
        return dec[j][0:1] * state + st[j].astype(F32)

    state_in = lax.fori_loop(0, me_e, carry_state, jnp.zeros((n_state, f_n), F32))
    state_col = state_in.T
    from_state = jnp.concatenate(
        [mm(state_col[h * hp : (h + 1) * hp], c_rows * fades[h], NN, HIGH) for h in range(heads)],
        axis=0,
    )
    resid_t = (x_t + (mixed + from_state)).astype(BF16).astype(F32)
    resid = resid_t.T.astype(BF16)
    to_blocks(xs_out, mm(pick, resid))
    xs_in[me_e] = xs_out[me_e]
    ex_xs.start()
    ar2[me_d] = jnp.concatenate(
        [
            jnp.sum(resid_t * resid_t, axis=0, keepdims=True),
            jnp.sum(resid_t * rw_gap, axis=0, keepdims=True),
        ],
        axis=0,
    )
    ex_ar2.start()
    ag_relay(rows_g, 0)
    ag_forwards(rows_g, 0, (1, 3, 5, 7, 6))

    ex_ar2.wait()
    sums = jnp.sum(ar2[...], axis=0)
    scale_two = lax.rsqrt(sums[0:1] / d_all + EPSILON)
    gap_raw = sums[1:2]
    logit_gap = scale_two * gap_raw
    first_w = 1.0 / (1.0 + jnp.exp(-logit_gap))
    second_w = 1.0 / (1.0 + jnp.exp(logit_gap))
    scale_col = jnp.sum((pick_a + pick_b) * scale_two, axis=1, keepdims=True)
    weight_col = jnp.sum(pick_a * first_w + pick_b * second_w, axis=1, keepdims=True)
    lane_q = iota((spots, 128), 1)
    slot_q = iota((spots, 128), 0) % pad
    lined = jnp.where(lane_q == slot_q, scale_col, 0.0) + jnp.where(
        lane_q == slot_q + 64, weight_col, 0.0
    )
    lined = jnp.sum(lined.reshape(ne, pad, 128), axis=1)
    for e in range(ne):
        sq_out[e] = lined[e : e + 1]
    sq_in[me_e] = sq_out[me_e]
    ex_sq.start()

    ex_xs.wait()
    rows_u[me_d] = mm(compact, from_blocks(xs_in)).astype(BF16)
    ag_begin(rows_u, 1)
    weight_copies[0].wait()
    ag_partners(rows_g, 0, range(chips))
    vacc[...] = mm(jnp.concatenate([rows_g[d] for d in range(nd)], axis=1), wd[...], NT)
    weight_copies[1].wait()
    weight_copies[2].wait()
    ex_dl.start()
    coefs = jnp.concatenate([c_rows * (fades[h] * scale_two) for h in range(heads)], axis=0)
    by_slot = mm(coefs.astype(BF16), pick, NT)
    cf_out[...] = jnp.zeros_like(cf_out)
    for e in range(ne):
        cf_out[e, :, 0:pad] = by_slot[:, e * pad : (e + 1) * pad].astype(BF16)
    cf_in[me_e] = cf_out[me_e]
    ex_cf.start()
    ag_relay(rows_u, 1)
    ag_forwards(rows_u, 1, (1, 3))
    take_rows((0, 1, 2, 3), True)
    ex_sq.wait()

    def by_row(ref):
        table = jnp.concatenate([ref[b] for b in range(ne)], axis=0)
        return mm(of_block, table, NN, HIGH)

    wide = by_row(sq_in)
    cols[0] = jnp.sum(jnp.where(lane_first, wide, 0.0), axis=1, keepdims=True)
    cols[1] = jnp.sum(jnp.where(lane_second, wide, 0.0), axis=1, keepdims=True)
    ag_forwards(rows_u, 1, (5, 7, 6))
    take_rows((4, 5, 7), False)
    take_rows((6,), False)
    part = rows // 5

    def units(k, carry):
        span = pl.ds(pl.multiple_of(k * part, part), part)
        scale, weight = cols[0, span], cols[1, span]
        gate_in, up_in, grad_in = gacc[span], uacc[span], vacc[span]
        gate, up, grad = gate_in * scale, up_in * scale, grad_in * weight
        sigma = 0.5 + 0.5 * jnp.tanh(0.5 * gate)
        silu = gate * sigma
        hidden = silu * up
        gate_back = grad * up * sigma * (1.0 + gate * (1.0 - sigma))
        up_back = grad * silu
        hid[span] = hidden.astype(BF16)
        gb[span] = gate_back.astype(BF16)
        ub[span] = up_back.astype(BF16)
        gs[span] = gate_back * scale
        us[span] = up_back * scale
        hs[span] = hidden * weight
        pair_sum = jnp.sum(hidden * grad_in, axis=1, keepdims=True)
        inner_sum = jnp.sum(gate_back * gate_in + up_back * up_in, axis=1, keepdims=True)
        lane = iota((part, 128), 1)
        row_r = iota((part, 128), 0) + k * part
        slot = row_r - (row_r * ((1 << 20) // cap + 1) >> 20) * cap
        zrow[span] = jnp.where(lane == slot, pair_sum, 0.0) + jnp.where(
            lane == slot + 64, inner_sum, 0.0
        )
        return carry

    lax.fori_loop(0, rows // part, units, 0)
    block_t_b, block_t_r = iota((ne, rows), 0) * cap, iota((ne, rows), 1)
    of_block_t = ((block_t_r >= block_t_b) & (block_t_r < block_t_b + cap)).astype(F32)
    ar3[me_d] = mm(of_block_t, zrow[...], NN, HIGH)
    ex_ar3.start()

    def pair_copy(k, j):
        return remote(
            pair_out.at[k, j], pair_in.at[k, j], pair_sem.at[k, 0], pair_sem.at[k, 1 + j], "dp", partner
        )

    def rs_move(k, src, i, group, peer):
        return remote(
            src, rs_in.at[k, i], rs_sem.at[k, 0], rs_sem.at[k, group], "dp", peer * 2 + core
        )

    def rs_wait(k, group, blocks):
        span = rs_in.at[k, pl.ds(0, blocks)]
        remote(span, span, rs_sem.at[k, 0], rs_sem.at[k, group], "dp", partner).wait_recv()

    def rs_far(k):
        rs_wait(k, 2, 1)
        rs_out[k, 2] = (rs_out[k, 2].astype(F32) + rs_in[k, ny + 2].astype(F32)).astype(BF16)
        rs_move(k, rs_out.at[k, 2], 2, 3, chip_after(2)).start()

    def rs_total(k, first, turns):
        total = rs_out[k, first].astype(F32)
        for i in turns:
            total = total + rs_in[k, i].astype(F32)
        return total

    def rs_relay(k):
        rs_wait(k, 1, 2)
        cross[k] = rs_total(k, ny, (ny + 3, ny + 1)).astype(BF16)
        rs_move(k, cross.at[k], ny, 3, chip_after(ny)).start()

    def rs_drain(k):
        span = pair_out.at[k]
        remote(span, span, pair_sem.at[k, 0], pair_sem.at[k, 1], "dp", partner).wait_send()
        span = rs_out.at[k, pl.ds(0, chips - 1)]
        remote(span, span, rs_sem.at[k, 0], rs_sem.at[k, 1], "dp", partner).wait_send()

    def rs_index(n):
        return (1 - n // ny) * ny + lax.rem(n + 2 + n // ny, ny)

    def rs_terms(k, n, terms):
        j = chip_after(rs_index(n))
        both = terms(pl.ds(pl.multiple_of(j * 2 * f_n, 2 * f_n), 2 * f_n))
        low, high = both[:, :f_n], both[:, f_n:]
        first = core == 0
        keep[k, j] = jnp.where(first, low, high)
        pair_out[k, j] = jnp.where(first, high, low).astype(BF16)
        pair_copy(k, j).start()

    def rs_join(k, n):
        i = rs_index(n)
        j = chip_after(i)
        remote(
            pair_in.at[k, j], pair_in.at[k, j], pair_sem.at[k, 0], pair_sem.at[k, 1 + j], "dp", partner
        ).wait_recv()
        rs_out[k, i] = (keep[k, j] + pair_in[k, j].astype(F32)).astype(BF16)
        return i

    def rs_send(k, i):
        @pl.when(lax.rem(i, 2) == 1)
        def _():
            rs_move(k, rs_out.at[k, i], i, 3 - i // ny * 2, chip_after(lax.rem(i, ny))).start()

        @pl.when(i == ny + 2)
        def _():
            rs_move(k, rs_out.at[k, i], i, 2, chip_after(ny)).start()

    lag = 3

    def side_step(n, carry):
        @pl.when(n < chips)
        def _():
            rs_terms(1, n, lambda span: mm(gb[...], wg[:, span]) + mm(ub[...], wu[:, span]))

        @pl.when(n >= lag)
        def _():
            rs_send(1, rs_join(1, n - lag))

        return carry

    lax.fori_loop(0, chips + lag, side_step, 0)

    ex_ar3.wait()
    line = jnp.sum(ar3[...], axis=0)
    for b in range(ne):
        sb_out[b] = line[b : b + 1]
    sb_in[me_e] = sb_out[me_e]
    ex_sb.start()

    def down_step(n, carry):
        @pl.when(n < chips)
        def _():
            rs_terms(0, n, lambda span: mm(hid[...], wd[:, span]))

        @pl.when(n >= lag)
        def _():
            rs_join(0, n - lag)

        return carry

    lax.fori_loop(0, ny, down_step, 0)
    rs_far(1)
    lax.fori_loop(ny, chips - 1, down_step, 0)
    rs_relay(1)
    lax.fori_loop(chips - 1, chips + lag, down_step, 0)

    def down_sends(n, carry):
        rs_send(0, rs_index(n))
        return carry

    lax.fori_loop(0, chips, down_sends, 0)

    ex_sb.wait()
    table = jnp.concatenate([sb_in[e] for e in range(ne)], axis=0)
    by_spot = mm(spread_rows.astype(F32), table, NN, HIGH)
    pair_spot = jnp.sum(jnp.where(lane_q == slot_q, by_spot, 0.0), axis=1, keepdims=True)
    inner_spot = jnp.sum(jnp.where(lane_q == slot_q + 64, by_spot, 0.0), axis=1, keepdims=True)
    back_gap = jnp.sum((pick_a - pick_b) * pair_spot, axis=0, keepdims=True)
    inner_two = jnp.sum((pick_a + pick_b) * inner_spot, axis=0, keepdims=True)
    gap_grad = first_w * second_w * back_gap
    inner_two = inner_two + gap_grad * gap_raw
    rout[me_e] = mm(hot_gap * (gap_grad * scale_two), resid_t, NT, HIGH)
    ex_rout.start()

    pick_at, pick_bt = pick_a.T.astype(BF16), pick_b.T.astype(BF16)
    resid_base = og.astype(F32).T + scale_two * (gap_grad * rw_gap) - resid_t * (
        scale_two * scale_two * scale_two * inner_two / d_all
    )
    first_m = jnp.broadcast_to(first_w, (f_n, t_n)).T
    second_m = jnp.broadcast_to(second_w, (f_n, t_n)).T
    base_grads = [mm(c_rows * fades[h], resid_base, NT, HIGH) for h in range(heads)]
    sg[me_e] = jnp.where(head_lane, base_grads[0], base_grads[1]).astype(BF16)
    ex_sg.start()

    ex_cf.wait()
    width = heads * n_state
    taken = jnp.concatenate([cf_in[b].astype(F32) for b in range(ne)], axis=0).astype(BF16)
    repeat = (iota((128, spots), 0) == iota((128, spots), 1) % pad).astype(BF16)
    own_block = iota((ne * width, spots), 0) // width == iota((ne * width, spots), 1) // pad
    diag[...] = jnp.where(own_block, mm(taken, repeat), 0.0).astype(BF16)
    for src, dst in ((gs, gst), (us, ust), (hs, hst)):
        dst[...] = src[...].T.astype(BF16)
    def rs_finish(k):
        rs_wait(k, 3, 4)
        total = rs_total(k, 0, (3, 1, ny, 2))
        wide_rows = lax.dot_general(
            compact, total.astype(BF16), (((0,), (0,)), ((), ())), preferred_element_type=F32
        )
        to_blocks(bk_out.at[k], wide_rows)
        bk_in[k, me_e] = bk_out[k, me_e]
        ex_bk[k].start()
        return wide_rows

    back_rows = rs_finish(1)
    shares = mm(diag[...], back_rows.astype(BF16))
    later = jnp.zeros((n_state, f_n), F32)
    lo_out[ne - 1] = later.astype(BF16)
    for b in range(ne - 1, 0, -1):
        low = shares[b * width : b * width + n_state]
        high = shares[b * width + n_state : (b + 1) * width]
        later = jnp.where(head_lane, low, high) + dec[b][0:1] * later
        lo_out[b - 1] = later.astype(BF16)
    lo_in[me_e] = lo_out[me_e]
    ex_lo.start()

    rs_far(0)

    def weight_grads(j, carry):
        span = pl.ds(pl.multiple_of(j * 2 * f_n, 2 * f_n), 2 * f_n)
        both_u = jnp.concatenate([rows_u[2 * j], rows_u[2 * j + 1]], axis=1)
        both_g = jnp.concatenate([rows_g[2 * j], rows_g[2 * j + 1]], axis=1)
        gate_made[:, span] = mm(gst[...], both_u).astype(BF16)
        up_made[:, span] = mm(ust[...], both_u).astype(BF16)
        down_made[:, span] = mm(hst[...], both_g).astype(BF16)
        return carry

    early = chips - 3
    lax.fori_loop(0, early, weight_grads, 0)
    rs_relay(0)
    lax.fori_loop(early, chips, weight_grads, 0)
    def carry_slope(j, both):
        state, slope = both
        here_dec = dec[j]
        return (
            here_dec[0:1] * state + st[j].astype(F32),
            here_dec[0:1] * slope + here_dec[1:2] * state + dl[j].astype(F32),
        )

    zero_state = jnp.zeros((n_state, f_n), F32)
    ex_dl.wait()
    slope_in = lax.fori_loop(0, me_e, carry_slope, (zero_state, zero_state))[1]

    rs_finish(0)
    ex_bk[1].wait()
    moe_grad = mm(pick_at + pick_bt, from_blocks(bk_in.at[1])).T
    grad = resid_base + scale_two * moe_grad
    state_grads = [mm(c_rows * fades[h], grad, NT, HIGH) for h in range(heads)]
    state_grad = jnp.where(head_lane, state_grads[0], state_grads[1])

    normed_rows = normed.T
    cum_f = jnp.where(head_row, cum[0:1], cum[1:2])
    rate_row = jnp.sum(state_grad * slope_in, axis=0, keepdims=True)
    state_part = grad * from_state * cum_f
    skip_part = grad * normed
    lane_s = iota((1, 128), 1)
    small = jnp.zeros((1, 128), F32)
    for h in range(heads):
        mine = head_row if h == 0 else jnp.logical_not(head_row)
        mine_lane = head_lane if h == 0 else jnp.logical_not(head_lane)
        pair_grad = mm(normed_rows, jnp.where(mine, grad, 0.0), NN, HIGH)
        table_part = pair_grad * mt[h] * spread[h]
        rows_h = slice(h * hp, (h + 1) * hp)
        rate_h = (
            jnp.sum(jnp.where(mine_lane, rate_row, 0.0), axis=1, keepdims=True)
            - jnp.sum(jnp.sum(table_part, axis=0, keepdims=True), axis=1, keepdims=True)
            - jnp.sum(jnp.sum(state_part[rows_h], axis=0, keepdims=True), axis=1, keepdims=True)
        )
        skip_h = jnp.sum(jnp.sum(skip_part[rows_h], axis=0, keepdims=True), axis=1, keepdims=True)
        small = small + jnp.where(lane_s == h, rate_h, 0.0)
        small = small + jnp.where(lane_s == heads + h, skip_h, 0.0)
    tot[me_e] = small
    ex_tot.start()
    normed_grad = jnp.concatenate(
        [mm(grad[h * hp : (h + 1) * hp], mt[h], NT, HIGH) for h in range(heads)], axis=0
    )
    normed_grad = normed_grad + skip_f * grad

    def carry_grad(n, later):
        j = ne - 1 - n
        ex_sg.wait_for(j)
        return dec[j][0:1] * later + sg[j].astype(F32)

    ex_lo.wait()
    later = lax.fori_loop(0, ne - 1 - me_e, carry_grad, zero_state)
    later = later + jnp.sum(lo_in[...].astype(F32), axis=0)
    normed_grad = normed_grad + tail * mm(later.T, b_rows, NN, HIGH)
    ar4[me_d] = jnp.sum(normed_grad * x_t, axis=0, keepdims=True)
    ex_ar4.start()
    grad_copies = [
        pltpu.make_async_copy(src, dst, local_sem.at[k])
        for k, (src, dst) in enumerate(((gate_made, gate_ref), (up_made, up_ref), (down_made, down_ref)))
    ]
    for copy in grad_copies:
        copy.start()
    for ex in (ex_ar1, ex_ar2, ex_ar3, ex_dec, ex_og, ex_xs, ex_sq):
        ex.drain()
    ex_st.drain()
    ex_dl.drain()
    ag_drain(rows_g, 0)
    ag_drain(rows_u, 1)
    for k in range(2):
        rs_drain(k)

    ex_rout.wait()
    router_ref[...] = jnp.sum(rout[...], axis=0)
    ex_bk[0].wait()
    came = from_blocks(bk_in.at[0])
    block_ref[...] = (
        resid.astype(F32) + (first_m * mm(pick_at, came) + second_m * mm(pick_bt, came))
    ).astype(BF16)

    ex_ar4.wait()
    inner_one = jnp.sum(ar4[...], axis=0)
    token_grad = (
        grad + scale_one * normed_grad - x_t * (scale_one * scale_one * scale_one * inner_one / d_all)
    )
    token_ref[...] = token_grad.T.astype(BF16)
    ex_tot.wait()
    small_ref[...] = jnp.sum(tot[...], axis=0)

    for copy in grad_copies:
        copy.wait()
    for ex in (ex_ar4, ex_tot, ex_rout, ex_sb, *ex_bk):
        ex.drain()
    ex_sg.drain()
    ex_cf.drain()
    ex_lo.drain()


def flush_kernel(*refs):
    made, small_ref, outs, sem = refs[:6], refs[6], refs[7:13], refs[15]
    copies = [pltpu.make_async_copy(a, b, sem.at[k]) for k, (a, b) in enumerate(zip(made, outs))]
    for copy in copies:
        copy.start()
    rate_ref, skip_ref = refs[13], refs[14]
    heads = rate_ref.shape[0]
    rate_ref[...] = small_ref[0, 0:heads]
    skip_ref[...] = small_ref[0, heads : 2 * heads]
    for copy in copies:
        copy.wait()


def body(
    tokens,
    routes,
    dt_raw,
    b_proj,
    c_proj,
    decay_rate,
    skip_gain,
    router_weight,
    gate_weight,
    up_weight,
    down_weight,
    out_grad,
):
    nd, ne = lax.axis_size("dp"), lax.axis_size("expert")
    t_n, f_n = tokens.shape
    heads, n_state = dt_raw.shape[1], b_proj.shape[1]
    d_all = nd * f_n
    units = down_weight.shape[1]
    cap, pad = CAPACITY, SLOT_PAD
    rows, chips = ne * cap, nd // 2
    vmem, hbm, anywhere = (
        pl.BlockSpec(memory_space=space) for space in (pltpu.VMEM, pltpu.HBM, pl.ANY)
    )
    def v(*s):
        return pltpu.VMEM(s, F32)

    def h(*s):
        return pltpu.VMEM(s, BF16)

    def shape(s, t):
        return jax.ShapeDtypeStruct(s, t)
    scratch = [
        h(t_n, f_n),
        pltpu.VMEM((2, t_n), jnp.int32),
        v(heads, t_n),
        v(n_state, t_n),
        v(n_state, t_n),
        pltpu.SMEM((heads,), F32),
        pltpu.SMEM((heads,), F32),
        v(ne, f_n),
        h(t_n, f_n),
        h(units, d_all),
        h(units, d_all),
        h(units, d_all),
        h(nd, rows, f_n),
        h(nd, rows, f_n),
        v(rows, units),
        v(rows, units),
        v(rows, units),
        h(rows, units),
        h(rows, units),
        h(rows, units),
        v(rows, units),
        v(rows, units),
        v(rows, units),
        h(units, rows),
        h(units, rows),
        h(units, rows),
        v(2, rows, 1),
        v(rows, 128),
        v(2, chips, rows, f_n),
        h(2, chips, rows, f_n),
        h(2, chips, rows, f_n),
        h(2, chips, rows, f_n),
        h(2, chips, rows, f_n),
        h(2, rows, f_n),
        v(nd, 1, t_n),
        v(nd, 2, t_n),
        v(nd, ne, 128),
        v(nd, 1, t_n),
        v(ne, 2, f_n),
        h(ne, n_state, f_n),
        h(ne, n_state, f_n),
        h(ne, n_state, f_n),
        v(ne, 1, 128),
        v(ne, ne, f_n),
        h(ne, pad, f_n),
        h(ne, pad, f_n),
        h(ne, pad, f_n),
        h(ne, pad, f_n),
        v(ne, 1, 128),
        v(ne, 1, 128),
        v(ne, 1, 128),
        v(ne, 1, 128),
        h(2, ne, pad, f_n),
        h(2, ne, pad, f_n),
        v(heads, t_n, t_n),
        v(heads, t_n, t_n),
        h(units, d_all),
        h(units, d_all),
        h(units, d_all),
        h(ne, heads * n_state, 128),
        h(ne, heads * n_state, 128),
        h(ne * heads * n_state, ne * pad),
        h(ne, n_state, f_n),
        h(ne, n_state, f_n),
        pltpu.SemaphoreType.DMA((12,)),
        pltpu.SemaphoreType.DMA((2, chips + 3)),
        pltpu.SemaphoreType.DMA((2, 1 + chips)),
        pltpu.SemaphoreType.DMA((2, 4)),
        pltpu.SemaphoreType.DMA((16, 2)),
        pltpu.SemaphoreType.DMA((2, ne)),
    ]
    grad_shape = h(units, d_all)
    token_shape = h(t_n, f_n)
    made = pl.pallas_call(
        functools.partial(block_kernel, (nd, ne, t_n, f_n, d_all, cap)),
        out_shape=[
            token_shape,
            token_shape,
            v(ne, f_n),
            v(1, 128),
            grad_shape,
            grad_shape,
            grad_shape,
        ],
        in_specs=[hbm] * 12,
        out_specs=[vmem] * 4 + [anywhere] * 3,
        scratch_shapes=scratch,
        compiler_params=pltpu.CompilerParams(
            collective_id=0, has_side_effects=True, vmem_limit_bytes=61400000
        ),
        name="block",
    )(
        tokens,
        routes.T,
        dt_raw.T,
        b_proj.T,
        c_proj.T,
        decay_rate,
        skip_gain,
        router_weight.T,
        out_grad,
        gate_weight[0].T,
        up_weight[0].T,
        down_weight[0],
    )
    block_out, token_grad, router_grad, small, gate_grad, up_grad, down_grad = made
    outs = (gate_grad, up_grad, down_grad, block_out, token_grad, router_grad)
    gate_grad, up_grad, down_grad, block_out, token_grad, router_grad, rate_grad, skip_grad = pl.pallas_call(
        flush_kernel,
        out_shape=[shape(a.shape, a.dtype) for a in outs] + [shape((heads,), F32)] * 2,
        in_specs=[anywhere] * 6 + [vmem],
        out_specs=[hbm] * 6 + [vmem] * 2,
        scratch_shapes=[pltpu.SemaphoreType.DMA((6,))],
        compiler_params=pltpu.CompilerParams(vmem_limit_bytes=4 * 1024 * 1024),
        name="flush",
    )(*outs, small)
    return (
        block_out,
        token_grad,
        gate_grad.T[None],
        up_grad.T[None],
        down_grad[None],
        router_grad.T,
        rate_grad,
        skip_grad,
    )


def solution(mesh):
    return jax.shard_map(
        body,
        mesh=mesh,
        in_specs=(
            P("expert", "dp"),
            P("expert", None),
            P("expert", "dp"),
            P("expert", None),
            P("expert", None),
            P("dp"),
            P("dp"),
            P("dp", None),
            P("expert", None, "dp"),
            P("expert", None, "dp"),
            P("expert", "dp", None),
            P("expert", "dp"),
        ),
        out_specs=(
            P("expert", "dp"),
            P("expert", "dp"),
            P("expert", None, "dp"),
            P("expert", None, "dp"),
            P("expert", "dp", None),
            P("dp", None),
            P("dp"),
            P("dp"),
        ),
        check_vma=False,
    )
```

```python
import functools

import jax
import jax.numpy as jnp
from jax import lax
from jax.experimental import pallas as pl
from jax.experimental.pallas import tpu as pltpu
from jax.sharding import PartitionSpec as P

EPSILON = 1e-06
CAPACITY = 20
SLOT_PAD = 24
HIGH = lax.Precision.HIGHEST
F32 = jnp.float32
BF16 = jnp.bfloat16
MESH = pl.DeviceIdType.MESH
NN = (((1,), (0,)), ((), ()))
NT = (((1,), (1,)), ((), ()))


def mm(a, b, dims=NN, precision=None):
    return lax.dot_general(a, b, dims, precision=precision, preferred_element_type=F32)


def iota(shape, dim):
    return lax.broadcasted_iota(jnp.int32, shape, dim)


def remote(src, dst, send_sem, recv_sem, axis, peer):
    return pltpu.make_async_remote_copy(
        src_ref=src,
        dst_ref=dst,
        send_sem=send_sem,
        recv_sem=recv_sem,
        device_id={axis: peer},
        device_id_type=MESH,
    )


def far_first(size):
    ring = min(8, size)
    order = sorted(range(ring), key=lambda k: -min(k, ring - k))
    return [base + k for base in range(size - ring, -1, -ring) for k in order if base + k]


class Exchange:
    def __init__(self, axis, me, size, src, dst, sems, width=None):
        self.axis, self.me, self.size = axis, me, size
        self.src, self.dst, self.sems, self.width = src, dst, sems, width

    def part(self, ref, spot):
        if self.width is None:
            return ref.at[spot]
        return ref.at[spot, pl.ds(0, self.width)]

    def copy(self, peer):
        src = self.part(self.dst, self.me) if self.src is None else self.part(self.src, peer)
        return remote(
            src, self.part(self.dst, self.me), self.sems.at[0], self.sems.at[1], self.axis, peer
        )

    def start(self):
        for k in far_first(self.size):
            self.copy(lax.rem(self.me + k, self.size)).start()

    def all_blocks(self):
        span = self.part(self.dst, pl.ds(0, self.size - 1))
        peer = lax.rem(self.me + 1, self.size)
        return remote(span, span, self.sems.at[0], self.sems.at[1], self.axis, peer)

    def wait(self):
        self.all_blocks().wait_recv()

    def drain(self):
        self.all_blocks().wait_send()


class Chain:
    def __init__(self, axis, me, size, dst, sems, later):
        self.axis, self.me, self.size, self.dst, self.sems = axis, me, size, dst, sems
        self.later = later

    def copy(self, peer):
        spot = self.dst.at[self.me]
        return remote(spot, spot, self.sems.at[0, peer], self.sems.at[1, self.me], self.axis, peer)

    def each(self, act):
        low, high = (self.me + 1, self.size) if self.later else (0, self.me)

        def step(p, carry):
            act(self.copy(p))
            return carry

        lax.fori_loop(low, high, step, 0)

    def start(self):
        self.each(lambda copy: copy.start())

    def drain(self):
        self.each(lambda copy: copy.wait_send())

    def wait_for(self, peer):
        spot = self.dst.at[peer]
        remote(spot, spot, self.sems.at[0, peer], self.sems.at[1, peer], self.axis, peer).wait_recv()


def block_kernel(
    dims,
    *refs,
):
    inputs, outputs, rest = refs[:12], refs[12:19], refs[19:]
    loaded, scratch = rest[:9], rest[9:]
    block_phases(dims, inputs, *loaded, *inputs[9:], *outputs, *scratch)


def block_phases(
    dims,
    inputs,
    x_ref,
    routes_ref,
    dt_ref,
    b_ref,
    c_ref,
    rate_ref,
    skip_ref,
    rw_ref,
    og_ref,
    wg_hbm,
    wu_hbm,
    wd_hbm,
    block_ref,
    token_ref,
    router_ref,
    small_ref,
    gate_ref,
    up_ref,
    down_ref,
    wg,
    wu,
    wd,
    rows_u,
    rows_g,
    gacc,
    uacc,
    vacc,
    hid,
    gb,
    ub,
    gst,
    ust,
    hst,
    cols,
    zrow,
    keep,
    pair_out,
    pair_in,
    rs_out,
    rs_in,
    cross,
    ar1,
    ar2,
    ar3,
    ar4,
    dec,
    st,
    dl,
    sg,
    tot,
    rout,
    og_out,
    og_in,
    xs_out,
    xs_in,
    sq_out,
    sq_in,
    sb_out,
    sb_in,
    bk_out,
    bk_in,
    mt,
    spread,
    gate_made,
    up_made,
    down_made,
    cf_out,
    cf_in,
    diag,
    lo_out,
    lo_in,
    local_sem,
    ag_sem,
    pair_sem,
    rs_sem,
    sem_x,
    sem_e,
):
    nd, ne, t_n, f_n, d_all, cap = dims
    pad = SLOT_PAD
    heads = dt_ref.shape[0]
    hp = f_n // heads
    n_state = b_ref.shape[0]
    rows = ne * cap
    spots = ne * pad
    chips = nd // 2
    ny = chips // 2
    nx = chips // ny
    me_d = lax.axis_index("dp")
    me_e = lax.axis_index("expert")
    core = lax.rem(me_d, 2)
    chip = me_d // 2
    chip_x, chip_y = chip // ny, lax.rem(chip, ny)
    partner = me_d + 1 - 2 * core

    def chip_after(i):
        return lax.rem(chip_x + i // ny, nx) * ny + lax.rem(chip_y + lax.rem(i, ny), ny)

    def chip_before(i):
        return lax.rem(chip_x + nx - i // ny, nx) * ny + lax.rem(chip_y + ny - lax.rem(i, ny), ny)

    barrier = pltpu.get_barrier_semaphore()

    def greet(axis, me, size):
        for k in far_first(size):
            pl.semaphore_signal(
                barrier, inc=1, device_id={axis: lax.rem(me + k, size)}, device_id_type=MESH
            )

    greet("expert", me_e, ne)
    greet("dp", me_d, nd)

    loaded = (x_ref, routes_ref, dt_ref, b_ref, c_ref, rate_ref, skip_ref, rw_ref, og_ref)
    small_copies = [
        pltpu.make_async_copy(src, dst, local_sem.at[3 + k])
        for k, (src, dst) in enumerate(zip(inputs, loaded))
    ]
    for copy in small_copies:
        copy.start()
    weight_copies = [
        pltpu.make_async_copy(src, dst, local_sem.at[k])
        for k, (src, dst) in enumerate(((wd_hbm, wd), (wg_hbm, wg), (wu_hbm, wu)))
    ]
    for copy in weight_copies:
        copy.start()

    def on_dp(dst, k):
        return Exchange("dp", me_d, nd, None, dst, sem_x.at[k])

    def on_expert(dst, k, src=None):
        return Exchange("expert", me_e, ne, src, dst, sem_x.at[k])

    ex_ar1, ex_ar2, ex_ar3, ex_ar4 = (on_dp(r, k) for k, r in enumerate((ar1, ar2, ar3, ar4)))
    ex_dec, ex_tot, ex_rout = (on_expert(r, 4 + k) for k, r in enumerate((dec, tot, rout)))
    ex_og = on_expert(og_in, 7, og_out)
    ex_xs = on_expert(xs_in, 8, xs_out)
    ex_sq = on_expert(sq_in, 9, sq_out)
    ex_sb = on_expert(sb_in, 10, sb_out)
    ex_bk = [on_expert(bk_in.at[k], 11 + k, bk_out.at[k]) for k in range(2)]
    ex_cf = on_expert(cf_in, 13, cf_out)
    ex_lo = on_expert(lo_in, 14, lo_out)
    ex_dl = on_expert(dl, 15)
    ex_st, ex_sg = (
        Chain("expert", me_e, ne, r, sem_e, k == 0) for k, r in enumerate((st, sg))
    )

    for copy in small_copies:
        copy.wait()

    def to_blocks(ref, value):
        for e in range(ne):
            ref[e] = value[e * pad : (e + 1) * pad].astype(BF16)

    def from_blocks(ref):
        return jnp.concatenate([ref[e].astype(F32) for e in range(ne)], axis=0).astype(BF16)

    x_t = x_ref[...].astype(F32).T
    ar1[me_d] = jnp.sum(x_t * x_t, axis=0, keepdims=True)
    row_id, col_id = iota((t_n, t_n), 0), iota((t_n, t_n), 1)
    causal = row_id <= col_id
    step_size = jnp.maximum(dt_ref[...], 0.0) + jnp.log1p(jnp.exp(-jnp.abs(dt_ref[...])))
    cum = mm(step_size, causal.astype(F32), NN, HIGH)
    head_lane = iota((1, f_n), 1) < hp
    head_row = iota((f_n, t_n), 0) < hp
    last = [jnp.sum(step_size[h : h + 1], axis=1, keepdims=True) for h in range(heads)]
    fade = [jnp.exp(-rate_ref[h] * last[h]) for h in range(heads)]
    dec[me_e] = jnp.concatenate(
        [
            jnp.where(head_lane, fade[0], fade[1]),
            jnp.where(head_lane, -last[0] * fade[0], -last[1] * fade[1]),
        ],
        axis=0,
    )

    expert_row = iota((ne, t_n), 0)
    hot_a = (expert_row == routes_ref[0:1, :]).astype(F32)
    hot_b = (expert_row == routes_ref[1:2, :]).astype(F32)
    before = mm((hot_a + hot_b).astype(BF16), (row_id < col_id).astype(BF16))
    spread_rows = (iota((spots, ne), 0) // pad == iota((spots, ne), 1)).astype(BF16)
    slot_of = iota((spots, t_n), 0) % pad
    fits = slot_of < cap
    here = (mm(spread_rows, before.astype(BF16)) == slot_of.astype(F32)) & fits
    pick_a = jnp.where(here, mm(spread_rows, hot_a.astype(BF16)), 0.0)
    pick_b = jnp.where(here, mm(spread_rows, hot_b.astype(BF16)), 0.0)
    pick = (pick_a + pick_b).astype(BF16)
    og = og_ref[...]
    to_blocks(og_out, mm(pick, og))
    og_in[me_e] = og_out[me_e]

    pl.semaphore_wait(barrier, nd + ne - 2)
    ex_ar1.start()
    ex_og.start()
    ex_dec.start()

    b_rows, c_rows = b_ref[...], c_ref[...]
    pairing = mm(b_rows.T, c_rows, NN, HIGH)
    fades, tails = [], []
    for h in range(heads):
        cum_h, dt_h = cum[h : h + 1], step_size[h : h + 1]
        gap = jnp.where(causal, cum_h - jnp.broadcast_to(cum_h, (t_n, t_n)).T, 0.0)
        spread[h] = gap
        mt[h] = (
            jnp.where(causal, jnp.exp(-rate_ref[h] * gap), 0.0)
            * pairing
            * jnp.broadcast_to(dt_h, (t_n, t_n)).T
        )
        fades.append(jnp.exp(-rate_ref[h] * cum_h))
        tails.append(jnp.exp(-rate_ref[h] * (last[h] - cum_h)) * dt_h)
    tail = jnp.where(head_row, tails[0], tails[1])
    reach = jnp.where(head_row, cum[0:1] - last[0], cum[1:2] - last[1])
    skip_f = jnp.where(head_row, skip_ref[0], skip_ref[1])
    hot_gap = hot_a - hot_b
    rw_gap = mm(rw_ref[...].T, hot_gap, NN, HIGH)
    spot_q = iota((rows, spots), 1)
    compact = (
        ((spot_q // pad) * cap + spot_q % pad == iota((rows, spots), 0)) & (spot_q % pad < cap)
    ).astype(BF16)
    of_block_r, of_block_b = iota((rows, ne), 0), iota((rows, ne), 1) * cap
    of_block = ((of_block_r >= of_block_b) & (of_block_r < of_block_b + cap)).astype(F32)
    lane_r = iota((rows, 128), 0)
    slot_r = lane_r - (lane_r * ((1 << 20) // cap + 1) >> 20) * cap
    lane_first = iota((rows, 128), 1) == slot_r
    lane_second = iota((rows, 128), 1) == slot_r + 64

    ex_ar1.wait()
    scale_one = lax.rsqrt(jnp.sum(ar1[...], axis=0) / d_all + EPSILON)
    normed = x_t * scale_one
    st[me_e] = mm(b_rows, normed * tail, NT, HIGH).astype(BF16)
    ex_st.start()
    dl[me_e] = mm(b_rows, normed * tail * reach, NT, HIGH).astype(BF16)
    mixed = jnp.concatenate(
        [mm(normed[h * hp : (h + 1) * hp], mt[h], NN, HIGH) for h in range(heads)], axis=0
    )
    mixed = mixed + skip_f * normed

    def ag_group(k, i):
        return chips if k == 0 or i < ny else chips + 1 if i != ny + 2 else chips + 2

    def ag_send(buf, k, i, spot, peer):
        piece = buf.at[spot]
        remote(piece, piece, ag_sem.at[k, 0], ag_sem.at[k, i], "dp", peer * 2 + core).start()

    def ag_pass(buf, k, i):
        piece = buf.at[chip_before(i) * 2 + core]
        remote(piece, piece, ag_sem.at[k, 0], ag_sem.at[k, ag_group(k, i)], "dp", partner).start()

    def ag_begin(buf, k):
        for i in (2, ny, 1, 3):
            ag_send(buf, k, i, me_d, chip_after(i))
        ag_pass(buf, k, 0)

    def ag_arrived(buf, k, i):
        spot = chip_before(i) * 2 + core
        remote(buf.at[spot], buf.at[spot], ag_sem.at[k, 0], ag_sem.at[k, i], "dp", spot).wait_recv()
        return spot

    def ag_relay(buf, k):
        spot = ag_arrived(buf, k, ny)
        for i in (1, 3):
            ag_send(buf, k, ny + i, spot, chip_after(i))
        ag_pass(buf, k, ny)
        spot = ag_arrived(buf, k, 2)
        ag_send(buf, k, ny + 2, spot, chip_after(ny))
        ag_pass(buf, k, 2)

    def ag_forward(buf, k, i):
        ag_arrived(buf, k, i)
        ag_pass(buf, k, i)

    def ag_drain(buf, k):
        every = buf.at[pl.ds(0, 2 * chips - 1)]
        remote(every, every, ag_sem.at[k, 0], ag_sem.at[k, 1], "dp", partner).wait_send()

    def ag_forwards(buf, k, turns):
        for i in turns:
            ag_forward(buf, k, i)

    def ag_partners(buf, k, turns):
        group = buf.at[pl.ds(0, len(turns))]
        remote(group, group, ag_sem.at[k, 0], ag_sem.at[k, ag_group(k, turns[0])], "dp", partner).wait_recv()

    def ag_chips(buf, turns):
        places = [chip_before(i) for i in turns]
        rows_of = jnp.concatenate([buf[2 * j + c] for j in places for c in range(2)], axis=1)
        return [pl.ds(pl.multiple_of(j * 2 * f_n, 2 * f_n), 2 * f_n) for j in places], rows_of

    def take_rows(turns, first):
        ag_partners(rows_u, 1, turns)
        spans, both = ag_chips(rows_u, turns)
        for acc, weight in ((gacc, wg), (uacc, wu)):
            part = mm(both, jnp.concatenate([weight[:, span] for span in spans], axis=1), NT)
            acc[...] = part if first else acc[...] + part

    ex_og.wait()
    rows_g[me_d] = mm(compact, from_blocks(og_in)).astype(BF16)
    ag_begin(rows_g, 0)

    ex_dec.wait()

    def carry_state(j, state):
        ex_st.wait_for(j)
        return dec[j][0:1] * state + st[j].astype(F32)

    state_in = lax.fori_loop(0, me_e, carry_state, jnp.zeros((n_state, f_n), F32))
    state_col = state_in.T
    from_state = jnp.concatenate(
        [mm(state_col[h * hp : (h + 1) * hp], c_rows * fades[h], NN, HIGH) for h in range(heads)],
        axis=0,
    )
    resid_t = (x_t + (mixed + from_state)).astype(BF16).astype(F32)
    resid = resid_t.T.astype(BF16)
    to_blocks(xs_out, mm(pick, resid))
    xs_in[me_e] = xs_out[me_e]
    ex_xs.start()
    ar2[me_d] = jnp.concatenate(
        [
            jnp.sum(resid_t * resid_t, axis=0, keepdims=True),
            jnp.sum(resid_t * rw_gap, axis=0, keepdims=True),
        ],
        axis=0,
    )
    ex_ar2.start()
    ag_relay(rows_g, 0)
    ag_forwards(rows_g, 0, (1, 3, 5, 7, 6))

    ex_ar2.wait()
    sums = jnp.sum(ar2[...], axis=0)
    scale_two = lax.rsqrt(sums[0:1] / d_all + EPSILON)
    gap_raw = sums[1:2]
    logit_gap = scale_two * gap_raw
    first_w = 1.0 / (1.0 + jnp.exp(-logit_gap))
    second_w = 1.0 / (1.0 + jnp.exp(logit_gap))
    scale_col = jnp.sum((pick_a + pick_b) * scale_two, axis=1, keepdims=True)
    weight_col = jnp.sum(pick_a * first_w + pick_b * second_w, axis=1, keepdims=True)
    lane_q = iota((spots, 128), 1)
    slot_q = iota((spots, 128), 0) % pad
    lined = jnp.where(lane_q == slot_q, scale_col, 0.0) + jnp.where(
        lane_q == slot_q + 64, weight_col, 0.0
    )
    lined = jnp.sum(lined.reshape(ne, pad, 128), axis=1)
    for e in range(ne):
        sq_out[e] = lined[e : e + 1]
    sq_in[me_e] = sq_out[me_e]
    ex_sq.start()

    ex_xs.wait()
    rows_u[me_d] = mm(compact, from_blocks(xs_in)).astype(BF16)
    ag_begin(rows_u, 1)
    weight_copies[0].wait()
    ag_partners(rows_g, 0, range(chips))
    vacc[...] = mm(jnp.concatenate([rows_g[d] for d in range(nd)], axis=1), wd[...], NT)
    weight_copies[1].wait()
    weight_copies[2].wait()
    ex_dl.start()
    coefs = jnp.concatenate([c_rows * (fades[h] * scale_two) for h in range(heads)], axis=0)
    by_slot = mm(coefs.astype(BF16), pick, NT)
    cf_out[...] = jnp.zeros_like(cf_out)
    for e in range(ne):
        cf_out[e, :, 0:pad] = by_slot[:, e * pad : (e + 1) * pad].astype(BF16)
    cf_in[me_e] = cf_out[me_e]
    ex_cf.start()
    ag_relay(rows_u, 1)
    ag_forwards(rows_u, 1, (1, 3))
    take_rows((0, 1, 2, 3), True)
    ex_sq.wait()

    def by_row(ref):
        table = jnp.concatenate([ref[b] for b in range(ne)], axis=0)
        return mm(of_block, table, NN, HIGH)

    wide = by_row(sq_in)
    cols[0] = jnp.sum(jnp.where(lane_first, wide, 0.0), axis=1, keepdims=True)
    cols[1] = jnp.sum(jnp.where(lane_second, wide, 0.0), axis=1, keepdims=True)
    ag_forwards(rows_u, 1, (5, 7, 6))
    take_rows((4, 5, 7), False)
    take_rows((6,), False)
    part = rows // 5

    def units(k, carry):
        span = pl.ds(pl.multiple_of(k * part, part), part)
        scale, weight = cols[0, span], cols[1, span]
        gate_in, up_in, grad_in = gacc[span], uacc[span], vacc[span]
        gate, up, grad = gate_in * scale, up_in * scale, grad_in * weight
        sigma = 0.5 + 0.5 * jnp.tanh(0.5 * gate)
        silu = gate * sigma
        hidden = silu * up
        gate_back = grad * up * sigma * (1.0 + gate * (1.0 - sigma))
        up_back = grad * silu
        hid[span] = hidden.astype(BF16)
        gb[span] = gate_back.astype(BF16)
        ub[span] = up_back.astype(BF16)
        pair_sum = jnp.sum(hidden * grad_in, axis=1, keepdims=True)
        inner_sum = jnp.sum(gate_back * gate_in + up_back * up_in, axis=1, keepdims=True)
        lane = iota((part, 128), 1)
        row_r = iota((part, 128), 0) + k * part
        slot = row_r - (row_r * ((1 << 20) // cap + 1) >> 20) * cap
        zrow[span] = jnp.where(lane == slot, pair_sum, 0.0) + jnp.where(
            lane == slot + 64, inner_sum, 0.0
        )
        return carry

    lax.fori_loop(0, rows // part, units, 0)
    block_t_b, block_t_r = iota((ne, rows), 0) * cap, iota((ne, rows), 1)
    of_block_t = ((block_t_r >= block_t_b) & (block_t_r < block_t_b + cap)).astype(F32)
    ar3[me_d] = mm(of_block_t, zrow[...], NN, HIGH)
    ex_ar3.start()

    def pair_copy(k, j):
        return remote(
            pair_out.at[k, j], pair_in.at[k, j], pair_sem.at[k, 0], pair_sem.at[k, 1 + j], "dp", partner
        )

    def rs_move(k, src, i, group, peer):
        return remote(
            src, rs_in.at[k, i], rs_sem.at[k, 0], rs_sem.at[k, group], "dp", peer * 2 + core
        )

    def rs_wait(k, group, blocks):
        span = rs_in.at[k, pl.ds(0, blocks)]
        remote(span, span, rs_sem.at[k, 0], rs_sem.at[k, group], "dp", partner).wait_recv()

    def rs_far(k):
        rs_wait(k, 2, 1)
        rs_out[k, 2] = (rs_out[k, 2].astype(F32) + rs_in[k, ny + 2].astype(F32)).astype(BF16)
        rs_move(k, rs_out.at[k, 2], 2, 3, chip_after(2)).start()

    def rs_total(k, first, turns):
        total = rs_out[k, first].astype(F32)
        for i in turns:
            total = total + rs_in[k, i].astype(F32)
        return total

    def rs_relay(k):
        rs_wait(k, 1, 2)
        cross[k] = rs_total(k, ny, (ny + 3, ny + 1)).astype(BF16)
        rs_move(k, cross.at[k], ny, 3, chip_after(ny)).start()

    def rs_drain(k):
        span = pair_out.at[k]
        remote(span, span, pair_sem.at[k, 0], pair_sem.at[k, 1], "dp", partner).wait_send()
        span = rs_out.at[k, pl.ds(0, chips - 1)]
        remote(span, span, rs_sem.at[k, 0], rs_sem.at[k, 1], "dp", partner).wait_send()

    def rs_index(n):
        return (1 - n // ny) * ny + lax.rem(n + 2 + n // ny, ny)

    def rs_terms(k, n, terms):
        j = chip_after(rs_index(n))
        both = terms(pl.ds(pl.multiple_of(j * 2 * f_n, 2 * f_n), 2 * f_n))
        low, high = both[:, :f_n], both[:, f_n:]
        first = core == 0
        keep[k, j] = jnp.where(first, low, high)
        pair_out[k, j] = jnp.where(first, high, low).astype(BF16)
        pair_copy(k, j).start()

    def rs_join(k, n):
        i = rs_index(n)
        j = chip_after(i)
        remote(
            pair_in.at[k, j], pair_in.at[k, j], pair_sem.at[k, 0], pair_sem.at[k, 1 + j], "dp", partner
        ).wait_recv()
        rs_out[k, i] = (keep[k, j] + pair_in[k, j].astype(F32)).astype(BF16)
        return i

    def rs_send(k, i):
        @pl.when(lax.rem(i, 2) == 1)
        def _():
            rs_move(k, rs_out.at[k, i], i, 3 - i // ny * 2, chip_after(lax.rem(i, ny))).start()

        @pl.when(i == ny + 2)
        def _():
            rs_move(k, rs_out.at[k, i], i, 2, chip_after(ny)).start()

    lag = 3

    def side_step(n, carry):
        @pl.when(n < chips)
        def _():
            rs_terms(1, n, lambda span: mm(gb[...], wg[:, span]) + mm(ub[...], wu[:, span]))

        @pl.when(n >= lag)
        def _():
            rs_send(1, rs_join(1, n - lag))

        return carry

    lax.fori_loop(0, chips + lag, side_step, 0)

    ex_ar3.wait()
    line = jnp.sum(ar3[...], axis=0)
    for b in range(ne):
        sb_out[b] = line[b : b + 1]
    sb_in[me_e] = sb_out[me_e]
    ex_sb.start()

    def down_step(n, carry):
        @pl.when(n < chips)
        def _():
            rs_terms(0, n, lambda span: mm(hid[...], wd[:, span]))

        @pl.when(n >= lag)
        def _():
            rs_join(0, n - lag)

        return carry

    lax.fori_loop(0, ny, down_step, 0)
    rs_far(1)
    lax.fori_loop(ny, chips - 1, down_step, 0)
    rs_relay(1)
    lax.fori_loop(chips - 1, chips + lag, down_step, 0)

    def down_sends(n, carry):
        rs_send(0, rs_index(n))
        return carry

    lax.fori_loop(0, chips, down_sends, 0)

    ex_sb.wait()
    table = jnp.concatenate([sb_in[e] for e in range(ne)], axis=0)
    by_spot = mm(spread_rows.astype(F32), table, NN, HIGH)
    pair_spot = jnp.sum(jnp.where(lane_q == slot_q, by_spot, 0.0), axis=1, keepdims=True)
    inner_spot = jnp.sum(jnp.where(lane_q == slot_q + 64, by_spot, 0.0), axis=1, keepdims=True)
    back_gap = jnp.sum((pick_a - pick_b) * pair_spot, axis=0, keepdims=True)
    inner_two = jnp.sum((pick_a + pick_b) * inner_spot, axis=0, keepdims=True)
    gap_grad = first_w * second_w * back_gap
    inner_two = inner_two + gap_grad * gap_raw
    rout[me_e] = mm(hot_gap * (gap_grad * scale_two), resid_t, NT, HIGH)
    ex_rout.start()

    pick_at, pick_bt = pick_a.T.astype(BF16), pick_b.T.astype(BF16)
    resid_base = og.astype(F32).T + scale_two * (gap_grad * rw_gap) - resid_t * (
        scale_two * scale_two * scale_two * inner_two / d_all
    )
    first_m = jnp.broadcast_to(first_w, (f_n, t_n)).T
    second_m = jnp.broadcast_to(second_w, (f_n, t_n)).T
    base_grads = [mm(c_rows * fades[h], resid_base, NT, HIGH) for h in range(heads)]
    sg[me_e] = jnp.where(head_lane, base_grads[0], base_grads[1]).astype(BF16)
    ex_sg.start()

    ex_cf.wait()
    width = heads * n_state
    taken = jnp.concatenate([cf_in[b].astype(F32) for b in range(ne)], axis=0).astype(BF16)
    repeat = (iota((128, spots), 0) == iota((128, spots), 1) % pad).astype(BF16)
    own_block = iota((ne * width, spots), 0) // width == iota((ne * width, spots), 1) // pad
    diag[...] = jnp.where(own_block, mm(taken, repeat), 0.0).astype(BF16)
    def rs_finish(k):
        rs_wait(k, 3, 4)
        total = rs_total(k, 0, (3, 1, ny, 2))
        wide_rows = lax.dot_general(
            compact, total.astype(BF16), (((0,), (0,)), ((), ())), preferred_element_type=F32
        )
        to_blocks(bk_out.at[k], wide_rows)
        bk_in[k, me_e] = bk_out[k, me_e]
        ex_bk[k].start()
        return wide_rows

    back_rows = rs_finish(1)
    shares = mm(diag[...], back_rows.astype(BF16))
    later = jnp.zeros((n_state, f_n), F32)
    lo_out[ne - 1] = later.astype(BF16)
    for b in range(ne - 1, 0, -1):
        low = shares[b * width : b * width + n_state]
        high = shares[b * width + n_state : (b + 1) * width]
        later = jnp.where(head_lane, low, high) + dec[b][0:1] * later
        lo_out[b - 1] = later.astype(BF16)
    lo_in[me_e] = lo_out[me_e]
    ex_lo.start()

    rs_far(0)

    rs_relay(0)
    for src, dst, k in ((gb, gst, 0), (ub, ust, 0), (hid, hst, 1)):
        dst[...] = (src[...].astype(F32) * cols[k]).T.astype(BF16)

    def weight_grads(j, carry):
        span = pl.ds(pl.multiple_of(j * 2 * f_n, 2 * f_n), 2 * f_n)
        both_u = jnp.concatenate([rows_u[2 * j], rows_u[2 * j + 1]], axis=1)
        both_g = jnp.concatenate([rows_g[2 * j], rows_g[2 * j + 1]], axis=1)
        gate_made[:, span] = mm(gst[...], both_u).astype(BF16)
        up_made[:, span] = mm(ust[...], both_u).astype(BF16)
        down_made[:, span] = mm(hst[...], both_g).astype(BF16)
        return carry

    early = chips - 3
    lax.fori_loop(0, early, weight_grads, 0)
    lax.fori_loop(early, chips, weight_grads, 0)
    def carry_slope(j, both):
        state, slope = both
        here_dec = dec[j]
        return (
            here_dec[0:1] * state + st[j].astype(F32),
            here_dec[0:1] * slope + here_dec[1:2] * state + dl[j].astype(F32),
        )

    zero_state = jnp.zeros((n_state, f_n), F32)
    ex_dl.wait()
    slope_in = lax.fori_loop(0, me_e, carry_slope, (zero_state, zero_state))[1]
    slope_col = slope_in.T
    cum_f = jnp.where(head_row, cum[0:1], cum[1:2])
    by_rate = jnp.concatenate(
        [
            mm(slope_col[h * hp : (h + 1) * hp], c_rows * fades[h], NN, HIGH)
            - mm(normed[h * hp : (h + 1) * hp], mt[h] * spread[h], NN, HIGH)
            for h in range(heads)
        ],
        axis=0,
    )
    by_rate = by_rate - cum_f * from_state

    rs_finish(0)
    ex_bk[1].wait()
    moe_grad = mm(pick_at + pick_bt, from_blocks(bk_in.at[1])).T
    grad = resid_base + scale_two * moe_grad
    lane_s = iota((1, 128), 1)
    small = jnp.zeros((1, 128), F32)
    for k, part in enumerate((grad * by_rate, grad * normed)):
        for h in range(heads):
            total = jnp.sum(part[h * hp : (h + 1) * hp], axis=0, keepdims=True)
            total = jnp.sum(total, axis=1, keepdims=True)
            small = small + jnp.where(lane_s == k * heads + h, total, 0.0)
    tot[me_e] = small
    ex_tot.start()
    normed_grad = jnp.concatenate(
        [mm(grad[h * hp : (h + 1) * hp], mt[h], NT, HIGH) for h in range(heads)], axis=0
    )
    normed_grad = normed_grad + skip_f * grad

    def carry_grad(n, later):
        j = ne - 1 - n
        ex_sg.wait_for(j)
        return dec[j][0:1] * later + sg[j].astype(F32)

    ex_lo.wait()
    later = lax.fori_loop(0, ne - 1 - me_e, carry_grad, zero_state)
    later = later + jnp.sum(lo_in[...].astype(F32), axis=0)
    normed_grad = normed_grad + tail * mm(later.T, b_rows, NN, HIGH)
    ar4[me_d] = jnp.sum(normed_grad * x_t, axis=0, keepdims=True)
    ex_ar4.start()
    grad_copies = [
        pltpu.make_async_copy(src, dst, local_sem.at[k])
        for k, (src, dst) in enumerate(((gate_made, gate_ref), (up_made, up_ref), (down_made, down_ref)))
    ]
    for copy in grad_copies:
        copy.start()
    for ex in (ex_ar1, ex_ar2, ex_ar3, ex_dec, ex_og, ex_xs, ex_sq):
        ex.drain()
    ex_st.drain()
    ex_dl.drain()
    ag_drain(rows_g, 0)
    ag_drain(rows_u, 1)
    for k in range(2):
        rs_drain(k)

    ex_rout.wait()
    router_ref[...] = jnp.sum(rout[...], axis=0)
    ex_bk[0].wait()
    came = from_blocks(bk_in.at[0])
    block_ref[...] = (
        resid.astype(F32) + (first_m * mm(pick_at, came) + second_m * mm(pick_bt, came))
    ).astype(BF16)

    ex_ar4.wait()
    inner_one = jnp.sum(ar4[...], axis=0)
    token_grad = (
        grad + scale_one * normed_grad - x_t * (scale_one * scale_one * scale_one * inner_one / d_all)
    )
    token_ref[...] = token_grad.T.astype(BF16)
    ex_tot.wait()
    small_ref[...] = jnp.sum(tot[...], axis=0)

    for copy in grad_copies:
        copy.wait()
    for ex in (ex_ar4, ex_tot, ex_rout, ex_sb, *ex_bk):
        ex.drain()
    ex_sg.drain()
    ex_cf.drain()
    ex_lo.drain()


def flush_kernel(*refs):
    made, small_ref, outs, sem = refs[:6], refs[6], refs[7:13], refs[15]
    copies = [pltpu.make_async_copy(a, b, sem.at[k]) for k, (a, b) in enumerate(zip(made, outs))]
    for copy in copies:
        copy.start()
    rate_ref, skip_ref = refs[13], refs[14]
    heads = rate_ref.shape[0]
    rate_ref[...] = small_ref[0, 0:heads]
    skip_ref[...] = small_ref[0, heads : 2 * heads]
    for copy in copies:
        copy.wait()


def body(
    tokens,
    routes,
    dt_raw,
    b_proj,
    c_proj,
    decay_rate,
    skip_gain,
    router_weight,
    gate_weight,
    up_weight,
    down_weight,
    out_grad,
):
    nd, ne = lax.axis_size("dp"), lax.axis_size("expert")
    t_n, f_n = tokens.shape
    heads, n_state = dt_raw.shape[1], b_proj.shape[1]
    d_all = nd * f_n
    units = down_weight.shape[1]
    cap, pad = CAPACITY, SLOT_PAD
    rows, chips = ne * cap, nd // 2
    vmem, hbm, anywhere = (
        pl.BlockSpec(memory_space=space) for space in (pltpu.VMEM, pltpu.HBM, pl.ANY)
    )
    def v(*s):
        return pltpu.VMEM(s, F32)

    def h(*s):
        return pltpu.VMEM(s, BF16)

    def shape(s, t):
        return jax.ShapeDtypeStruct(s, t)
    scratch = [
        h(t_n, f_n),
        pltpu.VMEM((2, t_n), jnp.int32),
        v(heads, t_n),
        v(n_state, t_n),
        v(n_state, t_n),
        pltpu.SMEM((heads,), F32),
        pltpu.SMEM((heads,), F32),
        v(ne, f_n),
        h(t_n, f_n),
        h(units, d_all),
        h(units, d_all),
        h(units, d_all),
        h(nd, rows, f_n),
        h(nd, rows, f_n),
        v(rows, units),
        v(rows, units),
        v(rows, units),
        h(rows, units),
        h(rows, units),
        h(rows, units),
        h(units, rows),
        h(units, rows),
        h(units, rows),
        v(2, rows, 1),
        v(rows, 128),
        v(2, chips, rows, f_n),
        h(2, chips, rows, f_n),
        h(2, chips, rows, f_n),
        h(2, chips, rows, f_n),
        h(2, chips, rows, f_n),
        h(2, rows, f_n),
        v(nd, 1, t_n),
        v(nd, 2, t_n),
        v(nd, ne, 128),
        v(nd, 1, t_n),
        v(ne, 2, f_n),
        h(ne, n_state, f_n),
        h(ne, n_state, f_n),
        h(ne, n_state, f_n),
        v(ne, 1, 128),
        v(ne, ne, f_n),
        h(ne, pad, f_n),
        h(ne, pad, f_n),
        h(ne, pad, f_n),
        h(ne, pad, f_n),
        v(ne, 1, 128),
        v(ne, 1, 128),
        v(ne, 1, 128),
        v(ne, 1, 128),
        h(2, ne, pad, f_n),
        h(2, ne, pad, f_n),
        v(heads, t_n, t_n),
        v(heads, t_n, t_n),
        h(units, d_all),
        h(units, d_all),
        h(units, d_all),
        h(ne, heads * n_state, 128),
        h(ne, heads * n_state, 128),
        h(ne * heads * n_state, ne * pad),
        h(ne, n_state, f_n),
        h(ne, n_state, f_n),
        pltpu.SemaphoreType.DMA((12,)),
        pltpu.SemaphoreType.DMA((2, chips + 3)),
        pltpu.SemaphoreType.DMA((2, 1 + chips)),
        pltpu.SemaphoreType.DMA((2, 4)),
        pltpu.SemaphoreType.DMA((16, 2)),
        pltpu.SemaphoreType.DMA((2, ne)),
    ]
    grad_shape = h(units, d_all)
    token_shape = h(t_n, f_n)
    made = pl.pallas_call(
        functools.partial(block_kernel, (nd, ne, t_n, f_n, d_all, cap)),
        out_shape=[
            token_shape,
            token_shape,
            v(ne, f_n),
            v(1, 128),
            grad_shape,
            grad_shape,
            grad_shape,
        ],
        in_specs=[hbm] * 12,
        out_specs=[vmem] * 4 + [anywhere] * 3,
        scratch_shapes=scratch,
        compiler_params=pltpu.CompilerParams(
            collective_id=0, has_side_effects=True, vmem_limit_bytes=61400000
        ),
        name="block",
    )(
        tokens,
        routes.T,
        dt_raw.T,
        b_proj.T,
        c_proj.T,
        decay_rate,
        skip_gain,
        router_weight.T,
        out_grad,
        gate_weight[0].T,
        up_weight[0].T,
        down_weight[0],
    )
    block_out, token_grad, router_grad, small, gate_grad, up_grad, down_grad = made
    outs = (gate_grad, up_grad, down_grad, block_out, token_grad, router_grad)
    gate_grad, up_grad, down_grad, block_out, token_grad, router_grad, rate_grad, skip_grad = pl.pallas_call(
        flush_kernel,
        out_shape=[shape(a.shape, a.dtype) for a in outs] + [shape((heads,), F32)] * 2,
        in_specs=[anywhere] * 6 + [vmem],
        out_specs=[hbm] * 6 + [vmem] * 2,
        scratch_shapes=[pltpu.SemaphoreType.DMA((6,))],
        compiler_params=pltpu.CompilerParams(vmem_limit_bytes=4 * 1024 * 1024),
        name="flush",
    )(*outs, small)
    return (
        block_out,
        token_grad,
        gate_grad.T[None],
        up_grad.T[None],
        down_grad[None],
        router_grad.T,
        rate_grad,
        skip_grad,
    )


def solution(mesh):
    return jax.shard_map(
        body,
        mesh=mesh,
        in_specs=(
            P("expert", "dp"),
            P("expert", None),
            P("expert", "dp"),
            P("expert", None),
            P("expert", None),
            P("dp"),
            P("dp"),
            P("dp", None),
            P("expert", None, "dp"),
            P("expert", None, "dp"),
            P("expert", "dp", None),
            P("expert", "dp"),
        ),
        out_specs=(
            P("expert", "dp"),
            P("expert", "dp"),
            P("expert", None, "dp"),
            P("expert", None, "dp"),
            P("expert", "dp", None),
            P("dp", None),
            P("dp"),
            P("dp"),
        ),
        check_vma=False,
    )
```

```python
import functools

import jax
import jax.numpy as jnp
from jax import lax
from jax.experimental import pallas as pl
from jax.experimental.pallas import tpu as pltpu
from jax.sharding import PartitionSpec as P

EPSILON = 1e-06
CAPACITY = 20
SLOT_PAD = 24
HIGH = lax.Precision.HIGHEST
F32 = jnp.float32
BF16 = jnp.bfloat16
MESH = pl.DeviceIdType.MESH
NN = (((1,), (0,)), ((), ()))
NT = (((1,), (1,)), ((), ()))


def mm(a, b, dims=NN, precision=None):
    return lax.dot_general(a, b, dims, precision=precision, preferred_element_type=F32)


def iota(shape, dim):
    return lax.broadcasted_iota(jnp.int32, shape, dim)


def remote(src, dst, send_sem, recv_sem, axis, peer):
    return pltpu.make_async_remote_copy(
        src_ref=src,
        dst_ref=dst,
        send_sem=send_sem,
        recv_sem=recv_sem,
        device_id={axis: peer},
        device_id_type=MESH,
    )


def far_first(size):
    ring = min(8, size)
    order = sorted(range(ring), key=lambda k: -min(k, ring - k))
    return [base + k for base in range(size - ring, -1, -ring) for k in order if base + k]


class Exchange:
    def __init__(self, axis, me, size, src, dst, sems, width=None):
        self.axis, self.me, self.size = axis, me, size
        self.src, self.dst, self.sems, self.width = src, dst, sems, width

    def part(self, ref, spot):
        if self.width is None:
            return ref.at[spot]
        return ref.at[spot, pl.ds(0, self.width)]

    def copy(self, peer):
        src = self.part(self.dst, self.me) if self.src is None else self.part(self.src, peer)
        return remote(
            src, self.part(self.dst, self.me), self.sems.at[0], self.sems.at[1], self.axis, peer
        )

    def start(self):
        for k in far_first(self.size):
            self.copy(lax.rem(self.me + k, self.size)).start()

    def all_blocks(self):
        span = self.part(self.dst, pl.ds(0, self.size - 1))
        peer = lax.rem(self.me + 1, self.size)
        return remote(span, span, self.sems.at[0], self.sems.at[1], self.axis, peer)

    def wait(self):
        self.all_blocks().wait_recv()

    def drain(self):
        self.all_blocks().wait_send()


class Chain:
    def __init__(self, axis, me, size, dst, sems, later):
        self.axis, self.me, self.size, self.dst, self.sems = axis, me, size, dst, sems
        self.later = later

    def copy(self, peer):
        spot = self.dst.at[self.me]
        return remote(spot, spot, self.sems.at[0, peer], self.sems.at[1, self.me], self.axis, peer)

    def each(self, act):
        low, high = (self.me + 1, self.size) if self.later else (0, self.me)

        def step(p, carry):
            act(self.copy(p))
            return carry

        lax.fori_loop(low, high, step, 0)

    def start(self):
        self.each(lambda copy: copy.start())

    def drain(self):
        self.each(lambda copy: copy.wait_send())

    def wait_for(self, peer):
        spot = self.dst.at[peer]
        remote(spot, spot, self.sems.at[0, peer], self.sems.at[1, peer], self.axis, peer).wait_recv()


def block_kernel(
    dims,
    *refs,
):
    inputs, outputs, rest = refs[:12], refs[12:19], refs[19:]
    loaded, scratch = rest[:9], rest[9:]
    block_phases(dims, inputs, *loaded, *inputs[9:], *outputs, *scratch)


def block_phases(
    dims,
    inputs,
    x_ref,
    routes_ref,
    dt_ref,
    b_ref,
    c_ref,
    rate_ref,
    skip_ref,
    rw_ref,
    og_ref,
    wg_hbm,
    wu_hbm,
    wd_hbm,
    block_ref,
    token_ref,
    router_ref,
    small_ref,
    gate_ref,
    up_ref,
    down_ref,
    wg,
    wu,
    wd,
    rows_u,
    rows_g,
    gacc,
    uacc,
    vacc,
    hid,
    gb,
    ub,
    gst,
    ust,
    hst,
    cols,
    zrow,
    keep,
    pair_out,
    pair_in,
    rs_out,
    rs_in,
    cross,
    ar1,
    ar2,
    ar3,
    ar4,
    dec,
    st,
    dl,
    sg,
    tot,
    rout,
    og_out,
    og_in,
    xs_out,
    xs_in,
    sq_out,
    sq_in,
    sb_out,
    sb_in,
    bk_out,
    bk_in,
    mt,
    spread,
    gate_made,
    up_made,
    down_made,
    cf_out,
    cf_in,
    diag,
    lo_out,
    lo_in,
    local_sem,
    ag_sem,
    pair_sem,
    rs_sem,
    sem_x,
    sem_e,
):
    nd, ne, t_n, f_n, d_all, cap = dims
    pad = SLOT_PAD
    heads = dt_ref.shape[0]
    hp = f_n // heads
    n_state = b_ref.shape[0]
    rows = ne * cap
    spots = ne * pad
    chips = nd // 2
    ny = chips // 2
    nx = chips // ny
    me_d = lax.axis_index("dp")
    me_e = lax.axis_index("expert")
    core = lax.rem(me_d, 2)
    chip = me_d // 2
    chip_x, chip_y = chip // ny, lax.rem(chip, ny)
    partner = me_d + 1 - 2 * core

    def chip_after(i):
        return lax.rem(chip_x + i // ny, nx) * ny + lax.rem(chip_y + lax.rem(i, ny), ny)

    def chip_before(i):
        return lax.rem(chip_x + nx - i // ny, nx) * ny + lax.rem(chip_y + ny - lax.rem(i, ny), ny)

    barrier = pltpu.get_barrier_semaphore()

    def greet(axis, me, size):
        for k in far_first(size):
            pl.semaphore_signal(
                barrier, inc=1, device_id={axis: lax.rem(me + k, size)}, device_id_type=MESH
            )

    greet("expert", me_e, ne)
    greet("dp", me_d, nd)

    loaded = (x_ref, routes_ref, dt_ref, b_ref, c_ref, rate_ref, skip_ref, rw_ref, og_ref)
    small_copies = [
        pltpu.make_async_copy(src, dst, local_sem.at[3 + k])
        for k, (src, dst) in enumerate(zip(inputs, loaded))
    ]
    for copy in small_copies:
        copy.start()
    weight_copies = [
        pltpu.make_async_copy(src, dst, local_sem.at[k])
        for k, (src, dst) in enumerate(((wd_hbm, wd), (wg_hbm, wg), (wu_hbm, wu)))
    ]
    for copy in weight_copies:
        copy.start()

    def on_dp(dst, k):
        return Exchange("dp", me_d, nd, None, dst, sem_x.at[k])

    def on_expert(dst, k, src=None):
        return Exchange("expert", me_e, ne, src, dst, sem_x.at[k])

    ex_ar1, ex_ar2, ex_ar3, ex_ar4 = (on_dp(r, k) for k, r in enumerate((ar1, ar2, ar3, ar4)))
    ex_dec, ex_tot, ex_rout = (on_expert(r, 4 + k) for k, r in enumerate((dec, tot, rout)))
    ex_og = on_expert(og_in, 7, og_out)
    ex_xs = on_expert(xs_in, 8, xs_out)
    ex_sq = on_expert(sq_in, 9, sq_out)
    ex_sb = on_expert(sb_in, 10, sb_out)
    ex_bk = [on_expert(bk_in.at[k], 11 + k, bk_out.at[k]) for k in range(2)]
    ex_cf = on_expert(cf_in, 13, cf_out)
    ex_lo = on_expert(lo_in, 14, lo_out)
    ex_dl = on_expert(dl, 15)
    ex_st, ex_sg = (
        Chain("expert", me_e, ne, r, sem_e, k == 0) for k, r in enumerate((st, sg))
    )

    for copy in small_copies:
        copy.wait()

    def to_blocks(ref, value):
        for e in range(ne):
            ref[e] = value[e * pad : (e + 1) * pad].astype(BF16)

    def from_blocks(ref):
        return jnp.concatenate([ref[e].astype(F32) for e in range(ne)], axis=0).astype(BF16)

    x_t = x_ref[...].astype(F32).T
    ar1[me_d] = jnp.sum(x_t * x_t, axis=0, keepdims=True)
    row_id, col_id = iota((t_n, t_n), 0), iota((t_n, t_n), 1)
    causal = row_id <= col_id
    step_size = jnp.maximum(dt_ref[...], 0.0) + jnp.log1p(jnp.exp(-jnp.abs(dt_ref[...])))
    cum = mm(step_size, causal.astype(F32), NN, HIGH)
    head_lane = iota((1, f_n), 1) < hp
    head_row = iota((f_n, t_n), 0) < hp
    last = [jnp.sum(step_size[h : h + 1], axis=1, keepdims=True) for h in range(heads)]
    fade = [jnp.exp(-rate_ref[h] * last[h]) for h in range(heads)]
    dec[me_e] = jnp.concatenate(
        [
            jnp.where(head_lane, fade[0], fade[1]),
            jnp.where(head_lane, -last[0] * fade[0], -last[1] * fade[1]),
        ],
        axis=0,
    )

    expert_row = iota((ne, t_n), 0)
    hot_a = (expert_row == routes_ref[0:1, :]).astype(F32)
    hot_b = (expert_row == routes_ref[1:2, :]).astype(F32)
    before = mm((hot_a + hot_b).astype(BF16), (row_id < col_id).astype(BF16))
    spread_rows = (iota((spots, ne), 0) // pad == iota((spots, ne), 1)).astype(BF16)
    slot_of = iota((spots, t_n), 0) % pad
    fits = slot_of < cap
    here = (mm(spread_rows, before.astype(BF16)) == slot_of.astype(F32)) & fits
    pick_a = jnp.where(here, mm(spread_rows, hot_a.astype(BF16)), 0.0)
    pick_b = jnp.where(here, mm(spread_rows, hot_b.astype(BF16)), 0.0)
    pick = (pick_a + pick_b).astype(BF16)
    og = og_ref[...]
    to_blocks(og_out, mm(pick, og))
    og_in[me_e] = og_out[me_e]

    pl.semaphore_wait(barrier, nd + ne - 2)
    ex_ar1.start()
    ex_og.start()
    ex_dec.start()

    b_rows, c_rows = b_ref[...], c_ref[...]
    pairing = mm(b_rows.T, c_rows, NN, HIGH)
    fades, tails = [], []
    for h in range(heads):
        cum_h, dt_h = cum[h : h + 1], step_size[h : h + 1]
        gap = jnp.where(causal, cum_h - jnp.broadcast_to(cum_h, (t_n, t_n)).T, 0.0)
        spread[h] = gap
        mt[h] = (
            jnp.where(causal, jnp.exp(-rate_ref[h] * gap), 0.0)
            * pairing
            * jnp.broadcast_to(dt_h, (t_n, t_n)).T
        )
        fades.append(jnp.exp(-rate_ref[h] * cum_h))
        tails.append(jnp.exp(-rate_ref[h] * (last[h] - cum_h)) * dt_h)
    tail = jnp.where(head_row, tails[0], tails[1])
    reach = jnp.where(head_row, cum[0:1] - last[0], cum[1:2] - last[1])
    skip_f = jnp.where(head_row, skip_ref[0], skip_ref[1])
    hot_gap = hot_a - hot_b
    rw_gap = mm(rw_ref[...].T, hot_gap, NN, HIGH)
    spot_q = iota((rows, spots), 1)
    compact = (
        ((spot_q // pad) * cap + spot_q % pad == iota((rows, spots), 0)) & (spot_q % pad < cap)
    ).astype(BF16)
    spot_qt = iota((spots, rows), 0)
    compact_t = (
        ((spot_qt // pad) * cap + spot_qt % pad == iota((spots, rows), 1)) & (spot_qt % pad < cap)
    ).astype(BF16)
    of_block_r, of_block_b = iota((rows, ne), 0), iota((rows, ne), 1) * cap
    of_block = ((of_block_r >= of_block_b) & (of_block_r < of_block_b + cap)).astype(F32)
    lane_r = iota((rows, 128), 0)
    slot_r = lane_r - (lane_r * ((1 << 20) // cap + 1) >> 20) * cap
    lane_first = iota((rows, 128), 1) == slot_r
    lane_second = iota((rows, 128), 1) == slot_r + 64

    ex_ar1.wait()
    scale_one = lax.rsqrt(jnp.sum(ar1[...], axis=0) / d_all + EPSILON)
    normed = x_t * scale_one
    st[me_e] = mm(b_rows.astype(BF16), (normed * tail).astype(BF16), NT).astype(BF16)
    ex_st.start()
    dl[me_e] = mm(b_rows, normed * tail * reach, NT, HIGH).astype(BF16)
    mixed = jnp.concatenate(
        [mm(normed[h * hp : (h + 1) * hp], mt[h], NN, HIGH) for h in range(heads)], axis=0
    )
    mixed = mixed + skip_f * normed

    def ag_group(k, i):
        return chips if k == 0 or i < ny else chips + 1 if i != ny + 2 else chips + 2

    def ag_send(buf, k, i, spot, peer):
        piece = buf.at[spot]
        remote(piece, piece, ag_sem.at[k, 0], ag_sem.at[k, i], "dp", peer * 2 + core).start()

    def ag_pass(buf, k, i):
        piece = buf.at[chip_before(i) * 2 + core]
        remote(piece, piece, ag_sem.at[k, 0], ag_sem.at[k, ag_group(k, i)], "dp", partner).start()

    def ag_begin(buf, k):
        for i in (2, ny, 1, 3):
            ag_send(buf, k, i, me_d, chip_after(i))
        ag_pass(buf, k, 0)

    def ag_arrived(buf, k, i):
        spot = chip_before(i) * 2 + core
        remote(buf.at[spot], buf.at[spot], ag_sem.at[k, 0], ag_sem.at[k, i], "dp", spot).wait_recv()
        return spot

    def ag_relay(buf, k):
        spot = ag_arrived(buf, k, ny)
        for i in (1, 3):
            ag_send(buf, k, ny + i, spot, chip_after(i))
        ag_pass(buf, k, ny)
        spot = ag_arrived(buf, k, 2)
        ag_send(buf, k, ny + 2, spot, chip_after(ny))
        ag_pass(buf, k, 2)

    def ag_forward(buf, k, i):
        ag_arrived(buf, k, i)
        ag_pass(buf, k, i)

    def ag_drain(buf, k):
        every = buf.at[pl.ds(0, 2 * chips - 1)]
        remote(every, every, ag_sem.at[k, 0], ag_sem.at[k, 1], "dp", partner).wait_send()

    def ag_forwards(buf, k, turns):
        for i in turns:
            ag_forward(buf, k, i)

    def ag_partners(buf, k, turns):
        group = buf.at[pl.ds(0, len(turns))]
        remote(group, group, ag_sem.at[k, 0], ag_sem.at[k, ag_group(k, turns[0])], "dp", partner).wait_recv()

    def ag_chips(buf, turns):
        places = [chip_before(i) for i in turns]
        rows_of = jnp.concatenate([buf[2 * j + c] for j in places for c in range(2)], axis=1)
        return [pl.ds(pl.multiple_of(j * 2 * f_n, 2 * f_n), 2 * f_n) for j in places], rows_of

    def take_rows(turns, first):
        ag_partners(rows_u, 1, turns)
        spans, both = ag_chips(rows_u, turns)
        for acc, weight in ((gacc, wg), (uacc, wu)):
            part = mm(both, jnp.concatenate([weight[:, span] for span in spans], axis=1), NT)
            acc[...] = part if first else acc[...] + part

    ex_og.wait()
    rows_g[me_d] = mm(compact, from_blocks(og_in)).astype(BF16)
    ag_begin(rows_g, 0)

    ex_dec.wait()

    def carry_state(j, state):
        ex_st.wait_for(j)
        return dec[j][0:1] * state + st[j].astype(F32)

    state_in = lax.fori_loop(0, me_e, carry_state, jnp.zeros((n_state, f_n), F32))
    state_col = state_in.T.astype(BF16)
    from_state = jnp.concatenate(
        [
            mm(state_col[h * hp : (h + 1) * hp], (c_rows * fades[h]).astype(BF16))
            for h in range(heads)
        ],
        axis=0,
    )
    resid_t = (x_t + (mixed + from_state)).astype(BF16).astype(F32)
    resid = resid_t.T.astype(BF16)
    to_blocks(xs_out, mm(pick, resid))
    xs_in[me_e] = xs_out[me_e]
    ex_xs.start()
    ar2[me_d] = jnp.concatenate(
        [
            jnp.sum(resid_t * resid_t, axis=0, keepdims=True),
            jnp.sum(resid_t * rw_gap, axis=0, keepdims=True),
        ],
        axis=0,
    )
    ex_ar2.start()
    ag_relay(rows_g, 0)
    ag_forwards(rows_g, 0, (1, 3, 5, 7, 6))

    ex_ar2.wait()
    sums = jnp.sum(ar2[...], axis=0)
    scale_two = lax.rsqrt(sums[0:1] / d_all + EPSILON)
    gap_raw = sums[1:2]
    logit_gap = scale_two * gap_raw
    first_w = 1.0 / (1.0 + jnp.exp(-logit_gap))
    second_w = 1.0 / (1.0 + jnp.exp(logit_gap))
    scale_col = jnp.sum((pick_a + pick_b) * scale_two, axis=1, keepdims=True)
    weight_col = jnp.sum(pick_a * first_w + pick_b * second_w, axis=1, keepdims=True)
    lane_q = iota((spots, 128), 1)
    slot_q = iota((spots, 128), 0) % pad
    lined = jnp.where(lane_q == slot_q, scale_col, 0.0) + jnp.where(
        lane_q == slot_q + 64, weight_col, 0.0
    )
    lined = jnp.sum(lined.reshape(ne, pad, 128), axis=1)
    for e in range(ne):
        sq_out[e] = lined[e : e + 1]
    sq_in[me_e] = sq_out[me_e]
    ex_sq.start()

    ex_xs.wait()
    rows_u[me_d] = mm(compact, from_blocks(xs_in)).astype(BF16)
    ag_begin(rows_u, 1)
    weight_copies[0].wait()
    ag_partners(rows_g, 0, range(chips))
    vacc[...] = mm(jnp.concatenate([rows_g[d] for d in range(nd)], axis=1), wd[...], NT)
    weight_copies[1].wait()
    weight_copies[2].wait()
    ex_dl.start()
    coefs = jnp.concatenate([c_rows * (fades[h] * scale_two) for h in range(heads)], axis=0)
    by_slot = mm(coefs.astype(BF16), pick, NT)
    cf_out[...] = jnp.zeros_like(cf_out)
    for e in range(ne):
        cf_out[e, :, 0:pad] = by_slot[:, e * pad : (e + 1) * pad].astype(BF16)
    cf_in[me_e] = cf_out[me_e]
    ex_cf.start()
    ag_relay(rows_u, 1)
    ag_forwards(rows_u, 1, (1, 3))
    take_rows((0, 1, 2, 3), True)
    ex_sq.wait()

    def by_row(ref):
        table = jnp.concatenate([ref[b] for b in range(ne)], axis=0)
        return mm(of_block, table, NN, HIGH)

    wide = by_row(sq_in)
    cols[0] = jnp.sum(jnp.where(lane_first, wide, 0.0), axis=1, keepdims=True)
    cols[1] = jnp.sum(jnp.where(lane_second, wide, 0.0), axis=1, keepdims=True)
    ag_forwards(rows_u, 1, (5, 7, 6))
    take_rows((4, 5, 7), False)
    take_rows((6,), False)
    part = rows // 5

    def units(k, carry):
        span = pl.ds(pl.multiple_of(k * part, part), part)
        scale, weight = cols[0, span], cols[1, span]
        gate_in, up_in, grad_in = gacc[span], uacc[span], vacc[span]
        gate, up, grad = gate_in * scale, up_in * scale, grad_in * weight
        sigma = 0.5 + 0.5 * jnp.tanh(0.5 * gate)
        silu = gate * sigma
        hidden = silu * up
        gate_back = grad * up * sigma * (1.0 + gate * (1.0 - sigma))
        up_back = grad * silu
        hid[span] = hidden.astype(BF16)
        gb[span] = gate_back.astype(BF16)
        ub[span] = up_back.astype(BF16)
        pair_sum = jnp.sum(hidden * grad_in, axis=1, keepdims=True)
        inner_sum = jnp.sum(gate_back * gate_in + up_back * up_in, axis=1, keepdims=True)
        lane = iota((part, 128), 1)
        row_r = iota((part, 128), 0) + k * part
        slot = row_r - (row_r * ((1 << 20) // cap + 1) >> 20) * cap
        zrow[span] = jnp.where(lane == slot, pair_sum, 0.0) + jnp.where(
            lane == slot + 64, inner_sum, 0.0
        )
        return carry

    lax.fori_loop(0, rows // part, units, 0)
    block_t_b, block_t_r = iota((ne, rows), 0) * cap, iota((ne, rows), 1)
    of_block_t = ((block_t_r >= block_t_b) & (block_t_r < block_t_b + cap)).astype(F32)
    ar3[me_d] = mm(of_block_t, zrow[...], NN, HIGH)
    ex_ar3.start()

    def pair_copy(k, j):
        return remote(
            pair_out.at[k, j], pair_in.at[k, j], pair_sem.at[k, 0], pair_sem.at[k, 1 + j], "dp", partner
        )

    def rs_move(k, src, i, group, peer):
        return remote(
            src, rs_in.at[k, i], rs_sem.at[k, 0], rs_sem.at[k, group], "dp", peer * 2 + core
        )

    def rs_wait(k, group, blocks):
        span = rs_in.at[k, pl.ds(0, blocks)]
        remote(span, span, rs_sem.at[k, 0], rs_sem.at[k, group], "dp", partner).wait_recv()

    def rs_far(k):
        rs_wait(k, 2, 1)
        rs_out[k, 2] = (rs_out[k, 2].astype(F32) + rs_in[k, ny + 2].astype(F32)).astype(BF16)
        rs_move(k, rs_out.at[k, 2], 2, 3, chip_after(2)).start()

    def rs_total(k, first, turns):
        total = rs_out[k, first].astype(F32)
        for i in turns:
            total = total + rs_in[k, i].astype(F32)
        return total

    def rs_relay(k):
        rs_wait(k, 1, 2)
        cross[k] = rs_total(k, ny, (ny + 3, ny + 1)).astype(BF16)
        rs_move(k, cross.at[k], ny, 3, chip_after(ny)).start()

    def rs_drain(k):
        span = pair_out.at[k]
        remote(span, span, pair_sem.at[k, 0], pair_sem.at[k, 1], "dp", partner).wait_send()
        span = rs_out.at[k, pl.ds(0, chips - 1)]
        remote(span, span, rs_sem.at[k, 0], rs_sem.at[k, 1], "dp", partner).wait_send()

    def rs_index(n):
        return (1 - n // ny) * ny + lax.rem(n + 2 + n // ny, ny)

    def rs_terms(k, n, terms):
        j = chip_after(rs_index(n))
        both = terms(pl.ds(pl.multiple_of(j * 2 * f_n, 2 * f_n), 2 * f_n))
        low, high = both[:, :f_n], both[:, f_n:]
        first = core == 0
        keep[k, j] = jnp.where(first, low, high)
        pair_out[k, j] = jnp.where(first, high, low).astype(BF16)
        pair_copy(k, j).start()

    def rs_join(k, n):
        i = rs_index(n)
        j = chip_after(i)
        remote(
            pair_in.at[k, j], pair_in.at[k, j], pair_sem.at[k, 0], pair_sem.at[k, 1 + j], "dp", partner
        ).wait_recv()
        rs_out[k, i] = (keep[k, j] + pair_in[k, j].astype(F32)).astype(BF16)
        return i

    def rs_send(k, i):
        @pl.when(lax.rem(i, 2) == 1)
        def _():
            rs_move(k, rs_out.at[k, i], i, 3 - i // ny * 2, chip_after(lax.rem(i, ny))).start()

        @pl.when(i == ny + 2)
        def _():
            rs_move(k, rs_out.at[k, i], i, 2, chip_after(ny)).start()

    lag = 3

    def side_step(n, carry):
        @pl.when(n < chips)
        def _():
            rs_terms(1, n, lambda span: mm(gb[...], wg[:, span]) + mm(ub[...], wu[:, span]))

        @pl.when(n >= lag)
        def _():
            rs_send(1, rs_join(1, n - lag))

        return carry

    lax.fori_loop(0, chips + lag, side_step, 0)

    ex_ar3.wait()
    line = jnp.sum(ar3[...], axis=0)
    for b in range(ne):
        sb_out[b] = line[b : b + 1]
    sb_in[me_e] = sb_out[me_e]
    ex_sb.start()

    def down_step(n, carry):
        @pl.when(n < chips)
        def _():
            rs_terms(0, n, lambda span: mm(hid[...], wd[:, span]))

        @pl.when(n >= lag)
        def _():
            rs_join(0, n - lag)

        return carry

    lax.fori_loop(0, ny, down_step, 0)
    rs_far(1)
    lax.fori_loop(ny, chips - 1, down_step, 0)
    rs_relay(1)
    lax.fori_loop(chips - 1, chips + lag, down_step, 0)

    def down_sends(n, carry):
        rs_send(0, rs_index(n))
        return carry

    lax.fori_loop(0, chips, down_sends, 0)

    ex_sb.wait()
    table = jnp.concatenate([sb_in[e] for e in range(ne)], axis=0)
    by_spot = mm(spread_rows.astype(F32), table, NN, HIGH)
    pair_spot = jnp.sum(jnp.where(lane_q == slot_q, by_spot, 0.0), axis=1, keepdims=True)
    inner_spot = jnp.sum(jnp.where(lane_q == slot_q + 64, by_spot, 0.0), axis=1, keepdims=True)
    back_gap = jnp.sum((pick_a - pick_b) * pair_spot, axis=0, keepdims=True)
    inner_two = jnp.sum((pick_a + pick_b) * inner_spot, axis=0, keepdims=True)
    gap_grad = first_w * second_w * back_gap
    inner_two = inner_two + gap_grad * gap_raw
    rout[me_e] = mm(hot_gap * (gap_grad * scale_two), resid_t, NT, HIGH)
    ex_rout.start()

    pick_at, pick_bt = pick_a.T.astype(BF16), pick_b.T.astype(BF16)
    resid_base = og.astype(F32).T + scale_two * (gap_grad * rw_gap) - resid_t * (
        scale_two * scale_two * scale_two * inner_two / d_all
    )
    first_m = jnp.broadcast_to(first_w, (f_n, t_n)).T
    second_m = jnp.broadcast_to(second_w, (f_n, t_n)).T
    base_grads = [mm(c_rows * fades[h], resid_base, NT, HIGH) for h in range(heads)]
    sg[me_e] = jnp.where(head_lane, base_grads[0], base_grads[1]).astype(BF16)
    ex_sg.start()

    ex_cf.wait()
    width = heads * n_state
    taken = jnp.concatenate([cf_in[b].astype(F32) for b in range(ne)], axis=0).astype(BF16)
    repeat = (iota((128, spots), 0) == iota((128, spots), 1) % pad).astype(BF16)
    own_block = iota((ne * width, spots), 0) // width == iota((ne * width, spots), 1) // pad
    diag[...] = jnp.where(own_block, mm(taken, repeat), 0.0).astype(BF16)
    def rs_finish(k):
        rs_wait(k, 3, 4)
        total = rs_total(k, 0, (3, 1, ny, 2))
        wide_rows = mm(compact_t, total.astype(BF16))
        to_blocks(bk_out.at[k], wide_rows)
        bk_in[k, me_e] = bk_out[k, me_e]
        ex_bk[k].start()
        return wide_rows

    back_rows = rs_finish(1)
    shares = mm(diag[...], back_rows.astype(BF16))
    later = jnp.zeros((n_state, f_n), F32)
    lo_out[ne - 1] = later.astype(BF16)
    for b in range(ne - 1, 0, -1):
        low = shares[b * width : b * width + n_state]
        high = shares[b * width + n_state : (b + 1) * width]
        later = jnp.where(head_lane, low, high) + dec[b][0:1] * later
        lo_out[b - 1] = later.astype(BF16)
    lo_in[me_e] = lo_out[me_e]
    ex_lo.start()

    rs_far(0)

    rs_relay(0)
    for src, dst, k in ((gb, gst, 0), (ub, ust, 0), (hid, hst, 1)):
        dst[...] = (src[...].astype(F32) * cols[k]).T.astype(BF16)

    def weight_grads(j, carry):
        span = pl.ds(pl.multiple_of(j * 2 * f_n, 2 * f_n), 2 * f_n)
        both_u = jnp.concatenate([rows_u[2 * j], rows_u[2 * j + 1]], axis=1)
        both_g = jnp.concatenate([rows_g[2 * j], rows_g[2 * j + 1]], axis=1)
        gate_made[:, span] = mm(gst[...], both_u).astype(BF16)
        up_made[:, span] = mm(ust[...], both_u).astype(BF16)
        down_made[:, span] = mm(hst[...], both_g).astype(BF16)
        return carry

    early = chips - 3
    lax.fori_loop(0, early, weight_grads, 0)
    lax.fori_loop(early, chips, weight_grads, 0)
    def carry_slope(j, both):
        state, slope = both
        here_dec = dec[j]
        return (
            here_dec[0:1] * state + st[j].astype(F32),
            here_dec[0:1] * slope + here_dec[1:2] * state + dl[j].astype(F32),
        )

    zero_state = jnp.zeros((n_state, f_n), F32)
    ex_dl.wait()
    slope_in = lax.fori_loop(0, me_e, carry_slope, (zero_state, zero_state))[1]
    slope_col = slope_in.T
    cum_f = jnp.where(head_row, cum[0:1], cum[1:2])
    by_rate = jnp.concatenate(
        [
            mm(slope_col[h * hp : (h + 1) * hp], c_rows * fades[h], NN, HIGH)
            - mm(normed[h * hp : (h + 1) * hp], mt[h] * spread[h], NN, HIGH)
            for h in range(heads)
        ],
        axis=0,
    )
    by_rate = by_rate - cum_f * from_state

    rs_finish(0)
    ex_bk[1].wait()
    moe_grad = mm(pick_at + pick_bt, from_blocks(bk_in.at[1])).T
    grad = resid_base + scale_two * moe_grad
    lane_s = iota((1, 128), 1)
    small = jnp.zeros((1, 128), F32)
    for k, part in enumerate((grad * by_rate, grad * normed)):
        for h in range(heads):
            total = jnp.sum(part[h * hp : (h + 1) * hp], axis=0, keepdims=True)
            total = jnp.sum(total, axis=1, keepdims=True)
            small = small + jnp.where(lane_s == k * heads + h, total, 0.0)
    tot[me_e] = small
    ex_tot.start()
    normed_grad = jnp.concatenate(
        [mm(grad[h * hp : (h + 1) * hp], mt[h], NT, HIGH) for h in range(heads)], axis=0
    )
    normed_grad = normed_grad + skip_f * grad

    def carry_grad(n, later):
        j = ne - 1 - n
        ex_sg.wait_for(j)
        return dec[j][0:1] * later + sg[j].astype(F32)

    ex_lo.wait()
    later = lax.fori_loop(0, ne - 1 - me_e, carry_grad, zero_state)
    later = later + jnp.sum(lo_in[...].astype(F32), axis=0)
    normed_grad = normed_grad + tail * mm(later.T.astype(BF16), b_rows.astype(BF16))
    ar4[me_d] = jnp.sum(normed_grad * x_t, axis=0, keepdims=True)
    ex_ar4.start()
    grad_copies = [
        pltpu.make_async_copy(src, dst, local_sem.at[k])
        for k, (src, dst) in enumerate(((gate_made, gate_ref), (up_made, up_ref), (down_made, down_ref)))
    ]
    for copy in grad_copies:
        copy.start()
    for ex in (ex_ar1, ex_ar2, ex_ar3, ex_dec, ex_og, ex_xs, ex_sq):
        ex.drain()
    ex_st.drain()
    ex_dl.drain()
    ag_drain(rows_g, 0)
    ag_drain(rows_u, 1)
    for k in range(2):
        rs_drain(k)

    ex_rout.wait()
    router_ref[...] = jnp.sum(rout[...], axis=0)
    ex_bk[0].wait()
    came = from_blocks(bk_in.at[0])
    block_ref[...] = (
        resid.astype(F32) + (first_m * mm(pick_at, came) + second_m * mm(pick_bt, came))
    ).astype(BF16)

    ex_ar4.wait()
    inner_one = jnp.sum(ar4[...], axis=0)
    token_grad = (
        grad + scale_one * normed_grad - x_t * (scale_one * scale_one * scale_one * inner_one / d_all)
    )
    token_ref[...] = token_grad.T.astype(BF16)
    ex_tot.wait()
    small_ref[...] = jnp.sum(tot[...], axis=0)

    for copy in grad_copies:
        copy.wait()
    for ex in (ex_ar4, ex_tot, ex_rout, ex_sb, *ex_bk):
        ex.drain()
    ex_sg.drain()
    ex_cf.drain()
    ex_lo.drain()


def flush_kernel(*refs):
    made, small_ref, outs, sem = refs[:6], refs[6], refs[7:13], refs[15]
    copies = [pltpu.make_async_copy(a, b, sem.at[k]) for k, (a, b) in enumerate(zip(made, outs))]
    for copy in copies:
        copy.start()
    rate_ref, skip_ref = refs[13], refs[14]
    heads = rate_ref.shape[0]
    rate_ref[...] = small_ref[0, 0:heads]
    skip_ref[...] = small_ref[0, heads : 2 * heads]
    for copy in copies:
        copy.wait()


def body(
    tokens,
    routes,
    dt_raw,
    b_proj,
    c_proj,
    decay_rate,
    skip_gain,
    router_weight,
    gate_weight,
    up_weight,
    down_weight,
    out_grad,
):
    nd, ne = lax.axis_size("dp"), lax.axis_size("expert")
    t_n, f_n = tokens.shape
    heads, n_state = dt_raw.shape[1], b_proj.shape[1]
    d_all = nd * f_n
    units = down_weight.shape[1]
    cap, pad = CAPACITY, SLOT_PAD
    rows, chips = ne * cap, nd // 2
    vmem, hbm, anywhere = (
        pl.BlockSpec(memory_space=space) for space in (pltpu.VMEM, pltpu.HBM, pl.ANY)
    )
    def v(*s):
        return pltpu.VMEM(s, F32)

    def h(*s):
        return pltpu.VMEM(s, BF16)

    def shape(s, t):
        return jax.ShapeDtypeStruct(s, t)
    scratch = [
        h(t_n, f_n),
        pltpu.VMEM((2, t_n), jnp.int32),
        v(heads, t_n),
        v(n_state, t_n),
        v(n_state, t_n),
        pltpu.SMEM((heads,), F32),
        pltpu.SMEM((heads,), F32),
        v(ne, f_n),
        h(t_n, f_n),
        h(units, d_all),
        h(units, d_all),
        h(units, d_all),
        h(nd, rows, f_n),
        h(nd, rows, f_n),
        v(rows, units),
        v(rows, units),
        v(rows, units),
        h(rows, units),
        h(rows, units),
        h(rows, units),
        h(units, rows),
        h(units, rows),
        h(units, rows),
        v(2, rows, 1),
        v(rows, 128),
        v(2, chips, rows, f_n),
        h(2, chips, rows, f_n),
        h(2, chips, rows, f_n),
        h(2, chips, rows, f_n),
        h(2, chips, rows, f_n),
        h(2, rows, f_n),
        v(nd, 1, t_n),
        v(nd, 2, t_n),
        v(nd, ne, 128),
        v(nd, 1, t_n),
        v(ne, 2, f_n),
        h(ne, n_state, f_n),
        h(ne, n_state, f_n),
        h(ne, n_state, f_n),
        v(ne, 1, 128),
        v(ne, ne, f_n),
        h(ne, pad, f_n),
        h(ne, pad, f_n),
        h(ne, pad, f_n),
        h(ne, pad, f_n),
        v(ne, 1, 128),
        v(ne, 1, 128),
        v(ne, 1, 128),
        v(ne, 1, 128),
        h(2, ne, pad, f_n),
        h(2, ne, pad, f_n),
        v(heads, t_n, t_n),
        v(heads, t_n, t_n),
        h(units, d_all),
        h(units, d_all),
        h(units, d_all),
        h(ne, heads * n_state, 128),
        h(ne, heads * n_state, 128),
        h(ne * heads * n_state, ne * pad),
        h(ne, n_state, f_n),
        h(ne, n_state, f_n),
        pltpu.SemaphoreType.DMA((12,)),
        pltpu.SemaphoreType.DMA((2, chips + 3)),
        pltpu.SemaphoreType.DMA((2, 1 + chips)),
        pltpu.SemaphoreType.DMA((2, 4)),
        pltpu.SemaphoreType.DMA((16, 2)),
        pltpu.SemaphoreType.DMA((2, ne)),
    ]
    grad_shape = h(units, d_all)
    token_shape = h(t_n, f_n)
    made = pl.pallas_call(
        functools.partial(block_kernel, (nd, ne, t_n, f_n, d_all, cap)),
        out_shape=[
            token_shape,
            token_shape,
            v(ne, f_n),
            v(1, 128),
            grad_shape,
            grad_shape,
            grad_shape,
        ],
        in_specs=[hbm] * 12,
        out_specs=[vmem] * 4 + [anywhere] * 3,
        scratch_shapes=scratch,
        compiler_params=pltpu.CompilerParams(
            collective_id=0, has_side_effects=True, vmem_limit_bytes=61400000
        ),
        name="block",
    )(
        tokens,
        routes.T,
        dt_raw.T,
        b_proj.T,
        c_proj.T,
        decay_rate,
        skip_gain,
        router_weight.T,
        out_grad,
        gate_weight[0].T,
        up_weight[0].T,
        down_weight[0],
    )
    block_out, token_grad, router_grad, small, gate_grad, up_grad, down_grad = made
    outs = (gate_grad, up_grad, down_grad, block_out, token_grad, router_grad)
    gate_grad, up_grad, down_grad, block_out, token_grad, router_grad, rate_grad, skip_grad = pl.pallas_call(
        flush_kernel,
        out_shape=[shape(a.shape, a.dtype) for a in outs] + [shape((heads,), F32)] * 2,
        in_specs=[anywhere] * 6 + [vmem],
        out_specs=[hbm] * 6 + [vmem] * 2,
        scratch_shapes=[pltpu.SemaphoreType.DMA((6,))],
        compiler_params=pltpu.CompilerParams(vmem_limit_bytes=4 * 1024 * 1024),
        name="flush",
    )(*outs, small)
    return (
        block_out,
        token_grad,
        gate_grad.T[None],
        up_grad.T[None],
        down_grad[None],
        router_grad.T,
        rate_grad,
        skip_grad,
    )


def solution(mesh):
    return jax.shard_map(
        body,
        mesh=mesh,
        in_specs=(
            P("expert", "dp"),
            P("expert", None),
            P("expert", "dp"),
            P("expert", None),
            P("expert", None),
            P("dp"),
            P("dp"),
            P("dp", None),
            P("expert", None, "dp"),
            P("expert", None, "dp"),
            P("expert", "dp", None),
            P("expert", "dp"),
        ),
        out_specs=(
            P("expert", "dp"),
            P("expert", "dp"),
            P("expert", None, "dp"),
            P("expert", None, "dp"),
            P("expert", "dp", None),
            P("dp", None),
            P("dp"),
            P("dp"),
        ),
        check_vma=False,
    )
```
